32 devices in a mesh: rep: 2 (over y), gx: 16 (over z, x, core).
Axes of the slice: x: 2, y: 2, z: 4, core: 2. Of those that a mesh axis runs over, the one named last changes fastest.
Arguments:
- positions: float32 [3, 32768], P(None, ('rep', 'gx')), parts along dimension 1, may hold values from 0 to 8, as said below
- field: float32 [3, 32768], P(None, ('rep', 'gx')), parts along dimension 1, may hold values from -45 to 45
- inv_polar: float32 [32768], P(('rep', 'gx')), parts along dimension 0, may hold values from 2 to 8
- x_spline: float32 [2, 5, 32768], P(None, None, ('rep', 'gx')), parts along dimension 2, may hold values from -1 to 1, as said below
- yz_spline: float32 [4, 32768, 128], P(None, ('rep', 'gx')), parts along dimension 1, may hold values from -1 to 1, as said below
- tile_list: int32 [256, 7], P(('rep', 'gx')), parts along dimension 0, may hold values from 0 to 13, as said below
- tile_count: int32 [256], P(('rep', 'gx')), parts along dimension 0, may hold values from 1 to 7, as said below
Outputs:
- dipoles: float32 [3, 32768], P(None, ('rep', 'gx')), parts along dimension 1
- residual: float32 [3, 32768], P(None, ('rep', 'gx')), parts along dimension 1
The draws below stay inside these ranges and needn't reach their ends.
There are 2 independent parts, one for each index of `rep`. The reference program is written for one: setup_inputs(seed, part) draws one part's arguments, and reference() takes and returns one part's arrays. A program takes and returns all parts, laid end to end along the dimension named above; each array names one. Nothing has to cross between parts.
Inputs may be any that keep to these rules, and one draw needn't show every extreme that they name: `positions`: the first coordinate of an atom of block b of its slab lies in [b, b + 1); the other two lie in [0, 2). x_spline[0, k, i] and x_spline[1, k, i] are the cardinal B-spline of order 5 and its derivative at u_i + 4 - k for some u_i in [0, 1). `yz_spline`: rows 0 and 1 hold, for each atom, the cardinal B-spline of order 5 and its derivative at u + 4 - k placed at grid line (t + k) mod 128 for k < 5, for some start t and some u in [0, 1), and zero elsewhere; rows 2 and 3 likewise with their own start and offset. `tile_list`: row g = s * 8 + b lists in rising order the extended blocks b + 3 + e, -3 <= e <= 3, for which global blocks g and g + e (modulo 128) are neighbours; being neighbours is symmetric and always holds for e = 0; entries from tile_count[g] on equal b + 3. `tile_count`: global block 0 has all 7 neighbours.
All inputs are finite; a program needn't handle non-finite values.
Results may differ from the reference program's by a relative error of at most 0.0003.
Values sent between devices are 32-bit elements; how exact they have to be, the bound alone decides.
A program may use at most 64 MiB of HBM per device.

```python
import math
import jax
import jax.numpy as jnp
from jax import lax

GRID = 128
ORDER = 5
TILE = 128
HALO_BLK = 3
ITERS = 3
ATOM_DEV = 1024
NNB = 7
ATOMS = 16384
SLAB_BLOCKS = 8
BLOCKS = 128
N_GX = 16


def cardinal(order_now, at_point):
    if order_now == 2:
        return jnp.maximum(0.0, 1.0 - jnp.abs(at_point - 1.0))
    lower_part = cardinal(order_now - 1, at_point)
    upper_part = cardinal(order_now - 1, at_point - 1.0)
    return (at_point * lower_part + (order_now - at_point) * upper_part) / (order_now - 1)


def spline_pair(frac):
    shifts = (ORDER - 1 - jnp.arange(ORDER, dtype=jnp.int32)).astype(jnp.float32)
    points = frac[None, :] + shifts[:, None]
    spline_value = cardinal(ORDER, points)
    spline_slope = cardinal(ORDER - 1, points) - cardinal(ORDER - 1, points - 1.0)
    return (spline_value, spline_slope)


def draw_positions(key, part):
    atom_index = jnp.arange(ATOMS, dtype=jnp.int32)
    block_of = (atom_index % ATOM_DEV // TILE).astype(jnp.float32)
    uniform_draw = jax.random.uniform(key, (3, ATOMS), jnp.float32)
    return jnp.stack([block_of + uniform_draw[0], 2.0 * uniform_draw[1], 2.0 * uniform_draw[2]]).astype(jnp.float32)


def draw_field(key, part):
    atom_index = jnp.arange(ATOMS, dtype=jnp.int32)
    slab_of = (atom_index // ATOM_DEV).astype(jnp.float32)
    slab_total = ATOMS // ATOM_DEV
    ramp = 1.0 + 2.0 * slab_of / max(slab_total - 1, 1)
    normal_draw = jnp.clip(jax.random.normal(jax.random.fold_in(key, 1), (3, ATOMS), jnp.float32), -4.0, 4.0)
    return (normal_draw * ramp[None, :]).astype(jnp.float32)


def draw_x_spline(key, part):
    frac = jax.random.uniform(key, (ATOMS,), jnp.float32)
    spline_value, spline_slope = spline_pair(frac)
    return jnp.stack([spline_value, spline_slope]).astype(jnp.float32)


def draw_yz_spline(key, part):
    grid_lines = jnp.arange(GRID, dtype=jnp.int32)
    tables = []
    for axis_code in (1, 2):
        sub_key = jax.random.fold_in(key, axis_code)
        start_line = jax.random.randint(jax.random.fold_in(sub_key, 1), (ATOMS,), 0, GRID, dtype=jnp.int32)
        frac = jax.random.uniform(jax.random.fold_in(sub_key, 2), (ATOMS,), jnp.float32)
        spline_value, spline_slope = spline_pair(frac)
        dense_value = jnp.zeros((ATOMS, GRID), jnp.float32)
        dense_slope = jnp.zeros((ATOMS, GRID), jnp.float32)
        for spline_step in range(ORDER):
            matches = ((start_line + spline_step) % GRID)[:, None] == grid_lines[None, :]
            dense_value = dense_value + jnp.where(matches, spline_value[spline_step][:, None], 0.0)
            dense_slope = dense_slope + jnp.where(matches, spline_slope[spline_step][:, None], 0.0)
        tables.append(dense_value)
        tables.append(dense_slope)
    return jnp.stack(tables).astype(jnp.float32)


def neighbour_table(key):
    block_ids = jnp.arange(BLOCKS, dtype=jnp.int32)
    reach = jnp.arange(1, HALO_BLK + 1, dtype=jnp.int32)
    coins = jax.random.randint(jax.random.fold_in(key, 7), (BLOCKS, HALO_BLK), 0, 2, dtype=jnp.int32)
    first_block = block_ids == 0
    partner = (block_ids[:, None] + reach[None, :]) % BLOCKS
    coins = jnp.where(first_block[:, None] | first_block[partner], 1, coins)
    upper_side = coins
    lower_rows = (block_ids[:, None] - reach[None, :]) % BLOCKS
    lower_side = coins[lower_rows, (reach - 1)[None, :]]
    linked = jnp.concatenate([lower_side[:, ::-1], jnp.ones((BLOCKS, 1), jnp.int32), upper_side], axis=1)
    live_count = jnp.sum(linked, axis=1).astype(jnp.int32)
    slot_ids = jnp.arange(NNB, dtype=jnp.int32)
    sort_keys = jnp.where(linked == 1, slot_ids[None, :], NNB + slot_ids[None, :])
    ordering = jnp.argsort(sort_keys, axis=1, stable=True).astype(jnp.int32)
    local_block = (block_ids % SLAB_BLOCKS)[:, None]
    entries = jnp.where(slot_ids[None, :] < live_count[:, None], local_block + ordering, local_block + HALO_BLK)
    return (entries.astype(jnp.int32), live_count)


def draw_tile_list(key, part):
    entries, live_count = neighbour_table(key)
    return entries


def draw_tile_count(key, part):
    entries, live_count = neighbour_table(key)
    return live_count.astype(jnp.int32)


def levels(stream_key, shape, split, low, high):
    gain, own = 1.0, jax.random.fold_in(stream_key, 6)
    for dim, shards_of in split:
        draws = jnp.exp(jax.random.uniform(jax.random.fold_in(own, dim), (shards_of,), jnp.float32, low / len(split), high / len(split)))
        gain = gain * jnp.repeat(draws, shape[dim] // shards_of).reshape([-1 if axis == dim else 1 for axis in range(len(shape))])
    return gain


def setup_inputs(seed: int = 0, part: int = 0) -> dict:
    keys = jax.random.split(jax.random.key(seed), 8)
    part_keys = jax.random.split(jax.random.fold_in(keys[7], part), 8)
    positions = draw_positions(jax.random.fold_in(jax.random.fold_in(keys[7], part), 71), part)
    field = draw_field(jax.random.fold_in(jax.random.fold_in(keys[7], part), 71), part)
    inv_polar = jnp.clip(jnp.exp(math.log(8.0) - 1.3862944 * jax.random.uniform(part_keys[2], (ATOMS,), jnp.float32) ** levels(part_keys[2], (ATOMS,), ((0, 16),), -0.2, 0.2)), 2.0, 8.0)
    x_spline = draw_x_spline(jax.random.fold_in(jax.random.fold_in(keys[7], part), 71), part)
    yz_spline = draw_yz_spline(jax.random.fold_in(jax.random.fold_in(keys[7], part), 71), part)
    tile_list = draw_tile_list(jax.random.fold_in(jax.random.fold_in(keys[7], part), 71), part)
    tile_count = draw_tile_count(jax.random.fold_in(jax.random.fold_in(keys[7], part), 71), part)
    return {"positions": positions, "field": field, "inv_polar": inv_polar, "x_spline": x_spline, "yz_spline": yz_spline, "tile_list": tile_list, "tile_count": tile_count}


PAIR_C = 0.025
RECIP_C = 8192.0
DAMP = 0.0008
EXACT = lax.Precision.HIGHEST

def pair_field(home_pos, ext_pos, ext_vec, tile_rows, live_counts):
    slab_blocks = home_pos.shape[1] // TILE
    ext_blocks = ext_pos.shape[1] // TILE
    home_blocks = home_pos.reshape(3, slab_blocks, TILE).transpose(1, 0, 2)
    pos_blocks = ext_pos.reshape(3, ext_blocks, TILE)
    vec_blocks = ext_vec.reshape(3, ext_blocks, TILE)
    slot_index = jnp.arange(tile_rows.shape[1], dtype=jnp.int32)
    self_pair = jnp.eye(TILE, dtype=bool)

    def one_block(carried, scan_item):
        home_block, tile_row, live_count, block_index = scan_item
        near_pos = jnp.take(pos_blocks, tile_row, axis=1)
        near_vec = jnp.take(vec_blocks, tile_row, axis=1)
        offsets = home_block[:, None, :, None] - near_pos[:, :, None, :]
        distance_sq = lax.optimization_barrier(jnp.sum(offsets * offsets, axis=0)) + 1.0
        inverse = lax.rsqrt(distance_sq)
        third_power = inverse * inverse * inverse
        fifth_power = third_power * inverse * inverse
        same_block = (tile_row == block_index + HALO_BLK)[:, None, None]
        live_mask = (slot_index < live_count)[:, None, None] & ~(same_block & self_pair[None])
        third_power = jnp.where(live_mask, third_power, 0.0)
        fifth_power = jnp.where(live_mask, fifth_power, 0.0)
        projection = lax.optimization_barrier(jnp.sum(offsets * near_vec[:, :, None, :], axis=0))
        field_sum = lax.optimization_barrier(jnp.sum(third_power[None] * near_vec[:, :, None, :] - 3.0 * (fifth_power * projection)[None] * offsets, axis=(1, 3)))
        return (carried, PAIR_C * field_sum)
    block_ids = jnp.arange(slab_blocks, dtype=jnp.int32)
    unused_carry, blocks_out = lax.scan(one_block, jnp.zeros((), jnp.float32), (home_blocks, tile_rows, live_counts, block_ids))
    return blocks_out.transpose(1, 0, 2).reshape(3, slab_blocks * TILE)

def slab_weights(local_plane, x_spline, planes):
    spline_steps = jnp.arange(ORDER, dtype=jnp.int32)
    plane_index = jnp.arange(planes, dtype=jnp.int32)
    matches = local_plane[None, :, None] + spline_steps[:, None, None] == plane_index[None, None, :]
    spline_value = lax.optimization_barrier(jnp.sum(jnp.where(matches, x_spline[0][:, :, None], 0.0), axis=0))
    spline_slope = lax.optimization_barrier(jnp.sum(jnp.where(matches, x_spline[1][:, :, None], 0.0), axis=0))
    return (spline_value, spline_slope)

def spread_dipoles(vector, spline_value, spline_slope, yz_spline):
    atoms_here = spline_value.shape[0]
    planes = spline_value.shape[1]
    grid_lines = yz_spline.shape[2]
    lead_terms = (vector[0][:, None] * spline_slope)[:, :, None] * yz_spline[0][:, None, :]
    lead_terms = lead_terms + (vector[1][:, None] * spline_value)[:, :, None] * yz_spline[1][:, None, :]
    tail_terms = (vector[2][:, None] * spline_value)[:, :, None] * yz_spline[0][:, None, :]
    contract = (((0,), (0,)), ((), ()))
    charge = lax.dot_general(lead_terms.reshape(atoms_here, planes * grid_lines), yz_spline[2], contract, precision=EXACT)
    charge = charge + lax.dot_general(tail_terms.reshape(atoms_here, planes * grid_lines), yz_spline[3], contract, precision=EXACT)
    return charge.reshape(planes, grid_lines, grid_lines)

def gather_field(potential, spline_value, spline_slope, yz_spline):
    planes = potential.shape[0]
    grid_lines = potential.shape[1]
    atoms_here = spline_value.shape[0]
    flat_grid = potential.reshape(planes * grid_lines, grid_lines)
    contract = (((1,), (1,)), ((), ()))
    plain_sum = lax.dot_general(yz_spline[2], flat_grid, contract, precision=EXACT).reshape(atoms_here, planes, grid_lines)
    tilted_sum = lax.dot_general(yz_spline[3], flat_grid, contract, precision=EXACT).reshape(atoms_here, planes, grid_lines)
    first_comp = lax.optimization_barrier(jnp.sum(spline_slope[:, :, None] * yz_spline[0][:, None, :] * plain_sum, axis=(1, 2)))
    second_comp = lax.optimization_barrier(jnp.sum(spline_value[:, :, None] * yz_spline[1][:, None, :] * plain_sum, axis=(1, 2)))
    third_comp = lax.optimization_barrier(jnp.sum(spline_value[:, :, None] * yz_spline[0][:, None, :] * tilted_sum, axis=(1, 2)))
    return jnp.stack([first_comp, second_comp, third_comp])

def reference_kernel():
    freq = jnp.arange(GRID, dtype=jnp.int32)
    signed = jnp.where(freq <= GRID // 2, freq, freq - GRID).astype(jnp.float32)
    last_freq = jnp.arange(GRID // 2 + 1, dtype=jnp.int32).astype(jnp.float32)
    mode_sq = signed[:, None, None] * signed[:, None, None] + signed[None, :, None] * signed[None, :, None] + last_freq[None, None, :] * last_freq[None, None, :]
    safe_sq = jnp.where(mode_sq > 0, mode_sq, 1.0)
    return jnp.where(mode_sq > 0, RECIP_C * jnp.exp(-DAMP * safe_sq) / safe_sq, 0.0)

def reference(positions, field, inv_polar, x_spline, yz_spline, tile_list, tile_count):
    slabs = N_GX
    planes = GRID // slabs
    extent = planes + 4
    halo_atoms = HALO_BLK * TILE
    slab_blocks = ATOM_DEV // TILE
    slab_ids = jnp.arange(slabs, dtype=jnp.int32)
    shift_x = jnp.concatenate([jnp.full((halo_atoms,), -1.0 * slab_blocks, jnp.float32), jnp.zeros((ATOM_DEV,), jnp.float32), jnp.full((halo_atoms,), 1.0 * slab_blocks, jnp.float32)])
    kernel = reference_kernel()
    place = slab_ids[:, None] * planes + jnp.arange(extent, dtype=jnp.int32)[None, :]
    local_plane = (jnp.arange(ATOM_DEV, dtype=jnp.int32) * planes // ATOM_DEV).astype(jnp.int32)

    def wrap_pad(array):
        return jnp.concatenate([array[:, -halo_atoms:], array, array[:, :halo_atoms]], axis=1)
    pos_pad = wrap_pad(positions)

    def slab_parts(slab):
        begin = slab * ATOM_DEV
        own_pos = lax.dynamic_slice_in_dim(positions, begin, ATOM_DEV, 1)
        ext_pos = lax.dynamic_slice_in_dim(pos_pad, begin, ATOM_DEV + 2 * halo_atoms, 1)
        ext_pos = ext_pos.at[0].add(shift_x)
        splines = lax.dynamic_slice_in_dim(x_spline, begin, ATOM_DEV, 2)
        dense = lax.dynamic_slice_in_dim(yz_spline, begin, ATOM_DEV, 1)
        tile_rows = lax.dynamic_slice_in_dim(tile_list, slab * slab_blocks, slab_blocks, 0)
        live_counts = lax.dynamic_slice_in_dim(tile_count, slab * slab_blocks, slab_blocks, 0)
        spline_value, spline_slope = slab_weights(local_plane, splines, extent)
        return (own_pos, ext_pos, spline_value, spline_slope, dense, tile_rows, live_counts)

    def apply(vector):
        vec_pad = wrap_pad(vector)

        def near_and_charge(slab):
            parts = slab_parts(slab)
            begin = slab * ATOM_DEV
            ext_vec = lax.dynamic_slice_in_dim(vec_pad, begin, ATOM_DEV + 2 * halo_atoms, 1)
            own_vec = lax.dynamic_slice_in_dim(vector, begin, ATOM_DEV, 1)
            near_field = pair_field(parts[0], parts[1], ext_vec, parts[5], parts[6])
            charge = spread_dipoles(own_vec, parts[2], parts[3], parts[4])
            return (near_field, charge)
        near_all, charges = lax.map(near_and_charge, slab_ids)
        padded = jnp.zeros((GRID + 4, GRID, GRID), jnp.float32).at[place].add(charges)
        whole = padded[2:GRID + 2]
        whole = whole.at[GRID - 2:].add(padded[:2]).at[:2].add(padded[GRID + 2:])
        potential = jnp.fft.irfftn(jnp.fft.rfftn(whole) * kernel, s=whole.shape)
        pot_pad = jnp.concatenate([potential[GRID - 2:], potential, potential[:2]], axis=0)

        def far_part(scan_item):
            slab, local_pot = scan_item
            parts = slab_parts(slab)
            return gather_field(local_pot, parts[2], parts[3], parts[4])
        far_all = lax.map(far_part, (slab_ids, pot_pad[place]))
        near_whole = near_all.transpose(1, 0, 2).reshape(3, ATOMS)
        far_whole = far_all.transpose(1, 0, 2).reshape(3, ATOMS)
        return inv_polar[None, :] * vector + far_whole - near_whole
    dipoles = jnp.zeros_like(field)
    residual = field
    precond = field / inv_polar[None, :]
    direction = precond
    rz_now = jnp.sum(residual * precond)
    for sweep_index in range(ITERS):
        applied = apply(direction)
        step_size = rz_now / jnp.sum(direction * applied)
        dipoles = dipoles + step_size * direction
        residual = residual - step_size * applied
        if sweep_index + 1 < ITERS:
            precond = residual / inv_polar[None, :]
            rz_next = jnp.sum(residual * precond)
            direction = precond + rz_next / rz_now * direction
            rz_now = rz_next
    return (dipoles, residual)
```

```python
import jax
import jax.numpy as jnp
from jax import lax
from jax.experimental import pallas as pl
from jax.experimental.pallas import tpu as pltpu
from jax.sharding import PartitionSpec as P
import functools
import numpy as np

GRID = 128
ORDER = 5
TILE = 128
HALO_BLK = 3
ITERS = 3


PAIR_C = 0.025
RECIP_C = 8192.0
DAMP = 0.0008
EXACT = lax.Precision.HIGHEST


def mode_of(freq, size):
    half_size = size // 2
    mode_num = jnp.where(freq <= half_size, freq, freq - half_size)
    weight = jnp.where((freq == 0) | (freq == half_size), 1.0 / size, 2.0 / size)
    return (mode_num.astype(jnp.float32), weight.astype(jnp.float32))


def basis_rows(size, points):
    freq = jnp.arange(size, dtype=jnp.int32)
    half_size = size // 2
    mode_num = jnp.where(freq <= half_size, freq, freq - half_size)
    phase = mode_num[:, None] * points[None, :] % size
    angle = phase.astype(jnp.float32) * (2.0 * jnp.pi / size)
    return jnp.where((freq <= half_size)[:, None], jnp.cos(angle), jnp.sin(angle))


def kernel_block(x_modes, x_weights, y_modes, y_weights, z_modes, z_weights):
    mode_sq = (
        x_modes[:, None, None] * x_modes[:, None, None]
        + y_modes[None, :, None] * y_modes[None, :, None]
        + z_modes[None, None, :] * z_modes[None, None, :]
    )
    safe_sq = jnp.where(mode_sq > 0, mode_sq, 1.0)
    green = jnp.where(mode_sq > 0, RECIP_C * jnp.exp(-DAMP * safe_sq) / safe_sq, 0.0)
    return green * x_weights[:, None, None] * y_weights[None, :, None] * z_weights[None, None, :]


F32 = jnp.float32
BF16 = jnp.bfloat16
VMEM = pl.BlockSpec(memory_space=pltpu.VMEM)


def split(x):
    high = x.astype(BF16)
    return high, (x - high.astype(F32)).astype(BF16)


def dot(a, b):
    return jnp.dot(a, b, preferred_element_type=F32)


def params(**more):
    return pltpu.CompilerParams(vmem_limit_bytes=56 * 1024 * 1024, **more)


def prep_kernel(yz_ref, rows_ref, yft_ref, zf_ref, zft_ref):
    rows = jnp.concatenate(split(rows_ref[...]), axis=0)

    def transformed(t):
        high, low = split(jnp.concatenate([yz_ref[t], yz_ref[t + 1]], axis=0))
        contract = (((1,), (1,)), ((), ()))
        wide = lax.dot_general(rows, high, contract, preferred_element_type=F32)
        more = lax.dot_general(rows[:GRID], low, contract, preferred_element_type=F32)
        return wide[:GRID] + wide[GRID:] + more

    lines = transformed(0)
    yft_ref[0, 0] = lines[:, :TILE]
    yft_ref[0, 1] = lines[:, TILE:]
    lines = transformed(2)
    zft_ref[0] = jnp.concatenate(split(lines), axis=0)
    zf_ref[0] = jnp.concatenate(split(lines.T), axis=1)


def prepare(yz_spline, rows, blocks):
    return pl.pallas_call(
        prep_kernel,
        grid=(blocks,),
        in_specs=[
            pl.BlockSpec((4, TILE, GRID), lambda b: (0, b, 0)),
            pl.BlockSpec((GRID, GRID), lambda b: (0, 0)),
        ],
        out_specs=[
            pl.BlockSpec((1, 2, GRID, TILE), lambda b: (b, 0, 0, 0)),
            pl.BlockSpec((1, 2 * TILE, 2 * GRID), lambda b: (b, 0, 0)),
            pl.BlockSpec((1, 2 * GRID, 2 * TILE), lambda b: (b, 0, 0)),
        ],
        out_shape=[
            jax.ShapeDtypeStruct((blocks, 2, GRID, TILE), F32),
            jax.ShapeDtypeStruct((blocks, 2 * TILE, 2 * GRID), BF16),
            jax.ShapeDtypeStruct((blocks, 2 * GRID, 2 * TILE), BF16),
        ],
        compiler_params=params(),
        name="prep",
    )(yz_spline, rows)


def spread_kernel(planes, ky_count, pv_ref, xs_ref, yft_ref, zf_ref, out_ref):
    blocks = pv_ref.shape[0]
    ranks = out_ref.shape[0]
    out_ref[...] = jnp.zeros_like(out_ref)

    def one_block(b, carry):
        base = b * planes // blocks
        y, dy = yft_ref[b, 0], yft_ref[b, 1]
        v0, v1, v2 = (pv_ref[b, 3 + c : 4 + c, :] for c in range(3))
        highs, lows = [], []
        for k in range(ORDER):
            x, dx = xs_ref[b, k : k + 1, :], xs_ref[b, ORDER + k : ORDER + k + 1, :]
            lead = (v0 * dx) * y + (v1 * x) * dy
            high, low = split(jnp.concatenate([lead, (v2 * x) * y], axis=1))
            highs.append(high)
            lows.append(low)
        weights = zf_ref[b]
        wide = dot(jnp.concatenate(highs, axis=0), weights)
        total = (
            wide[:, :GRID] + wide[:, GRID:] + dot(jnp.concatenate(lows, axis=0), weights[:, :GRID])
        )
        for k in range(ORDER):
            part = total[k * GRID : (k + 1) * GRID].reshape(ranks, ky_count, GRID)
            out_ref[:, base + k, :ky_count, :] += part
        return carry

    lax.fori_loop(0, blocks, one_block, 0)


def gather_kernel(
    planes, ky_count, ret_ref, xs_ref, yft_ref, zft_ref, pair_ref, pv_ref, polar_ref,
    next_ref, pv_next_ref, wide_ref, low_ref,
):
    blocks = xs_ref.shape[0]
    extent = ret_ref.shape[1]
    for p in range(extent):
        high, low = split(ret_ref[:, p, :ky_count, :].reshape(GRID, GRID))
        wide_ref[p] = jnp.concatenate([high, high], axis=1)
        low_ref[p] = low

    def one_block(b, carry):
        base = b * planes // blocks
        weights = zft_ref[b]
        wide = wide_ref[pl.ds(base, ORDER)].reshape(ORDER * GRID, 2 * GRID)
        low = low_ref[pl.ds(base, ORDER)].reshape(ORDER * GRID, GRID)
        sums = dot(wide, weights) + dot(low, weights[:GRID])
        one = two = three = 0.0
        for k in range(ORDER):
            x, dx = xs_ref[b, k : k + 1, :], xs_ref[b, ORDER + k : ORDER + k + 1, :]
            plain = sums[k * GRID : (k + 1) * GRID, :TILE]
            one += dx * plain
            two += x * plain
            three += x * sums[k * GRID : (k + 1) * GRID, TILE:]
        y, dy = yft_ref[b, 0], yft_ref[b, 1]
        far = jnp.concatenate(
            [jnp.sum(t, axis=0, keepdims=True) for t in (y * one, dy * two, y * three)], axis=0
        )
        following = pair_ref[b] - far
        next_ref[b] = following
        pv_next_ref[b, 0:3] = pv_ref[b, 0:3]
        pv_next_ref[b, 3:6] = following / polar_ref[b]
        pv_next_ref[b, 6:8] = jnp.zeros((2, TILE), F32)
        return carry

    lax.fori_loop(0, blocks, one_block, 0)


def pair_sum(near_ref, pv_ref, before_ref, after_ref, out_ref, ext_ref, col_ref):
    blocks = pv_ref.shape[0]
    reach = 2 * HALO_BLK + 1
    first_row = lax.broadcasted_iota(jnp.int32, (HALO_BLK, 8, TILE), 1) == 0
    ext_ref[:HALO_BLK] = before_ref[...] + jnp.where(first_row, -1.0 * blocks, 0.0)
    ext_ref[HALO_BLK : HALO_BLK + blocks] = pv_ref[...]
    ext_ref[HALO_BLK + blocks :] = after_ref[...] + jnp.where(first_row, 1.0 * blocks, 0.0)
    lag = lax.broadcasted_iota(jnp.int32, (8, TILE), 1) - lax.broadcasted_iota(
        jnp.int32, (8, TILE), 0
    )

    def spread_columns(e, carry):
        for c in range(6):
            col_ref[e, c] = jnp.broadcast_to(ext_ref[e, c : c + 1, :], (TILE, TILE)).T
        return carry

    lax.fori_loop(0, blocks + 2 * HALO_BLK, spread_columns, 0)

    def one_home(b, carry):
        home = [jnp.broadcast_to(pv_ref[b, c : c + 1, :], (8, TILE)) for c in range(3)]

        def one_source(k, sums):
            shift = jnp.where(k == HALO_BLK, 0, 4 * TILE)
            direct = [jnp.zeros((8, TILE), F32) for c in range(3)]
            tilted = [jnp.zeros((8, TILE), F32) for c in range(3)]
            for j in range(TILE // 8):
                rows = slice(8 * j, 8 * j + 8)
                r = [home[c] - col_ref[b + k, c, rows, :] for c in range(3)]
                v = [col_ref[b + k, 3 + c, rows, :] for c in range(3)]
                inverse = lax.rsqrt(r[0] * r[0] + r[1] * r[1] + r[2] * r[2] + 1.0)
                inverse = jnp.where(lag != 8 * j + shift, inverse, 0.0)
                square = inverse * inverse
                third = square * inverse
                weight = third * square * (r[0] * v[0] + r[1] * v[1] + r[2] * v[2])
                for c in range(3):
                    direct[c] += third * v[c]
                    tilted[c] += weight * r[c]
            near = near_ref[b * reach + k]
            return tuple(
                sums[c] + near * (direct[c] - 3.0 * tilted[c]) for c in range(3)
            )

        sums = lax.fori_loop(0, reach, one_source, (jnp.zeros((8, TILE), F32),) * 3)
        out_ref[b] = PAIR_C * jnp.concatenate(
            [jnp.sum(t, axis=0, keepdims=True) for t in sums], axis=0
        )
        return carry

    lax.fori_loop(0, blocks, one_home, 0)


def greet(ranks, me):
    barrier = pltpu.get_barrier_semaphore()

    def signal(d, carry):
        pl.semaphore_signal(
            barrier,
            inc=1,
            device_id={"gx": lax.rem(me + d, ranks)},
            device_id_type=pl.DeviceIdType.MESH,
        )
        return carry

    lax.fori_loop(1, ranks, signal, 0)
    pl.semaphore_wait(barrier, ranks - 1)


def exchange(ranks, me, source, target, local_sem, send_sem, recv_sem):
    def copy(d, slot):
        peer = lax.rem(me + d, ranks)
        return pltpu.make_async_remote_copy(
            src_ref=source(peer),
            dst_ref=target(slot),
            send_sem=send_sem.at[d],
            recv_sem=recv_sem.at[d],
            device_id={"gx": peer},
            device_id_type=pl.DeviceIdType.MESH,
        )

    def start(d, carry):
        copy(d, me).start()
        return carry

    def finish(d, carry):
        copy(d, lax.rem(me - d + ranks, ranks)).wait()
        return carry

    lax.fori_loop(1, ranks, start, 0)
    own = pltpu.make_async_copy(source(me), target(me), local_sem)
    own.start()

    def wait():
        own.wait()
        lax.fori_loop(1, ranks, finish, 0)

    return wait


def middle_kernel(
    ranks, ky_count, near_ref, spec_ref, pv_ref, green_ref, across_ref, back_ref,
    ret_ref, pair_ref,
    before_ref, after_ref, ext_ref, col_ref, recv_ref, done_ref, local_sems, send1, recv1, send2, recv2, halo_send, halo_recv,
):
    me = lax.axis_index("gx")
    blocks = pv_ref.shape[0]
    extent = spec_ref.shape[1]
    rows = ranks * extent
    greet(ranks, me)
    halos = []
    for t, (piece, into, step) in enumerate(
        (
            (pv_ref.at[pl.ds(blocks - HALO_BLK, HALO_BLK)], before_ref, 1),
            (pv_ref.at[pl.ds(0, HALO_BLK)], after_ref, ranks - 1),
        )
    ):
        halos.append(
            pltpu.make_async_remote_copy(
                src_ref=piece,
                dst_ref=into,
                send_sem=halo_send.at[t],
                recv_sem=halo_recv.at[t],
                device_id={"gx": lax.rem(me + step, ranks)},
                device_id_type=pl.DeviceIdType.MESH,
            )
        )
        halos[-1].start()
    wait = exchange(
        ranks, me, lambda d: spec_ref.at[d], lambda d: recv_ref.at[d], local_sems.at[0], send1, recv1
    )
    across_high, across_low = split(across_ref[...])
    back_high, back_low = split(back_ref[...])
    wait()
    lines_in = recv_ref.reshape(rows * 8, GRID)
    lines_out = done_ref.reshape(rows * 8, GRID)
    for q in range(ky_count):
        high, low = split(lines_in[pl.ds(q, rows, stride=8), :])
        wide = dot(across_high, jnp.concatenate([high, low], axis=1))
        line = wide[:, :GRID] + wide[:, GRID:] + dot(across_low, high)
        high, low = split(line * green_ref[q])
        wide = dot(back_high, jnp.concatenate([high, low], axis=1))
        lines_out[pl.ds(q, rows, stride=8), :] = (
            wide[:, :GRID] + wide[:, GRID:] + dot(back_low, high)
        )
    wait = exchange(
        ranks, me, lambda d: done_ref.at[d], lambda d: ret_ref.at[d], local_sems.at[1], send2, recv2
    )
    for halo in halos:
        halo.wait()
    pair_sum(near_ref, pv_ref, before_ref, after_ref, pair_ref, ext_ref, col_ref)
    wait()


def middle(near, spec, pv, green, across, back, ranks, ky_count):
    dma = pltpu.SemaphoreType.DMA
    blocks = pv.shape[0]
    halo = pltpu.VMEM((HALO_BLK, 8, TILE), F32)
    return pl.pallas_call(
        functools.partial(middle_kernel, ranks, ky_count),
        in_specs=[pl.BlockSpec(memory_space=pltpu.SMEM)] + [VMEM] * 5,
        out_specs=[VMEM] * 2,
        out_shape=[
            jax.ShapeDtypeStruct(spec.shape, F32),
            jax.ShapeDtypeStruct((blocks, 3, TILE), F32),
        ],
        scratch_shapes=[
            halo,
            halo,
            pltpu.VMEM((blocks + 2 * HALO_BLK, 8, TILE), F32),
            pltpu.VMEM((blocks + 2 * HALO_BLK, 6, TILE, TILE), F32),
            pltpu.VMEM(spec.shape, F32),
            pltpu.VMEM(spec.shape, F32),
            dma((2,)), dma((ranks,)), dma((ranks,)), dma((ranks,)), dma((ranks,)),
            dma((2,)), dma((2,)),
        ],
        compiler_params=params(collective_id=0, has_side_effects=True),
        name="middle",
    )(near, spec, pv, green, across, back)


def combine(weights, parts):
    terms = [w * p for w, p in zip(weights, parts) if w is not None]
    return functools.reduce(jnp.add, terms)


def scaled(a, x, y):
    pairs = zip(x, y)
    return [p if q is None else (a * q if p is None else p + a * q) for p, q in pairs]


def solve_kernel(
    ranks, b0_ref, b1_ref, b2_ref, b3_ref, polar_ref,
    dipoles_ref, residual_ref, part_ref, slots, local_sem, send_sem, recv_sem,
):
    me = lax.axis_index("gx")
    bases = [ref[...] for ref in (b0_ref, b1_ref, b2_ref, b3_ref)]
    soft = [b / polar_ref[...] for b in bases]
    count = ITERS + 1
    place = {}
    part_ref[...] = jnp.zeros_like(part_ref)
    for i in range(count):
        for j in range(i, count):
            place[i, j] = place[j, i] = row = len(set(place.values()))
            part_ref[row : row + 1] = jnp.sum(
                jnp.sum(bases[i] * soft[j], axis=0), axis=0, keepdims=True
            )
    greet(ranks, me)
    wait = exchange(
        ranks, me, lambda d: part_ref, lambda d: slots.at[d], local_sem.at[0], send_sem, recv_sem
    )
    wait()
    sums = jnp.sum(jnp.sum(slots[...], axis=0), axis=1, keepdims=True)
    sums = jnp.broadcast_to(sums, (sums.shape[0], TILE))

    def inner(x, y):
        value = None
        for i in range(count):
            for j in range(count):
                if x[i] is not None and y[j] is not None:
                    row = place[i, j]
                    term = x[i] * y[j] * sums[row : row + 1]
                    value = term if value is None else value + term
        return value

    none = [None] * (count - 1)
    residual = [jnp.ones((1, TILE), F32)] + none
    direction = list(residual)
    dipoles = [None] * count
    rz_now = inner(residual, residual)
    for sweep in range(ITERS):
        image = scaled(-1.0, direction, [None] + direction[:-1])
        step = rz_now / inner(direction, image)
        dipoles = scaled(step, dipoles, direction)
        residual = scaled(-step, residual, image)
        if sweep + 1 < ITERS:
            rz_next = inner(residual, residual)
            direction = scaled(rz_next / rz_now, residual, direction)
            rz_now = rz_next
    dipoles_ref[...] = combine(dipoles, soft)
    residual_ref[...] = combine(residual, bases)


def solve(bases, polar, ranks):
    dma = pltpu.SemaphoreType.DMA
    shape = bases[0].shape
    return pl.pallas_call(
        functools.partial(solve_kernel, ranks),
        in_specs=[VMEM] * 5,
        out_specs=[VMEM] * 2,
        out_shape=[jax.ShapeDtypeStruct(shape, F32)] * 2,
        scratch_shapes=[
            pltpu.VMEM((16, TILE), F32), pltpu.VMEM((ranks, 16, TILE), F32),
            dma((1,)), dma((ranks,)), dma((ranks,)),
        ],
        compiler_params=params(collective_id=1, has_side_effects=True),
        name="solve",
    )(*bases, polar)


def fixed_rows(points):
    half_size = GRID // 2
    freq = np.arange(GRID)
    mode_num = np.where(freq <= half_size, freq, freq - half_size)
    angle = (mode_num[:, None] * points[None, :] % GRID) * (2.0 * np.pi / GRID)
    return np.where((freq <= half_size)[:, None], np.cos(angle), np.sin(angle)).astype(np.float32)


def per_device(positions, field, inv_polar, x_spline, yz_spline, tile_list, tile_count):
    ranks = lax.axis_size("gx")
    rank_index = lax.axis_index("gx")
    atoms_here = positions.shape[1]
    planes = GRID // ranks
    extent = planes + 4
    blocks = atoms_here // TILE
    reach = 2 * HALO_BLK + 1
    ky_count = GRID // ranks

    def blocked(x):
        return x.reshape(-1, blocks, TILE).transpose(1, 0, 2)

    all_freq = jnp.arange(GRID, dtype=jnp.int32)
    fourier_rows = jnp.asarray(fixed_rows(np.arange(GRID)))
    ky_freq = rank_index * ky_count + jnp.arange(ky_count, dtype=jnp.int32)
    full_modes, full_weights = mode_of(all_freq, GRID)
    ky_modes, ky_weights = mode_of(ky_freq, GRID)
    green = kernel_block(ky_modes, ky_weights, full_modes, full_weights, full_modes, full_weights)
    source_rows = np.arange(ranks * extent)
    points = (source_rows // extent * planes - 2 + source_rows % extent) % GRID
    across = fixed_rows(points)
    back = jnp.asarray(np.ascontiguousarray(across.T))
    across = jnp.asarray(across)
    slots = jnp.arange(tile_list.shape[1], dtype=jnp.int32)
    wanted = jnp.arange(blocks, dtype=jnp.int32)[:, None] + jnp.arange(reach, dtype=jnp.int32)
    live = (slots[None, :] < tile_count[:, None])[:, :, None]
    near = jnp.any((tile_list[:, :, None] == wanted[:, None, :]) & live, axis=1)
    near = near.astype(F32).reshape(-1)
    yft, zf, zft = prepare(yz_spline, fourier_rows, blocks)
    xs = blocked(x_spline.reshape(2 * ORDER, atoms_here))
    pos = blocked(positions)
    polar = inv_polar.reshape(blocks, 1, TILE)
    spec_shape = jax.ShapeDtypeStruct((ranks, extent, 8, GRID), F32)
    rows_shape = jax.ShapeDtypeStruct((blocks, 3, TILE), F32)

    def advance(pv):
        spec = pl.pallas_call(
            functools.partial(spread_kernel, planes, ky_count),
            in_specs=[VMEM] * 4,
            out_specs=VMEM,
            out_shape=spec_shape,
            compiler_params=params(),
            name="spread",
        )(pv, xs, yft, zf)
        ret, pair = middle(near, spec, pv, green, across, back, ranks, ky_count)
        return pl.pallas_call(
            functools.partial(gather_kernel, planes, ky_count),
            in_specs=[VMEM] * 7,
            out_specs=[VMEM] * 2,
            out_shape=[rows_shape, jax.ShapeDtypeStruct((blocks, 8, TILE), F32)],
            scratch_shapes=[
                pltpu.VMEM((extent, GRID, 2 * GRID), BF16),
                pltpu.VMEM((extent, GRID, GRID), BF16),
            ],
            compiler_params=params(),
            name="gather",
        )(ret, xs, yft, zft, pair, pv, polar)

    bases = [blocked(field)]
    pv = jnp.concatenate([pos, bases[0] / polar, jnp.zeros((blocks, 2, TILE), F32)], axis=1)
    for sweep in range(ITERS):
        following, pv = advance(pv)
        bases.append(following)
    dipoles, residual = solve(bases, polar, ranks)

    def flat(x):
        return x.transpose(1, 0, 2).reshape(3, atoms_here)

    return flat(dipoles), flat(residual)


FIELD0 = 5


def spline_rows(u):
    v = 1.0 - u

    def inner(p):
        return ((((-4.0 * p + 4.0) * p + 6.0) * p + 4.0) * p + 1.0) * (1.0 / 24.0)

    def slope(p):
        return (((-4.0 * p + 3.0) * p + 3.0) * p + 1.0) * (1.0 / 6.0)

    middle_value = ((((6.0 * u - 12.0) * u - 6.0) * u + 12.0) * u + 11.0) * (1.0 / 24.0)
    middle_slope = (((2.0 * u - 3.0) * u - 1.0) * u + 1.0) * 0.5
    values = [v * v * v * v * (1.0 / 24.0), inner(v), middle_value, inner(u), u * u * u * u * (1.0 / 24.0)]
    slopes = [v * v * v * (-1.0 / 6.0), -slope(v), middle_slope, slope(u), u * u * u * (1.0 / 6.0)]
    return values, slopes


def turn(steps):
    wrapped = steps - GRID * jnp.floor(steps * (1.0 / GRID) + 0.5)
    half = wrapped * (np.pi / GRID)
    square = half * half
    sine = -1.0 / 39916800.0
    for c in (1.0 / 362880.0, -1.0 / 5040.0, 1.0 / 120.0, -1.0 / 6.0, 1.0):
        sine = sine * square + c
    sine = sine * half
    cosine = 1.0 / 479001600.0
    for c in (-1.0 / 3628800.0, 1.0 / 40320.0, -1.0 / 720.0, 1.0 / 24.0, -0.5, 1.0):
        cosine = cosine * square + c
    return 1.0 - 2.0 * sine * sine, 2.0 * sine * cosine


def iota(shape, dim):
    return lax.broadcasted_iota(jnp.int32, shape, dim)


CONTRACT_LANES = (((1,), (1,)), ((), ()))


def fast_kernel(
    ranks, pos_ref, field_ref, polar_ref, xs_ref, list_ref, count_ref,
    center_ref, zin_ref, zout_ref, xin_ref, xout_ref, yz_ref,
    dip_ref, res_ref,
    lines, info, table, yq, xw, wt, vx, grid, spec, wide, low, green, tens, cols, place, sides, ext,
    bases, pair, out_part, in_part, part, slots,
    local_sem, ag_send, ag_recv, rs_send, rs_recv, side_send, side_recv, gram_send, gram_recv,
):
    me = lax.axis_index("gx")
    blocks = polar_ref.shape[0]
    planes = GRID // ranks
    kys = GRID // ranks
    halves = blocks // 4
    reach = 2 * HALO_BLK + 1

    def lanes(b):
        return slice(b * TILE, (b + 1) * TILE)

    loads = [
        pltpu.make_async_copy(yz_ref.at[2 * t], lines.at[t], local_sem.at[t]) for t in range(2)
    ]
    for load in loads:
        load.start()

    barrier = pltpu.get_barrier_semaphore()

    def greet_one(d, carry):
        pl.semaphore_signal(
            barrier, inc=1, device_id={"gx": lax.rem(me + d, ranks)}, device_id_type=pl.DeviceIdType.MESH
        )
        return carry

    lax.fori_loop(1, ranks, greet_one, 0)

    for c in range(3):
        for b in range(blocks):
            place[c, b : b + 1, :] = pos_ref[c : c + 1, lanes(b)]
            bases[0, c, b : b + 1, :] = field_ref[c : c + 1, lanes(b)]
    for c in range(3):
        info[me, FIELD0 + c] = bases[0, c] / polar_ref[...]
    offset = -1.5
    for k in range(1, ORDER):
        offset = offset + (1.0 * k) * xs_ref[k, 0:1, :]
    for b in range(blocks):
        info[me, 4, b : b + 1, :] = offset[:, lanes(b)]
    for load in loads:
        load.wait()
    marks = iota((GRID, TILE), 0).astype(F32)
    for t in range(2):
        for b in range(blocks):
            line = lines[t, lanes(b), :]
            high = line.astype(BF16)
            rest = line - high.astype(F32)
            mid, tail = split(rest)
            moment = lax.dot_general(
                center_ref[...], jnp.concatenate([high, mid, tail], axis=1), CONTRACT_LANES,
                preferred_element_type=F32,
            )
            moment, weight = moment[:GRID], moment[GRID:]
            best = jnp.max(
                jnp.where((jnp.abs(moment) < 0.5001) & (weight > 0.25), marks, -1.0), axis=0, keepdims=True
            )
            shift = jnp.sum(jnp.where(marks == best, moment, 0.0), axis=0, keepdims=True)
            start = best - 2.0
            info[me, 2 * t, b : b + 1, :] = jnp.where(start < 0, start + GRID, start)
            info[me, 2 * t + 1, b : b + 1, :] = shift + 0.5

    pl.semaphore_wait(barrier, ranks - 1)

    def share(i, first, source=None):
        owner = me if source is None else source
        span = info.at[owner] if first else info.at[owner, pl.ds(FIELD0, 3)]
        return pltpu.make_async_remote_copy(
            src_ref=span, dst_ref=span, send_sem=ag_send.at[i], recv_sem=ag_recv.at[i],
            device_id={"gx": lax.rem(me + i, ranks)}, device_id_type=pl.DeviceIdType.MESH,
        )

    def fold(i, slab):
        return pltpu.make_async_remote_copy(
            src_ref=out_part.at[slab], dst_ref=in_part.at[i], send_sem=rs_send.at[i], recv_sem=rs_recv.at[i],
            device_id={"gx": slab}, device_id_type=pl.DeviceIdType.MESH,
        )

    def away(d):
        step = (d + 1) // 2
        return lax.rem(jnp.where(d % 2 == 1, step, ranks - step), ranks)

    def start_share(first):
        def one(d, carry):
            share(away(d), first).start()
            return carry

        lax.fori_loop(1, ranks, one, 0)

    def sent_share(first):
        def one(i, carry):
            share(i, first).wait_send()
            return carry

        lax.fori_loop(1, ranks, one, 0)

    def got_share(d, first):
        off = away(d)
        share(lax.rem(ranks - off, ranks), first, lax.rem(me + off, ranks)).wait_recv()

    start_share(True)
    neighbours = [
        pltpu.make_async_remote_copy(
            src_ref=place, dst_ref=sides.at[t], send_sem=side_send.at[t], recv_sem=side_recv.at[t],
            device_id={"gx": lax.rem(me + step, ranks)}, device_id_type=pl.DeviceIdType.MESH,
        )
        for t, step in enumerate((1, ranks - 1))
    ]
    for copy in neighbours:
        copy.start()

    def modes(freq):
        number = jnp.where(freq <= GRID // 2, freq, freq - GRID // 2)
        return number.astype(F32), jnp.where((freq == 0) | (freq == GRID // 2), 1.0 / GRID, 2.0 / GRID)

    x_modes, x_weights = modes(iota((GRID, GRID), 0))
    z_modes, z_weights = modes(iota((GRID, GRID), 1))
    flat_sq = x_modes * x_modes + z_modes * z_modes
    flat_weights = x_weights * z_weights

    def filter_one(q, carry):
        y_modes, y_weights = modes(jnp.full((GRID, GRID), me * kys + q, jnp.int32))
        mode_sq = flat_sq + y_modes * y_modes
        safe_sq = jnp.where(mode_sq > 0, mode_sq, 1.0)
        value = jnp.where(mode_sq > 0, RECIP_C * jnp.exp(-DAMP * safe_sq) / safe_sq, 0.0)
        green[q] = value * (flat_weights * y_weights)
        return carry

    lax.fori_loop(0, kys, filter_one, 0)

    for copy in neighbours:
        copy.wait()

    def spread_columns(e, rows):
        for c in range(3):
            cols[e, c] = jnp.broadcast_to(rows[c], (TILE, TILE)).T

    for e in range(blocks + 2 * HALO_BLK):
        for c in range(3):
            if e < HALO_BLK:
                row = blocks - HALO_BLK + e
                value = sides[0, c, row : row + 1, :] - (1.0 * blocks if c == 0 else 0.0)
            elif e < HALO_BLK + blocks:
                value = place[c, e - HALO_BLK : e - HALO_BLK + 1, :]
            else:
                row = e - HALO_BLK - blocks
                value = sides[1, c, row : row + 1, :] + (1.0 * blocks if c == 0 else 0.0)
            ext[e, c : c + 1, :] = value

    def position_columns(e, carry):
        spread_columns(e, [ext[e, c : c + 1, :] for c in range(3)])
        return carry

    lax.fori_loop(0, blocks + 2 * HALO_BLK, position_columns, 0)
    lag = iota((8, TILE), 1) - iota((8, TILE), 0)

    def tensors(index, carry):
        b, k = index // reach, index % reach
        near = jnp.float32(0.0)
        for s in range(reach):
            near = jnp.where((list_ref[b, s] == b + k) & (s < count_ref[b]), 1.0, near)
        home = [jnp.broadcast_to(ext[b + HALO_BLK, c : c + 1, :], (8, TILE)) for c in range(3)]
        hide = jnp.where(k == HALO_BLK, 0, 4 * TILE)
        for j in range(TILE // 8):
            rows = slice(8 * j, 8 * j + 8)
            r = [home[c] - cols[b + k, c, rows, :] for c in range(3)]
            inverse = lax.rsqrt(r[0] * r[0] + r[1] * r[1] + r[2] * r[2] + 1.0)
            live = jnp.where(lag != 8 * j + hide, near, 0.0)
            square = live * inverse * inverse
            tens[index, 0, rows, :] = PAIR_C * (square * inverse)
            weight = (3.0 * PAIR_C) ** 0.5 * (square * jnp.sqrt(inverse))
            for c in range(3):
                tens[index, 1 + c, rows, :] = weight * r[c]
        return carry

    lax.fori_loop(0, blocks * reach, tensors, 0)

    freq = me * kys + iota((kys, TILE), 0)
    sine_mode = freq > GRID // 2
    number = jnp.where(sine_mode, freq - GRID // 2, freq).astype(F32)
    lead_in = jnp.where(sine_mode, GRID // 4, 0).astype(F32)
    shifts = [turn(number * (1.0 * k)) for k in range(ORDER)]

    def slab_tables(d, carry):
        @pl.when(d > 0)
        def _():
            got_share(d, True)

        slab = lax.rem(me + away(d), ranks)
        values, slopes = spline_rows(info[slab, 4])
        for k in range(ORDER):
            xw[slab, k] = values[k]
            xw[slab, ORDER + k] = slopes[k]
        for t in range(2):
            values, slopes = spline_rows(info[slab, 2 * t + 1])
            for k in range(ORDER):
                wt[t, k] = values[k]
                wt[t, ORDER + k] = slopes[k]

        def block_tables(h, inner):
            for j in range(4):
                b = 4 * h + j

                def row(t, k):
                    return wt[t, k, pl.ds(b, 1), :]

                first = jnp.broadcast_to(info[slab, 0, pl.ds(b, 1), :], (kys, TILE))
                cosine, sine = turn(number * first - lead_in)
                for t in range(2):
                    real = combine([s[0] for s in shifts], [row(0, ORDER * t + k) for k in range(ORDER)])
                    imag = combine([s[1] for s in shifts], [row(0, ORDER * t + k) for k in range(ORDER)])
                    yq[slab * blocks + b, t] = cosine * real - sine * imag
                begin = info[slab, 2, pl.ds(b, 1), :].astype(jnp.int32)
                for i in range(GRID // 16):
                    gap = (iota((16, TILE), 0) + (16 * i - begin)) & (GRID - 1)
                    for t in range(2):
                        dense = jnp.zeros((16, TILE), F32)
                        for k in range(ORDER):
                            dense = jnp.where(gap == k, row(1, ORDER * t + k), dense)
                        high, rest = split(dense)
                        at = slice((2 * j + t) * TILE, (2 * j + t + 1) * TILE)
                        table[slab * halves + h, 16 * i : 16 * i + 16, at] = high
                        table[slab * halves + h, GRID + 16 * i : GRID + 16 * i + 16, at] = rest
            return inner

        lax.fori_loop(0, halves, block_tables, 0)
        return carry

    lax.fori_loop(0, ranks, slab_tables, 0)
    sent_share(True)

    def spread_half(slab, h):
        highs, lows = [], []
        for j in range(4):
            b = 4 * h + j
            y, dy = yq[slab * blocks + b, 0], yq[slab * blocks + b, 1]
            none = jnp.zeros((kys, TILE), F32)
            lead, tail = [none] * 8, [none] * 8
            for k in range(ORDER):
                lead[j + k] = vx[k, pl.ds(b, 1), :] * y + vx[ORDER + k, pl.ds(b, 1), :] * dy
                tail[j + k] = vx[2 * ORDER + k, pl.ds(b, 1), :] * y
            both = jnp.concatenate(
                [jnp.concatenate(lead, axis=0), jnp.concatenate(tail, axis=0)], axis=1
            )
            high, rest = split(both)
            highs.append(high)
            lows.append(rest)
        left = jnp.concatenate(
            [jnp.concatenate(highs, axis=1), jnp.concatenate(lows, axis=1)], axis=0
        )
        sums = lax.dot_general(
            left, table[slab * halves + h], CONTRACT_LANES, preferred_element_type=F32
        )
        count = 8 * kys
        at = pl.ds(pl.multiple_of((slab * planes + 4 * h) * kys, 4 * kys), count)
        grid[at, :] += sums[:count, :GRID] + sums[:count, GRID:] + sums[count:, :GRID]

    def gather_half(slab, h):
        count = 8 * kys
        at = pl.ds(pl.multiple_of((slab * planes + 4 * h) * kys, 4 * kys), count)
        sums = dot(jnp.concatenate([wide[at, :], low[at, :]], axis=0), table[slab * halves + h])
        for j in range(4):
            b = 4 * h + j
            one = two = three = 0.0
            for k in range(ORDER):
                rows = slice((j + k) * kys, (j + k + 1) * kys)
                more = slice(count + (j + k) * kys, count + (j + k + 1) * kys)
                value, slope = slice(2 * j * TILE, (2 * j + 1) * TILE), slice((2 * j + 1) * TILE, (2 * j + 2) * TILE)
                plain = sums[rows, value] + sums[more, value]
                tilted = sums[rows, slope] + sums[more, slope]
                x, dx = xw[slab, k, pl.ds(b, 1), :], xw[slab, ORDER + k, pl.ds(b, 1), :]
                one += dx * plain
                two += x * plain
                three += x * tilted
            y, dy = yq[slab * blocks + b, 0], yq[slab * blocks + b, 1]
            for c, term in enumerate((y * one, dy * two, y * three)):
                out_part[slab, c, pl.ds(b, 1), :] = jnp.sum(term, axis=0, keepdims=True)

    def sweep(it, carry):
        @pl.when(it > 0)
        def _():
            start_share(False)
            got_share(1, False)
            got_share(2, False)

        for e in range(blocks + 2 * HALO_BLK):
            slab = lax.rem(me + (ranks - 1 if e < HALO_BLK else 0 if e < HALO_BLK + blocks else 1), ranks)
            row = (e - HALO_BLK) % blocks
            spread_columns(e, [info[slab, FIELD0 + c, row : row + 1, :] for c in range(3)])

        def one_home(b, inner):
            def one_source(k, sums):
                sums = list(sums)
                for j in range(TILE // 8):
                    rows = slice(8 * j, 8 * j + 8)
                    v = [cols[b + k, c, rows, :] for c in range(3)]
                    w = [tens[b * reach + k, 1 + c, rows, :] for c in range(3)]
                    third = tens[b * reach + k, 0, rows, :]
                    along = w[0] * v[0] + w[1] * v[1] + w[2] * v[2]
                    for c in range(3):
                        sums[c] = sums[c] + third * v[c]
                        sums[3 + c] = sums[3 + c] + along * w[c]
                return tuple(sums)

            sums = lax.fori_loop(0, reach, one_source, (jnp.zeros((8, TILE), F32),) * 6)
            for c in range(3):
                pair[c, pl.ds(b, 1), :] = jnp.sum(sums[c] - sums[3 + c], axis=0, keepdims=True)
            return inner

        lax.fori_loop(0, blocks, one_home, 0)

        grid[...] = jnp.zeros_like(grid)

        def spread_slab(d, inner):
            @pl.when((it > 0) & (d > 2))
            def _():
                got_share(d, False)

            slab = lax.rem(me + away(d), ranks)
            v = [info[slab, FIELD0 + c] for c in range(3)]
            for k in range(ORDER):
                x, dx = xw[slab, k], xw[slab, ORDER + k]
                vx[k] = v[0] * dx
                vx[ORDER + k] = v[1] * x
                vx[2 * ORDER + k] = v[2] * x
            for h in range(halves):
                spread_half(slab, h)
            return inner

        lax.fori_loop(0, ranks, spread_slab, 0)

        size = GRID * kys
        edge = 2 * kys
        grid[size : size + edge, :] += grid[0:edge, :]
        grid[edge : 2 * edge, :] += grid[size + edge : size + 2 * edge, :]

        step = 2 * GRID
        for i in range(size // step):
            high, rest = split(grid[edge + i * step : edge + (i + 1) * step, :])
            sums = dot(jnp.concatenate([high, rest], axis=1), zin_ref[...])
            spec[i * step : (i + 1) * step, :] = sums[:, :GRID] + sums[:, GRID:]
        for q in range(0, kys, 2):
            pairs = [pl.ds(q, GRID, stride=kys), pl.ds(q + 1, GRID, stride=kys)]
            high, rest = split(jnp.concatenate([spec[s, :] for s in pairs], axis=1))
            line = dot(xin_ref[...], jnp.concatenate([high, rest, high], axis=0))
            line = line * jnp.concatenate([green[q], green[q + 1]], axis=1)
            high, rest = split(line)
            line = dot(xout_ref[...], jnp.concatenate([high, rest, high], axis=0))
            spec[pairs[0], :] = line[:, :GRID]
            spec[pairs[1], :] = line[:, GRID:]
        for i in range(size // step):
            high, rest = split(spec[i * step : (i + 1) * step, :])
            sums = dot(jnp.concatenate([high, rest], axis=1), zout_ref[...])
            high, rest = split(sums[:, :GRID] + sums[:, GRID:])
            rows = slice(edge + i * step, edge + (i + 1) * step)
            wide[rows, :] = jnp.concatenate([high, high], axis=1)
            low[rows, :] = jnp.concatenate([rest, jnp.zeros_like(rest)], axis=1)
        for ref in (wide, low):
            ref[0:edge, :] = ref[size : size + edge, :]
            ref[size + edge : size + 2 * edge, :] = ref[edge : 2 * edge, :]

        def gather_slab(t, inner):
            off = away(ranks - 1 - t)
            slab = lax.rem(me + off, ranks)
            for h in range(halves):
                gather_half(slab, h)

            @pl.when(t < ranks - 1)
            def _():
                fold(off, slab).start()

            return inner

        lax.fori_loop(0, ranks, gather_slab, 0)

        @pl.when(it > 0)
        def _():
            sent_share(False)

        def landed(i, inner):
            fold(i, lax.rem(me + i, ranks)).wait()
            return inner

        lax.fori_loop(1, ranks, landed, 0)
        for c in range(3):
            total = out_part[me, c]
            for i in range(1, ranks):
                total = total + in_part[i, c]
            following = pair[c] - total
            bases[it + 1, c] = following
            info[me, FIELD0 + c] = following / polar_ref[...]
        return carry

    lax.fori_loop(0, ITERS, sweep, 0)

    count = ITERS + 1
    place_of = {}
    part[...] = jnp.zeros_like(part)
    for i in range(count):
        for j in range(i, count):
            place_of[i, j] = place_of[j, i] = row = len(set(place_of.values()))
            value = 0.0
            for c in range(3):
                value += bases[i, c] * (bases[j, c] / polar_ref[...])
            part[row : row + 1, :] = jnp.sum(value, axis=0, keepdims=True)

    def tell(i, row):
        return pltpu.make_async_remote_copy(
            src_ref=part, dst_ref=slots.at[lax.rem(me + row, ranks)], send_sem=gram_send.at[i], recv_sem=gram_recv.at[i],
            device_id={"gx": lax.rem(me + i, ranks)}, device_id_type=pl.DeviceIdType.MESH,
        )

    def tell_start(i, carry):
        tell(i, 0).start()
        return carry

    def tell_wait(i, carry):
        tell(i, ranks - i).wait()
        return carry

    lax.fori_loop(1, ranks, tell_start, 0)
    slots[me] = part[...]
    lax.fori_loop(1, ranks, tell_wait, 0)
    sums = jnp.sum(jnp.sum(slots[...], axis=0), axis=1, keepdims=True)
    sums = jnp.broadcast_to(sums, (sums.shape[0], TILE))
    dipoles, residual = krylov(sums, place_of, count)
    for c in range(3):
        basis = [bases[i, c] for i in range(count)]
        first = combine(dipoles, [b / polar_ref[...] for b in basis])
        second = combine(residual, basis)
        for b in range(blocks):
            dip_ref[c : c + 1, lanes(b)] = first[b : b + 1, :]
            res_ref[c : c + 1, lanes(b)] = second[b : b + 1, :]


def krylov(sums, place, count):
    def inner(x, y):
        value = None
        for i in range(count):
            for j in range(count):
                if x[i] is not None and y[j] is not None:
                    row = place[i, j]
                    term = x[i] * y[j] * sums[row : row + 1]
                    value = term if value is None else value + term
        return value

    none = [None] * (count - 1)
    residual = [jnp.ones((1, TILE), F32)] + none
    direction = list(residual)
    dipoles = [None] * count
    rz_now = inner(residual, residual)
    for sweep in range(ITERS):
        image = scaled(-1.0, direction, [None] + direction[:-1])
        step = rz_now / inner(direction, image)
        dipoles = scaled(step, dipoles, direction)
        residual = scaled(-step, residual, image)
        if sweep + 1 < ITERS:
            rz_next = inner(residual, residual)
            direction = scaled(rz_next / rz_now, residual, direction)
            rz_now = rz_next
    return dipoles, residual


def fast_shapes(ranks, blocks):
    kys = GRID // ranks
    ext_blocks = blocks + 2 * HALO_BLK
    rows = (GRID + 4) * kys
    dma = pltpu.SemaphoreType.DMA
    tile = (blocks, TILE)
    buffers = [
        ((2, blocks * TILE, GRID), F32),
        ((ranks, 8) + tile, F32),
        ((ranks * blocks // 4, 2 * GRID, 8 * TILE), BF16),
        ((ranks * blocks, 2, kys, TILE), F32),
        ((ranks, 2 * ORDER) + tile, F32),
        ((2, 2 * ORDER) + tile, F32),
        ((3 * ORDER,) + tile, F32),
        ((rows, GRID), F32),
        ((GRID * kys, GRID), F32),
        ((rows, 2 * GRID), BF16),
        ((rows, 2 * GRID), BF16),
        ((kys, GRID, GRID), F32),
        ((blocks * (2 * HALO_BLK + 1), 4, TILE, TILE), F32),
        ((ext_blocks, 3, TILE, TILE), F32),
        ((3,) + tile, F32),
        ((2, 3) + tile, F32),
        ((ext_blocks, 8, TILE), F32),
        ((ITERS + 1, 3) + tile, F32),
        ((3,) + tile, F32),
        ((ranks, 3) + tile, F32),
        ((ranks, 3) + tile, F32),
        ((16, TILE), F32),
        ((ranks, 16, TILE), F32),
    ]
    sems = [dma((2,))] + [dma((ranks,))] * 4 + [dma((2,))] * 2 + [dma((ranks,))] * 2
    return buffers, sems


def fits_fast(ranks, blocks):
    if blocks != 8 or GRID % ranks or GRID // ranks != blocks:
        return False
    buffers, _ = fast_shapes(ranks, blocks)
    return sum(int(np.prod(s)) * np.dtype(t).itemsize for s, t in buffers) < 50 * 1024 * 1024


def halves_of(x):
    high = x.astype(BF16)
    return high, (x - high.astype(np.float32)).astype(BF16)


def fast_device(positions, field, inv_polar, x_spline, yz_spline, tile_list, tile_count):
    ranks = lax.axis_size("gx")
    atoms_here = positions.shape[1]
    blocks = atoms_here // TILE
    line = np.arange(GRID)
    center = (line[None, :] - line[:, None] + GRID // 2) % GRID - GRID // 2
    center = np.concatenate([center, np.eye(GRID)], axis=0)
    center = np.concatenate([center.astype(np.float32).astype(BF16)] * 3, axis=1)
    rows = fixed_rows(line)

    def along_z(m):
        high, rest = halves_of(np.ascontiguousarray(m))
        return np.concatenate(
            [np.concatenate([high, rest], axis=1), np.concatenate([high, np.zeros_like(rest)], axis=1)], axis=0
        )

    def along_x(m):
        high, rest = halves_of(np.ascontiguousarray(m))
        return np.concatenate([high, high, rest], axis=1)

    constants = [center, along_z(rows.T), along_z(rows), along_x(rows), along_x(rows.T)]
    buffers, sems = fast_shapes(ranks, blocks)
    smem = pl.BlockSpec(memory_space=pltpu.SMEM)
    return pl.pallas_call(
        functools.partial(fast_kernel, ranks),
        in_specs=[VMEM] * 4 + [smem] * 2 + [VMEM] * 5 + [pl.BlockSpec(memory_space=pl.ANY)],
        out_specs=[VMEM] * 2,
        out_shape=[jax.ShapeDtypeStruct(positions.shape, F32)] * 2,
        scratch_shapes=[pltpu.VMEM(s, t) for s, t in buffers] + sems,
        compiler_params=pltpu.CompilerParams(
            vmem_limit_bytes=62 * 1024 * 1024, collective_id=2, has_side_effects=True
        ),
        name="induced",
    )(
        positions, field, inv_polar.reshape(blocks, TILE), x_spline.transpose(1, 0, 2),
        tile_list, tile_count, *[jnp.asarray(c) for c in constants], yz_spline,
    )


def solution(mesh):
    placed = (
        P(None, ("rep", "gx")),
        P(None, ("rep", "gx")),
        P(("rep", "gx")),
        P(None, None, ("rep", "gx")),
        P(None, ("rep", "gx"), None),
        P(("rep", "gx"), None),
        P(("rep", "gx")),
    )
    ranks = mesh.shape["gx"]

    def choose(*arrays):
        device = fast_device if fits_fast(ranks, arrays[0].shape[1] // TILE) else per_device
        return device(*arrays)

    return jax.shard_map(
        choose,
        mesh=mesh,
        in_specs=placed,
        out_specs=(P(None, ("rep", "gx")), P(None, ("rep", "gx"))),
        check_vma=False,
    )
```

```python
import jax
import jax.numpy as jnp
from jax import lax
from jax.experimental import pallas as pl
from jax.experimental.pallas import tpu as pltpu
from jax.sharding import PartitionSpec as P
import functools
import numpy as np

GRID = 128
ORDER = 5
TILE = 128
HALO_BLK = 3
ITERS = 3


PAIR_C = 0.025
RECIP_C = 8192.0
DAMP = 0.0008
EXACT = lax.Precision.HIGHEST


def mode_of(freq, size):
    half_size = size // 2
    mode_num = jnp.where(freq <= half_size, freq, freq - half_size)
    weight = jnp.where((freq == 0) | (freq == half_size), 1.0 / size, 2.0 / size)
    return (mode_num.astype(jnp.float32), weight.astype(jnp.float32))


def basis_rows(size, points):
    freq = jnp.arange(size, dtype=jnp.int32)
    half_size = size // 2
    mode_num = jnp.where(freq <= half_size, freq, freq - half_size)
    phase = mode_num[:, None] * points[None, :] % size
    angle = phase.astype(jnp.float32) * (2.0 * jnp.pi / size)
    return jnp.where((freq <= half_size)[:, None], jnp.cos(angle), jnp.sin(angle))


def kernel_block(x_modes, x_weights, y_modes, y_weights, z_modes, z_weights):
    mode_sq = (
        x_modes[:, None, None] * x_modes[:, None, None]
        + y_modes[None, :, None] * y_modes[None, :, None]
        + z_modes[None, None, :] * z_modes[None, None, :]
    )
    safe_sq = jnp.where(mode_sq > 0, mode_sq, 1.0)
    green = jnp.where(mode_sq > 0, RECIP_C * jnp.exp(-DAMP * safe_sq) / safe_sq, 0.0)
    return green * x_weights[:, None, None] * y_weights[None, :, None] * z_weights[None, None, :]


F32 = jnp.float32
BF16 = jnp.bfloat16
VMEM = pl.BlockSpec(memory_space=pltpu.VMEM)


def split(x):
    high = x.astype(BF16)
    return high, (x - high.astype(F32)).astype(BF16)


def dot(a, b):
    return jnp.dot(a, b, preferred_element_type=F32)


def params(**more):
    return pltpu.CompilerParams(vmem_limit_bytes=56 * 1024 * 1024, **more)


def prep_kernel(yz_ref, rows_ref, yft_ref, zf_ref, zft_ref):
    rows = jnp.concatenate(split(rows_ref[...]), axis=0)

    def transformed(t):
        high, low = split(jnp.concatenate([yz_ref[t], yz_ref[t + 1]], axis=0))
        contract = (((1,), (1,)), ((), ()))
        wide = lax.dot_general(rows, high, contract, preferred_element_type=F32)
        more = lax.dot_general(rows[:GRID], low, contract, preferred_element_type=F32)
        return wide[:GRID] + wide[GRID:] + more

    lines = transformed(0)
    yft_ref[0, 0] = lines[:, :TILE]
    yft_ref[0, 1] = lines[:, TILE:]
    lines = transformed(2)
    zft_ref[0] = jnp.concatenate(split(lines), axis=0)
    zf_ref[0] = jnp.concatenate(split(lines.T), axis=1)


def prepare(yz_spline, rows, blocks):
    return pl.pallas_call(
        prep_kernel,
        grid=(blocks,),
        in_specs=[
            pl.BlockSpec((4, TILE, GRID), lambda b: (0, b, 0)),
            pl.BlockSpec((GRID, GRID), lambda b: (0, 0)),
        ],
        out_specs=[
            pl.BlockSpec((1, 2, GRID, TILE), lambda b: (b, 0, 0, 0)),
            pl.BlockSpec((1, 2 * TILE, 2 * GRID), lambda b: (b, 0, 0)),
            pl.BlockSpec((1, 2 * GRID, 2 * TILE), lambda b: (b, 0, 0)),
        ],
        out_shape=[
            jax.ShapeDtypeStruct((blocks, 2, GRID, TILE), F32),
            jax.ShapeDtypeStruct((blocks, 2 * TILE, 2 * GRID), BF16),
            jax.ShapeDtypeStruct((blocks, 2 * GRID, 2 * TILE), BF16),
        ],
        compiler_params=params(),
        name="prep",
    )(yz_spline, rows)


def spread_kernel(planes, ky_count, pv_ref, xs_ref, yft_ref, zf_ref, out_ref):
    blocks = pv_ref.shape[0]
    ranks = out_ref.shape[0]
    out_ref[...] = jnp.zeros_like(out_ref)

    def one_block(b, carry):
        base = b * planes // blocks
        y, dy = yft_ref[b, 0], yft_ref[b, 1]
        v0, v1, v2 = (pv_ref[b, 3 + c : 4 + c, :] for c in range(3))
        highs, lows = [], []
        for k in range(ORDER):
            x, dx = xs_ref[b, k : k + 1, :], xs_ref[b, ORDER + k : ORDER + k + 1, :]
            lead = (v0 * dx) * y + (v1 * x) * dy
            high, low = split(jnp.concatenate([lead, (v2 * x) * y], axis=1))
            highs.append(high)
            lows.append(low)
        weights = zf_ref[b]
        wide = dot(jnp.concatenate(highs, axis=0), weights)
        total = (
            wide[:, :GRID] + wide[:, GRID:] + dot(jnp.concatenate(lows, axis=0), weights[:, :GRID])
        )
        for k in range(ORDER):
            part = total[k * GRID : (k + 1) * GRID].reshape(ranks, ky_count, GRID)
            out_ref[:, base + k, :ky_count, :] += part
        return carry

    lax.fori_loop(0, blocks, one_block, 0)


def gather_kernel(
    planes, ky_count, ret_ref, xs_ref, yft_ref, zft_ref, pair_ref, pv_ref, polar_ref,
    next_ref, pv_next_ref, wide_ref, low_ref,
):
    blocks = xs_ref.shape[0]
    extent = ret_ref.shape[1]
    for p in range(extent):
        high, low = split(ret_ref[:, p, :ky_count, :].reshape(GRID, GRID))
        wide_ref[p] = jnp.concatenate([high, high], axis=1)
        low_ref[p] = low

    def one_block(b, carry):
        base = b * planes // blocks
        weights = zft_ref[b]
        wide = wide_ref[pl.ds(base, ORDER)].reshape(ORDER * GRID, 2 * GRID)
        low = low_ref[pl.ds(base, ORDER)].reshape(ORDER * GRID, GRID)
        sums = dot(wide, weights) + dot(low, weights[:GRID])
        one = two = three = 0.0
        for k in range(ORDER):
            x, dx = xs_ref[b, k : k + 1, :], xs_ref[b, ORDER + k : ORDER + k + 1, :]
            plain = sums[k * GRID : (k + 1) * GRID, :TILE]
            one += dx * plain
            two += x * plain
            three += x * sums[k * GRID : (k + 1) * GRID, TILE:]
        y, dy = yft_ref[b, 0], yft_ref[b, 1]
        far = jnp.concatenate(
            [jnp.sum(t, axis=0, keepdims=True) for t in (y * one, dy * two, y * three)], axis=0
        )
        following = pair_ref[b] - far
        next_ref[b] = following
        pv_next_ref[b, 0:3] = pv_ref[b, 0:3]
        pv_next_ref[b, 3:6] = following / polar_ref[b]
        pv_next_ref[b, 6:8] = jnp.zeros((2, TILE), F32)
        return carry

    lax.fori_loop(0, blocks, one_block, 0)


def pair_sum(near_ref, pv_ref, before_ref, after_ref, out_ref, ext_ref, col_ref):
    blocks = pv_ref.shape[0]
    reach = 2 * HALO_BLK + 1
    first_row = lax.broadcasted_iota(jnp.int32, (HALO_BLK, 8, TILE), 1) == 0
    ext_ref[:HALO_BLK] = before_ref[...] + jnp.where(first_row, -1.0 * blocks, 0.0)
    ext_ref[HALO_BLK : HALO_BLK + blocks] = pv_ref[...]
    ext_ref[HALO_BLK + blocks :] = after_ref[...] + jnp.where(first_row, 1.0 * blocks, 0.0)
    lag = lax.broadcasted_iota(jnp.int32, (8, TILE), 1) - lax.broadcasted_iota(
        jnp.int32, (8, TILE), 0
    )

    def spread_columns(e, carry):
        for c in range(6):
            col_ref[e, c] = jnp.broadcast_to(ext_ref[e, c : c + 1, :], (TILE, TILE)).T
        return carry

    lax.fori_loop(0, blocks + 2 * HALO_BLK, spread_columns, 0)

    def one_home(b, carry):
        home = [jnp.broadcast_to(pv_ref[b, c : c + 1, :], (8, TILE)) for c in range(3)]

        def one_source(k, sums):
            shift = jnp.where(k == HALO_BLK, 0, 4 * TILE)
            direct = [jnp.zeros((8, TILE), F32) for c in range(3)]
            tilted = [jnp.zeros((8, TILE), F32) for c in range(3)]
            for j in range(TILE // 8):
                rows = slice(8 * j, 8 * j + 8)
                r = [home[c] - col_ref[b + k, c, rows, :] for c in range(3)]
                v = [col_ref[b + k, 3 + c, rows, :] for c in range(3)]
                inverse = lax.rsqrt(r[0] * r[0] + r[1] * r[1] + r[2] * r[2] + 1.0)
                inverse = jnp.where(lag != 8 * j + shift, inverse, 0.0)
                square = inverse * inverse
                third = square * inverse
                weight = third * square * (r[0] * v[0] + r[1] * v[1] + r[2] * v[2])
                for c in range(3):
                    direct[c] += third * v[c]
                    tilted[c] += weight * r[c]
            near = near_ref[b * reach + k]
            return tuple(
                sums[c] + near * (direct[c] - 3.0 * tilted[c]) for c in range(3)
            )

        sums = lax.fori_loop(0, reach, one_source, (jnp.zeros((8, TILE), F32),) * 3)
        out_ref[b] = PAIR_C * jnp.concatenate(
            [jnp.sum(t, axis=0, keepdims=True) for t in sums], axis=0
        )
        return carry

    lax.fori_loop(0, blocks, one_home, 0)


def greet(ranks, me):
    barrier = pltpu.get_barrier_semaphore()

    def signal(d, carry):
        pl.semaphore_signal(
            barrier,
            inc=1,
            device_id={"gx": lax.rem(me + d, ranks)},
            device_id_type=pl.DeviceIdType.MESH,
        )
        return carry

    lax.fori_loop(1, ranks, signal, 0)
    pl.semaphore_wait(barrier, ranks - 1)


def exchange(ranks, me, source, target, local_sem, send_sem, recv_sem):
    def copy(d, slot):
        peer = lax.rem(me + d, ranks)
        return pltpu.make_async_remote_copy(
            src_ref=source(peer),
            dst_ref=target(slot),
            send_sem=send_sem.at[d],
            recv_sem=recv_sem.at[d],
            device_id={"gx": peer},
            device_id_type=pl.DeviceIdType.MESH,
        )

    def start(d, carry):
        copy(d, me).start()
        return carry

    def finish(d, carry):
        copy(d, lax.rem(me - d + ranks, ranks)).wait()
        return carry

    lax.fori_loop(1, ranks, start, 0)
    own = pltpu.make_async_copy(source(me), target(me), local_sem)
    own.start()

    def wait():
        own.wait()
        lax.fori_loop(1, ranks, finish, 0)

    return wait


def middle_kernel(
    ranks, ky_count, near_ref, spec_ref, pv_ref, green_ref, across_ref, back_ref,
    ret_ref, pair_ref,
    before_ref, after_ref, ext_ref, col_ref, recv_ref, done_ref, local_sems, send1, recv1, send2, recv2, halo_send, halo_recv,
):
    me = lax.axis_index("gx")
    blocks = pv_ref.shape[0]
    extent = spec_ref.shape[1]
    rows = ranks * extent
    greet(ranks, me)
    halos = []
    for t, (piece, into, step) in enumerate(
        (
            (pv_ref.at[pl.ds(blocks - HALO_BLK, HALO_BLK)], before_ref, 1),
            (pv_ref.at[pl.ds(0, HALO_BLK)], after_ref, ranks - 1),
        )
    ):
        halos.append(
            pltpu.make_async_remote_copy(
                src_ref=piece,
                dst_ref=into,
                send_sem=halo_send.at[t],
                recv_sem=halo_recv.at[t],
                device_id={"gx": lax.rem(me + step, ranks)},
                device_id_type=pl.DeviceIdType.MESH,
            )
        )
        halos[-1].start()
    wait = exchange(
        ranks, me, lambda d: spec_ref.at[d], lambda d: recv_ref.at[d], local_sems.at[0], send1, recv1
    )
    across_high, across_low = split(across_ref[...])
    back_high, back_low = split(back_ref[...])
    wait()
    lines_in = recv_ref.reshape(rows * 8, GRID)
    lines_out = done_ref.reshape(rows * 8, GRID)
    for q in range(ky_count):
        high, low = split(lines_in[pl.ds(q, rows, stride=8), :])
        wide = dot(across_high, jnp.concatenate([high, low], axis=1))
        line = wide[:, :GRID] + wide[:, GRID:] + dot(across_low, high)
        high, low = split(line * green_ref[q])
        wide = dot(back_high, jnp.concatenate([high, low], axis=1))
        lines_out[pl.ds(q, rows, stride=8), :] = (
            wide[:, :GRID] + wide[:, GRID:] + dot(back_low, high)
        )
    wait = exchange(
        ranks, me, lambda d: done_ref.at[d], lambda d: ret_ref.at[d], local_sems.at[1], send2, recv2
    )
    for halo in halos:
        halo.wait()
    pair_sum(near_ref, pv_ref, before_ref, after_ref, pair_ref, ext_ref, col_ref)
    wait()


def middle(near, spec, pv, green, across, back, ranks, ky_count):
    dma = pltpu.SemaphoreType.DMA
    blocks = pv.shape[0]
    halo = pltpu.VMEM((HALO_BLK, 8, TILE), F32)
    return pl.pallas_call(
        functools.partial(middle_kernel, ranks, ky_count),
        in_specs=[pl.BlockSpec(memory_space=pltpu.SMEM)] + [VMEM] * 5,
        out_specs=[VMEM] * 2,
        out_shape=[
            jax.ShapeDtypeStruct(spec.shape, F32),
            jax.ShapeDtypeStruct((blocks, 3, TILE), F32),
        ],
        scratch_shapes=[
            halo,
            halo,
            pltpu.VMEM((blocks + 2 * HALO_BLK, 8, TILE), F32),
            pltpu.VMEM((blocks + 2 * HALO_BLK, 6, TILE, TILE), F32),
            pltpu.VMEM(spec.shape, F32),
            pltpu.VMEM(spec.shape, F32),
            dma((2,)), dma((ranks,)), dma((ranks,)), dma((ranks,)), dma((ranks,)),
            dma((2,)), dma((2,)),
        ],
        compiler_params=params(collective_id=0, has_side_effects=True),
        name="middle",
    )(near, spec, pv, green, across, back)


def combine(weights, parts):
    terms = [w * p for w, p in zip(weights, parts) if w is not None]
    return functools.reduce(jnp.add, terms)


def scaled(a, x, y):
    pairs = zip(x, y)
    return [p if q is None else (a * q if p is None else p + a * q) for p, q in pairs]


def solve_kernel(
    ranks, b0_ref, b1_ref, b2_ref, b3_ref, polar_ref,
    dipoles_ref, residual_ref, part_ref, slots, local_sem, send_sem, recv_sem,
):
    me = lax.axis_index("gx")
    bases = [ref[...] for ref in (b0_ref, b1_ref, b2_ref, b3_ref)]
    soft = [b / polar_ref[...] for b in bases]
    count = ITERS + 1
    place = {}
    part_ref[...] = jnp.zeros_like(part_ref)
    for i in range(count):
        for j in range(i, count):
            place[i, j] = place[j, i] = row = len(set(place.values()))
            part_ref[row : row + 1] = jnp.sum(
                jnp.sum(bases[i] * soft[j], axis=0), axis=0, keepdims=True
            )
    greet(ranks, me)
    wait = exchange(
        ranks, me, lambda d: part_ref, lambda d: slots.at[d], local_sem.at[0], send_sem, recv_sem
    )
    wait()
    sums = jnp.sum(jnp.sum(slots[...], axis=0), axis=1, keepdims=True)
    sums = jnp.broadcast_to(sums, (sums.shape[0], TILE))

    def inner(x, y):
        value = None
        for i in range(count):
            for j in range(count):
                if x[i] is not None and y[j] is not None:
                    row = place[i, j]
                    term = x[i] * y[j] * sums[row : row + 1]
                    value = term if value is None else value + term
        return value

    none = [None] * (count - 1)
    residual = [jnp.ones((1, TILE), F32)] + none
    direction = list(residual)
    dipoles = [None] * count
    rz_now = inner(residual, residual)
    for sweep in range(ITERS):
        image = scaled(-1.0, direction, [None] + direction[:-1])
        step = rz_now / inner(direction, image)
        dipoles = scaled(step, dipoles, direction)
        residual = scaled(-step, residual, image)
        if sweep + 1 < ITERS:
            rz_next = inner(residual, residual)
            direction = scaled(rz_next / rz_now, residual, direction)
            rz_now = rz_next
    dipoles_ref[...] = combine(dipoles, soft)
    residual_ref[...] = combine(residual, bases)


def solve(bases, polar, ranks):
    dma = pltpu.SemaphoreType.DMA
    shape = bases[0].shape
    return pl.pallas_call(
        functools.partial(solve_kernel, ranks),
        in_specs=[VMEM] * 5,
        out_specs=[VMEM] * 2,
        out_shape=[jax.ShapeDtypeStruct(shape, F32)] * 2,
        scratch_shapes=[
            pltpu.VMEM((16, TILE), F32), pltpu.VMEM((ranks, 16, TILE), F32),
            dma((1,)), dma((ranks,)), dma((ranks,)),
        ],
        compiler_params=params(collective_id=1, has_side_effects=True),
        name="solve",
    )(*bases, polar)


def fixed_rows(points):
    half_size = GRID // 2
    freq = np.arange(GRID)
    mode_num = np.where(freq <= half_size, freq, freq - half_size)
    angle = (mode_num[:, None] * points[None, :] % GRID) * (2.0 * np.pi / GRID)
    return np.where((freq <= half_size)[:, None], np.cos(angle), np.sin(angle)).astype(np.float32)


def per_device(positions, field, inv_polar, x_spline, yz_spline, tile_list, tile_count):
    ranks = lax.axis_size("gx")
    rank_index = lax.axis_index("gx")
    atoms_here = positions.shape[1]
    planes = GRID // ranks
    extent = planes + 4
    blocks = atoms_here // TILE
    reach = 2 * HALO_BLK + 1
    ky_count = GRID // ranks

    def blocked(x):
        return x.reshape(-1, blocks, TILE).transpose(1, 0, 2)

    all_freq = jnp.arange(GRID, dtype=jnp.int32)
    fourier_rows = jnp.asarray(fixed_rows(np.arange(GRID)))
    ky_freq = rank_index * ky_count + jnp.arange(ky_count, dtype=jnp.int32)
    full_modes, full_weights = mode_of(all_freq, GRID)
    ky_modes, ky_weights = mode_of(ky_freq, GRID)
    green = kernel_block(ky_modes, ky_weights, full_modes, full_weights, full_modes, full_weights)
    source_rows = np.arange(ranks * extent)
    points = (source_rows // extent * planes - 2 + source_rows % extent) % GRID
    across = fixed_rows(points)
    back = jnp.asarray(np.ascontiguousarray(across.T))
    across = jnp.asarray(across)
    slots = jnp.arange(tile_list.shape[1], dtype=jnp.int32)
    wanted = jnp.arange(blocks, dtype=jnp.int32)[:, None] + jnp.arange(reach, dtype=jnp.int32)
    live = (slots[None, :] < tile_count[:, None])[:, :, None]
    near = jnp.any((tile_list[:, :, None] == wanted[:, None, :]) & live, axis=1)
    near = near.astype(F32).reshape(-1)
    yft, zf, zft = prepare(yz_spline, fourier_rows, blocks)
    xs = blocked(x_spline.reshape(2 * ORDER, atoms_here))
    pos = blocked(positions)
    polar = inv_polar.reshape(blocks, 1, TILE)
    spec_shape = jax.ShapeDtypeStruct((ranks, extent, 8, GRID), F32)
    rows_shape = jax.ShapeDtypeStruct((blocks, 3, TILE), F32)

    def advance(pv):
        spec = pl.pallas_call(
            functools.partial(spread_kernel, planes, ky_count),
            in_specs=[VMEM] * 4,
            out_specs=VMEM,
            out_shape=spec_shape,
            compiler_params=params(),
            name="spread",
        )(pv, xs, yft, zf)
        ret, pair = middle(near, spec, pv, green, across, back, ranks, ky_count)
        return pl.pallas_call(
            functools.partial(gather_kernel, planes, ky_count),
            in_specs=[VMEM] * 7,
            out_specs=[VMEM] * 2,
            out_shape=[rows_shape, jax.ShapeDtypeStruct((blocks, 8, TILE), F32)],
            scratch_shapes=[
                pltpu.VMEM((extent, GRID, 2 * GRID), BF16),
                pltpu.VMEM((extent, GRID, GRID), BF16),
            ],
            compiler_params=params(),
            name="gather",
        )(ret, xs, yft, zft, pair, pv, polar)

    bases = [blocked(field)]
    pv = jnp.concatenate([pos, bases[0] / polar, jnp.zeros((blocks, 2, TILE), F32)], axis=1)
    for sweep in range(ITERS):
        following, pv = advance(pv)
        bases.append(following)
    dipoles, residual = solve(bases, polar, ranks)

    def flat(x):
        return x.transpose(1, 0, 2).reshape(3, atoms_here)

    return flat(dipoles), flat(residual)


FIELD0 = 5


def spline_rows(u):
    v = 1.0 - u

    def inner(p):
        return ((((-4.0 * p + 4.0) * p + 6.0) * p + 4.0) * p + 1.0) * (1.0 / 24.0)

    def slope(p):
        return (((-4.0 * p + 3.0) * p + 3.0) * p + 1.0) * (1.0 / 6.0)

    middle_value = ((((6.0 * u - 12.0) * u - 6.0) * u + 12.0) * u + 11.0) * (1.0 / 24.0)
    middle_slope = (((2.0 * u - 3.0) * u - 1.0) * u + 1.0) * 0.5
    values = [v * v * v * v * (1.0 / 24.0), inner(v), middle_value, inner(u), u * u * u * u * (1.0 / 24.0)]
    slopes = [v * v * v * (-1.0 / 6.0), -slope(v), middle_slope, slope(u), u * u * u * (1.0 / 6.0)]
    return values, slopes


def turn(steps):
    wrapped = steps - GRID * jnp.floor(steps * (1.0 / GRID) + 0.5)
    half = wrapped * (np.pi / GRID)
    square = half * half
    sine = -1.0 / 39916800.0
    for c in (1.0 / 362880.0, -1.0 / 5040.0, 1.0 / 120.0, -1.0 / 6.0, 1.0):
        sine = sine * square + c
    sine = sine * half
    cosine = 1.0 / 479001600.0
    for c in (-1.0 / 3628800.0, 1.0 / 40320.0, -1.0 / 720.0, 1.0 / 24.0, -0.5, 1.0):
        cosine = cosine * square + c
    return 1.0 - 2.0 * sine * sine, 2.0 * sine * cosine


def total_of(x):
    return jnp.sum(jnp.sum(x, axis=0, keepdims=True), axis=1, keepdims=True)


def pick(rows, index):
    return jnp.take_along_axis(rows, index, axis=0, mode="promise_in_bounds")


def iota(shape, dim):
    return lax.broadcasted_iota(jnp.int32, shape, dim)


CONTRACT_LANES = (((1,), (1,)), ((), ()))


def fast_kernel(
    ranks, pos_ref, field_ref, polar_ref, xs_ref, list_ref, count_ref,
    center_ref, eye_ref, zin_ref, zout_ref, xin_ref, xout_ref, yz_ref,
    dip_ref, res_ref,
    lines, info, table, flipped, yq, xw, wt, wz, vx, mix, hold, grid, spec, wide, low, green, tens, cols, place, sides, ext,
    bases, pair, out_part, in_part, part, slots, energy,
    local_sem, ag_send, ag_recv, rs_send, rs_recv, side_send, side_recv, gram_send, gram_recv,
):
    me = lax.axis_index("gx")
    blocks = polar_ref.shape[0]
    planes = GRID // ranks
    kys = GRID // ranks
    halves = blocks // 4
    reach = 2 * HALO_BLK + 1

    def lanes(b):
        return slice(b * TILE, (b + 1) * TILE)

    loads = [
        pltpu.make_async_copy(yz_ref.at[2 * t], lines.at[t], local_sem.at[t]) for t in range(2)
    ]
    for load in loads:
        load.start()

    barrier = pltpu.get_barrier_semaphore()

    def greet_one(d, carry):
        pl.semaphore_signal(
            barrier, inc=1, device_id={"gx": lax.rem(me + d, ranks)}, device_id_type=pl.DeviceIdType.MESH
        )
        return carry

    lax.fori_loop(1, ranks, greet_one, 0)

    for c in range(3):
        for b in range(blocks):
            place[c, b : b + 1, :] = pos_ref[c : c + 1, lanes(b)]
    with jax.named_scope("greet_wait"):
        pl.semaphore_wait(barrier, ranks - 1)
    neighbours = [
        pltpu.make_async_remote_copy(
            src_ref=place, dst_ref=sides.at[t], send_sem=side_send.at[t], recv_sem=side_recv.at[t],
            device_id={"gx": lax.rem(me + step, ranks)}, device_id_type=pl.DeviceIdType.MESH,
        )
        for t, step in enumerate((1, ranks - 1))
    ]
    for copy in neighbours:
        copy.start()
    for c in range(3):
        for b in range(blocks):
            bases[0, c, b : b + 1, :] = field_ref[c : c + 1, lanes(b)]
    for c in range(3):
        info[me, FIELD0 + c] = bases[0, c] / polar_ref[...]
    offset = -1.5
    for k in range(1, ORDER):
        offset = offset + (1.0 * k) * xs_ref[k, 0:1, :]
    for b in range(blocks):
        info[me, 4, b : b + 1, :] = offset[:, lanes(b)]
    with jax.named_scope("yz_wait"):
        for load in loads:
            load.wait()
    marks = iota((GRID, TILE), 0).astype(F32)
    with jax.named_scope("moments"):
        for t in range(2):
            for b in range(blocks):
                line = lines[t, lanes(b), :]
                high = line.astype(BF16)
                rest = line - high.astype(F32)
                mid, tail = split(rest)
                moment = lax.dot_general(
                    center_ref[...], jnp.concatenate([high, mid, tail], axis=1), CONTRACT_LANES,
                    preferred_element_type=F32,
                )
                moment, weight = moment[:GRID], moment[GRID:]
                best = jnp.max(
                    jnp.where((jnp.abs(moment) < 0.5001) & (weight > 0.25), marks, -1.0), axis=0, keepdims=True
                )
                shift = jnp.sum(jnp.where(marks == best, moment, 0.0), axis=0, keepdims=True)
                start = best - 2.0
                info[me, 2 * t, b : b + 1, :] = jnp.where(start < 0, start + GRID, start)
                info[me, 2 * t + 1, b : b + 1, :] = shift + 0.5

    def share(i, first, source=None):
        owner = me if source is None else source
        span = info.at[owner] if first else info.at[owner, pl.ds(FIELD0, 3)]
        return pltpu.make_async_remote_copy(
            src_ref=span, dst_ref=span, send_sem=ag_send.at[i], recv_sem=ag_recv.at[i],
            device_id={"gx": lax.rem(me + i, ranks)}, device_id_type=pl.DeviceIdType.MESH,
        )

    def fold(i, slab):
        return pltpu.make_async_remote_copy(
            src_ref=out_part.at[slab], dst_ref=in_part.at[i], send_sem=rs_send.at[i], recv_sem=rs_recv.at[i],
            device_id={"gx": slab}, device_id_type=pl.DeviceIdType.MESH,
        )

    def away(d):
        step = (d + 1) // 2
        return lax.rem(jnp.where(d % 2 == 1, step, ranks - step), ranks)

    def start_share(first):
        def one(d, carry):
            share(away(d), first).start()
            return carry

        lax.fori_loop(1, ranks, one, 0)

    def sent_share(first):
        def one(i, carry):
            share(i, first).wait_send()
            return carry

        lax.fori_loop(1, ranks, one, 0)

    def got_share(d, first):
        off = away(d)
        share(lax.rem(ranks - off, ranks), first, lax.rem(me + off, ranks)).wait_recv()

    start_share(True)
    def modes(freq):
        number = jnp.where(freq <= GRID // 2, freq, freq - GRID // 2)
        return number.astype(F32), jnp.where((freq == 0) | (freq == GRID // 2), 1.0 / GRID, 2.0 / GRID)

    x_modes, x_weights = modes(iota((GRID, GRID), 0))
    z_modes, z_weights = modes(iota((GRID, GRID), 1))
    flat_sq = x_modes * x_modes + z_modes * z_modes
    flat_weights = x_weights * z_weights

    def filter_one(q, carry):
        y_modes, y_weights = modes(jnp.full((GRID, GRID), me * kys + q, jnp.int32))
        mode_sq = flat_sq + y_modes * y_modes
        safe_sq = jnp.where(mode_sq > 0, mode_sq, 1.0)
        value = jnp.where(mode_sq > 0, RECIP_C * jnp.exp(-DAMP * safe_sq) / safe_sq, 0.0)
        green[q] = value * (flat_weights * y_weights)
        return carry

    with jax.named_scope("filter"):
        lax.fori_loop(0, kys, filter_one, 0)

    with jax.named_scope("side_wait"):
        for copy in neighbours:
            copy.wait()

    def spread_columns(e, rows):
        for c in range(3):
            cols[e, c] = jnp.broadcast_to(rows[c], (TILE, TILE)).T

    for e in range(blocks + 2 * HALO_BLK):
        for c in range(3):
            if e < HALO_BLK:
                row = blocks - HALO_BLK + e
                value = sides[0, c, row : row + 1, :] - (1.0 * blocks if c == 0 else 0.0)
            elif e < HALO_BLK + blocks:
                value = place[c, e - HALO_BLK : e - HALO_BLK + 1, :]
            else:
                row = e - HALO_BLK - blocks
                value = sides[1, c, row : row + 1, :] + (1.0 * blocks if c == 0 else 0.0)
            ext[e, c : c + 1, :] = value

    def position_columns(e, carry):
        spread_columns(e, [ext[e, c : c + 1, :] for c in range(3)])
        return carry

    with jax.named_scope("poscols"):
        lax.fori_loop(0, blocks + 2 * HALO_BLK, position_columns, 0)
    lag = iota((8, TILE), 1) - iota((8, TILE), 0)

    def tensors(index, carry):
        b, k = index // reach, index % reach
        near = jnp.float32(0.0)
        for s in range(reach):
            near = jnp.where((list_ref[b, s] == b + k) & (s < count_ref[b]), 1.0, near)
        home = [jnp.broadcast_to(ext[b + HALO_BLK, c : c + 1, :], (8, TILE)) for c in range(3)]
        hide = jnp.where(k == HALO_BLK, 0, 4 * TILE)
        for j in range(TILE // 8):
            rows = slice(8 * j, 8 * j + 8)
            r = [home[c] - cols[b + k, c, rows, :] for c in range(3)]
            inverse = lax.rsqrt(r[0] * r[0] + r[1] * r[1] + r[2] * r[2] + 1.0)
            live = jnp.where(lag != 8 * j + hide, near, 0.0)
            square = live * inverse * inverse
            tens[index, 0, rows, :] = PAIR_C * (square * inverse)
            weight = (3.0 * PAIR_C) ** 0.5 * (square * inverse * lax.rsqrt(inverse))
            for c in range(3):
                tens[index, 1 + c, rows, :] = weight * r[c]
        return carry

    with jax.named_scope("tensors"):
        lax.fori_loop(0, blocks * reach, tensors, 0)

    freq = me * kys + iota((kys, TILE), 0)
    sine_mode = freq > GRID // 2
    number = jnp.where(sine_mode, freq - GRID // 2, freq).astype(F32)
    lead_in = jnp.where(sine_mode, GRID // 4, 0).astype(F32)
    shifts = [turn(number * (1.0 * k)) for k in range(ORDER)]

    wz[...] = jnp.zeros_like(wz)

    def flip(at):
        for j in range(4):
            both = slice(2 * j * TILE, (2 * j + 2) * TILE)
            turned = lax.dot_general(
                eye_ref[...], table[at, :, both], CONTRACT_LANES, preferred_element_type=F32
            )
            flipped[at, both, :] = turned.astype(BF16)

    def block_tables(slab, b):
        at, j = slab * halves + b // 4, b % 4
        first = jnp.broadcast_to(info[slab, 0, b : b + 1, :], (kys, TILE))
        cosine, sine = turn(number * first - lead_in)
        for t in range(2):
            rows = [wt[ORDER * t + k, b : b + 1, :] for k in range(ORDER)]
            real = combine([s[0] for s in shifts], rows)
            imag = combine([s[1] for s in shifts], rows)
            yq[slab * blocks + b, t] = cosine * real - sine * imag
        begin = jnp.broadcast_to(info[slab, 2, b : b + 1, :], (8, TILE)).astype(jnp.int32)
        for i in range(GRID // 16):
            gaps = [
                jnp.minimum((iota((8, TILE), 0) + (16 * i + 8 * r - begin)) & (GRID - 1), 7)
                for r in range(2)
            ]
            for t in range(2):
                dense = jnp.concatenate([pick(wz[t, b], gap) for gap in gaps], axis=0)
                high, rest = split(dense)
                table[at, 16 * i : 16 * i + 16, lanes(2 * j + t)] = high
                table[at, GRID + 16 * i : GRID + 16 * i + 16, lanes(2 * j + t)] = rest

    def slab_tables(d, carry):
        with jax.named_scope("info_wait"):
            @pl.when(d > 0)
            def _():
                got_share(d, True)

        slab = lax.rem(me + away(d), ranks)
        values, slopes = spline_rows(info[slab, 4])
        for k in range(ORDER):
            xw[slab, k] = values[k]
            xw[slab, ORDER + k] = slopes[k]
        for t in range(2):
            values, slopes = spline_rows(info[slab, 2 * t + 1])
            for k in range(ORDER):
                if t == 0:
                    wt[k] = values[k]
                    wt[ORDER + k] = slopes[k]
                else:
                    for b in range(blocks):
                        wz[0, b, k : k + 1, :] = values[k][b : b + 1, :]
                        wz[1, b, k : k + 1, :] = slopes[k][b : b + 1, :]

        before = lax.rem(me + away(jnp.maximum(d - 1, 0)), ranks) * halves + halves - 1
        with jax.named_scope("tables"):
            for h in range(halves):
                flip(before if h == 0 else slab * halves + h - 1)
                for j in range(4):
                    block_tables(slab, 4 * h + j)
        return carry

    lax.fori_loop(0, ranks, slab_tables, 0)
    flip(lax.rem(me + away(ranks - 1), ranks) * halves + halves - 1)
    sent_share(True)

    def weigh(slab, slot):
        v = [info[slab, FIELD0 + c] for c in range(3)]
        for k in range(ORDER):
            x, dx = xw[slab, k], xw[slab, ORDER + k]
            vx[slot, k] = v[0] * dx
            vx[slot, ORDER + k] = v[1] * x
            vx[slot, 2 * ORDER + k] = v[2] * x
        for h in range(halves):
            for j in range(4):
                b = 4 * h + j
                y, dy = yq[slab * blocks + b, 0], yq[slab * blocks + b, 1]
                none = jnp.zeros((kys, TILE), F32)
                lead, tail = [none] * 8, [none] * 8
                for k in range(ORDER):
                    lead[j + k] = vx[slot, k, b : b + 1, :] * y + vx[slot, ORDER + k, b : b + 1, :] * dy
                    tail[j + k] = vx[slot, 2 * ORDER + k, b : b + 1, :] * y
                for t, pieces in enumerate((lead, tail)):
                    high, rest = split(jnp.concatenate(pieces, axis=0))
                    mix[slot, h, : 8 * kys, lanes(2 * j + t)] = high
                    mix[slot, h, 8 * kys :, lanes(2 * j + t)] = rest

    def window(slab, h):
        return pl.ds(pl.multiple_of((slab * planes + 4 * h) * kys, 4 * kys), 8 * kys)

    def spread_slab(slab, slot):
        count = 8 * kys
        for h in range(halves):
            sums = dot(mix[slot, h], flipped[slab * halves + h])
            grid[window(slab, h), :] += sums[:count, :GRID] + sums[:count, GRID:] + sums[count:, :GRID]

    def read_slab(slab, slot):
        for h in range(halves):
            at = window(slab, h)
            left = jnp.concatenate([wide[at, :], low[at, :]], axis=0)
            hold[slot, h] = dot(left, table[slab * halves + h])

    def gather_slab(slab, slot):
        count = 8 * kys
        for h in range(halves):
            for j in range(4):
                b = 4 * h + j
                one = two = three = 0.0
                for k in range(ORDER):
                    rows = slice((j + k) * kys, (j + k + 1) * kys)
                    more = slice(count + (j + k) * kys, count + (j + k + 1) * kys)
                    plain = hold[slot, h, rows, lanes(2 * j)] + hold[slot, h, more, lanes(2 * j)]
                    tilted = hold[slot, h, rows, lanes(2 * j + 1)] + hold[slot, h, more, lanes(2 * j + 1)]
                    x, dx = xw[slab, k, b : b + 1, :], xw[slab, ORDER + k, b : b + 1, :]
                    one += dx * plain
                    two += x * plain
                    three += x * tilted
                y, dy = yq[slab * blocks + b, 0], yq[slab * blocks + b, 1]
                for c, term in enumerate((y * one, dy * two, y * three)):
                    out_part[slab, c, b : b + 1, :] = jnp.sum(term, axis=0, keepdims=True)

    count = ITERS + 1
    entries = {}
    for i in range(ITERS):
        for j in range(i, ITERS):
            entries[i, j] = entries[j, i] = len(set(entries.values()))
    last = len(set(entries.values()))
    for i in range(ITERS - 1):
        entries[i, ITERS] = entries[i + 1, ITERS - 1]
    entries[ITERS - 1, ITERS] = last

    def tell(i, row):
        return pltpu.make_async_remote_copy(
            src_ref=part, dst_ref=slots.at[lax.rem(me + row, ranks)], send_sem=gram_send.at[i],
            recv_sem=gram_recv.at[i], device_id={"gx": lax.rem(me + i, ranks)},
            device_id_type=pl.DeviceIdType.MESH,
        )

    def send_products():
        column = iota((1, TILE), 1)
        packed = jnp.zeros((1, TILE), F32)
        for i in range(ITERS):
            for j in range(i, ITERS):
                value = 0.0
                for c in range(3):
                    value += bases[i, c] * (bases[j, c] / polar_ref[...])
                packed = jnp.where(column == entries[i, j], total_of(value), packed)
        value = 0.0
        for c in range(3):
            value += pair[c] * info[me, FIELD0 + c]
        packed = jnp.where(column == last, total_of(value) - total_of(energy[...]), packed)
        part[...] = packed
        slots[me] = packed

        def one(i, carry):
            tell(i, 0).start()
            return carry

        lax.fori_loop(1, ranks, one, 0)

    def sweep(it, carry):
        with jax.named_scope("near_wait"):
            @pl.when(it > 0)
            def _():
                start_share(False)

        grid[...] = jnp.zeros_like(grid)

        def slab_at(d):
            return lax.rem(me + away(jnp.minimum(d, ranks - 1)), ranks)

        def vector_columns(n):
            n = jnp.minimum(n, blocks + 2 * HALO_BLK - 1)
            e = jnp.where(n < blocks, n + HALO_BLK, jnp.where(n < blocks + HALO_BLK, n - blocks, n))
            step = jnp.where(e < HALO_BLK, ranks - 1, jnp.where(e < HALO_BLK + blocks, 0, 1))
            slab = lax.rem(me + step, ranks)
            row = lax.rem(e + blocks - HALO_BLK, blocks)
            spread_columns(e, [info[slab, FIELD0 + c, pl.ds(row, 1), :] for c in range(3)])

        def spread_two(m, inner):
            with jax.named_scope("far_wait"):
                for d in (2 * m + 1, 2 * m + 2):

                    @pl.when((it > 0) & (d < ranks))
                    def _(d=d):
                        got_share(d, False)

            with jax.named_scope("spread"):
                weigh(slab_at(2 * m + 1), 1)
                spread_slab(slab_at(2 * m), 0)
                for n in (2 * m, 2 * m + 1):
                    vector_columns(n)
                weigh(slab_at(2 * m + 2), 0)
                spread_slab(slab_at(2 * m + 1), 1)
            return inner

        weigh(me, 0)
        lax.fori_loop(0, ranks // 2, spread_two, 0)

        with jax.named_scope("fold"):
            size = GRID * kys
            edge = 2 * kys
            grid[size : size + edge, :] += grid[0:edge, :]
            grid[edge : 2 * edge, :] += grid[size + edge : size + 2 * edge, :]

        step = 2 * GRID
        with jax.named_scope("zin"):
            for i in range(size // step):
                high, rest = split(grid[edge + i * step : edge + (i + 1) * step, :])
                sums = dot(jnp.concatenate([high, rest], axis=1), zin_ref[...])
                spec[i * step : (i + 1) * step, :] = sums[:, :GRID] + sums[:, GRID:]
        with jax.named_scope("xinout"):
            power = jnp.zeros((8, GRID), F32)
            for q in range(0, kys, 2):
                pairs = [pl.ds(q, GRID, stride=kys), pl.ds(q + 1, GRID, stride=kys)]
                high, rest = split(jnp.concatenate([spec[s, :] for s in pairs], axis=1))
                line = dot(xin_ref[...], jnp.concatenate([high, rest, high], axis=0))
                passed = line * jnp.concatenate([green[q], green[q + 1]], axis=1)
                worth = line * passed
                power += jnp.sum((worth[:, :GRID] + worth[:, GRID:]).reshape(GRID // 8, 8, GRID), axis=0)
                line = passed
                high, rest = split(line)
                line = dot(xout_ref[...], jnp.concatenate([high, rest, high], axis=0))
                spec[pairs[0], :] = line[:, :GRID]
                spec[pairs[1], :] = line[:, GRID:]
            energy[...] = power
        with jax.named_scope("zout"):
            for i in range(size // step):
                high, rest = split(spec[i * step : (i + 1) * step, :])
                sums = dot(jnp.concatenate([high, rest], axis=1), zout_ref[...])
                high, rest = split(sums[:, :GRID] + sums[:, GRID:])
                rows = slice(edge + i * step, edge + (i + 1) * step)
                wide[rows, :] = jnp.concatenate([high, high], axis=1)
                low[rows, :] = jnp.concatenate([rest, jnp.zeros_like(rest)], axis=1)
            for ref in (wide, low):
                ref[0:edge, :] = ref[size : size + edge, :]
                ref[size + edge : size + 2 * edge, :] = ref[edge : 2 * edge, :]

        def gather_two(m, inner):
            first, second = ranks - 1 - 2 * m, ranks - 2 - 2 * m
            with jax.named_scope("gather"):
                read_slab(slab_at(second), 1)
                gather_slab(slab_at(first), 0)
                read_slab(slab_at(jnp.maximum(second - 1, 0)), 0)
                gather_slab(slab_at(second), 1)
            fold(away(first), slab_at(first)).start()

            @pl.when(second > 0)
            def _():
                fold(away(second), slab_at(second)).start()

            return inner

        read_slab(slab_at(ranks - 1), 0)
        lax.fori_loop(0, ranks // 2, gather_two, 0)

        def one_home(b, inner):
            def one_source(k, sums):
                sums = list(sums)
                for j in range(TILE // 8):
                    rows = slice(8 * j, 8 * j + 8)
                    v = [cols[b + k, c, rows, :] for c in range(3)]
                    w = [tens[b * reach + k, 1 + c, rows, :] for c in range(3)]
                    third = tens[b * reach + k, 0, rows, :]
                    along = w[0] * v[0] + w[1] * v[1] + w[2] * v[2]
                    for c in range(3):
                        sums[c] = sums[c] + third * v[c]
                        sums[3 + c] = sums[3 + c] + along * w[c]
                return tuple(sums)

            sums = lax.fori_loop(0, reach, one_source, (jnp.zeros((8, TILE), F32),) * 6)
            for c in range(3):
                pair[c, pl.ds(b, 1), :] = jnp.sum(sums[c] - sums[3 + c], axis=0, keepdims=True)
            return inner

        with jax.named_scope("pair"):
            lax.fori_loop(0, blocks, one_home, 0)

        @pl.when(it == ITERS - 1)
        def _():
            with jax.named_scope("gram"):
                send_products()

        with jax.named_scope("sent_wait"):
            @pl.when(it > 0)
            def _():
                sent_share(False)

        def landed(i, inner):
            fold(i, lax.rem(me + i, ranks)).wait()
            return inner

        with jax.named_scope("rs_wait"):
            lax.fori_loop(1, ranks, landed, 0)
        with jax.named_scope("update"):
            for c in range(3):
                total = out_part[me, c]
                for i in range(1, ranks):
                    total = total + in_part[i, c]
                following = pair[c] - total
                bases[it + 1, c] = following
                info[me, FIELD0 + c] = following / polar_ref[...]
        return carry

    lax.fori_loop(0, ITERS, sweep, 0)

    def tell_wait(i, carry):
        tell(i, ranks - i).wait()
        return carry

    with jax.named_scope("gram_wait"):
        lax.fori_loop(1, ranks, tell_wait, 0)
    sums = jnp.sum(slots[...], axis=0)
    sums = {r: jnp.broadcast_to(sums[:, r : r + 1], (1, TILE)) for r in range(last + 1)}
    dipoles, residual = krylov(sums, entries, count)
    for c in range(3):
        basis = [bases[i, c] for i in range(count)]
        first = combine(dipoles, [b / polar_ref[...] for b in basis])
        second = combine(residual, basis)
        for b in range(blocks):
            dip_ref[c : c + 1, lanes(b)] = first[b : b + 1, :]
            res_ref[c : c + 1, lanes(b)] = second[b : b + 1, :]


def krylov(sums, place, count):
    def inner(x, y):
        value = None
        for i in range(count):
            for j in range(count):
                if x[i] is not None and y[j] is not None:
                    row = place[i, j]
                    term = x[i] * y[j] * sums[row]
                    value = term if value is None else value + term
        return value

    none = [None] * (count - 1)
    residual = [jnp.ones((1, TILE), F32)] + none
    direction = list(residual)
    dipoles = [None] * count
    rz_now = inner(residual, residual)
    for sweep in range(ITERS):
        image = scaled(-1.0, direction, [None] + direction[:-1])
        step = rz_now / inner(direction, image)
        dipoles = scaled(step, dipoles, direction)
        residual = scaled(-step, residual, image)
        if sweep + 1 < ITERS:
            rz_next = inner(residual, residual)
            direction = scaled(rz_next / rz_now, residual, direction)
            rz_now = rz_next
    return dipoles, residual


def fast_shapes(ranks, blocks):
    kys = GRID // ranks
    ext_blocks = blocks + 2 * HALO_BLK
    rows = (GRID + 4) * kys
    dma = pltpu.SemaphoreType.DMA
    tile = (blocks, TILE)
    buffers = [
        ((2, blocks * TILE, GRID), F32),
        ((ranks, 8) + tile, F32),
        ((ranks * blocks // 4, 2 * GRID, 8 * TILE), BF16),
        ((ranks * blocks // 4, 8 * TILE, 2 * GRID), BF16),
        ((ranks * blocks, 2, kys, TILE), F32),
        ((ranks, 2 * ORDER) + tile, F32),
        ((2 * ORDER,) + tile, F32),
        ((2, blocks, 8, TILE), F32),
        ((2, 3 * ORDER) + tile, F32),
        ((2, blocks // 4, 16 * kys, 8 * TILE), BF16),
        ((2, blocks // 4, 16 * kys, 8 * TILE), F32),
        ((rows, GRID), F32),
        ((GRID * kys, GRID), F32),
        ((rows, 2 * GRID), BF16),
        ((rows, 2 * GRID), BF16),
        ((kys, GRID, GRID), F32),
        ((blocks * (2 * HALO_BLK + 1), 4, TILE, TILE), F32),
        ((ext_blocks, 3, TILE, TILE), F32),
        ((3,) + tile, F32),
        ((2, 3) + tile, F32),
        ((ext_blocks, 8, TILE), F32),
        ((ITERS + 1, 3) + tile, F32),
        ((3,) + tile, F32),
        ((ranks, 3) + tile, F32),
        ((ranks, 3) + tile, F32),
        ((1, TILE), F32),
        ((ranks, 1, TILE), F32),
        ((8, GRID), F32),
    ]
    sems = [dma((2,))] + [dma((ranks,))] * 4 + [dma((2,))] * 2 + [dma((ranks,))] * 2
    return buffers, sems


def fits_fast(ranks, blocks):
    if blocks != 8 or GRID % ranks or GRID // ranks != blocks:
        return False
    buffers, _ = fast_shapes(ranks, blocks)
    return sum(int(np.prod(s)) * np.dtype(t).itemsize for s, t in buffers) < 60 * 1024 * 1024


def halves_of(x):
    high = x.astype(BF16)
    return high, (x - high.astype(np.float32)).astype(BF16)


def fast_device(positions, field, inv_polar, x_spline, yz_spline, tile_list, tile_count):
    ranks = lax.axis_size("gx")
    atoms_here = positions.shape[1]
    blocks = atoms_here // TILE
    line = np.arange(GRID)
    center = (line[None, :] - line[:, None] + GRID // 2) % GRID - GRID // 2
    center = np.concatenate([center, np.eye(GRID)], axis=0)
    center = np.concatenate([center.astype(np.float32).astype(BF16)] * 3, axis=1)
    rows = fixed_rows(line)

    def along_z(m):
        high, rest = halves_of(np.ascontiguousarray(m))
        return np.concatenate(
            [np.concatenate([high, rest], axis=1), np.concatenate([high, np.zeros_like(rest)], axis=1)], axis=0
        )

    def along_x(m):
        high, rest = halves_of(np.ascontiguousarray(m))
        return np.concatenate([high, high, rest], axis=1)

    eye = np.eye(2 * TILE, dtype=np.float32).astype(BF16)
    constants = [center, eye, along_z(rows.T), along_z(rows), along_x(rows), along_x(rows.T)]
    buffers, sems = fast_shapes(ranks, blocks)
    smem = pl.BlockSpec(memory_space=pltpu.SMEM)
    return pl.pallas_call(
        functools.partial(fast_kernel, ranks),
        in_specs=[VMEM] * 4 + [smem] * 2 + [VMEM] * len(constants) + [pl.BlockSpec(memory_space=pl.ANY)],
        out_specs=[VMEM] * 2,
        out_shape=[jax.ShapeDtypeStruct(positions.shape, F32)] * 2,
        scratch_shapes=[pltpu.VMEM(s, t) for s, t in buffers] + sems,
        compiler_params=pltpu.CompilerParams(
            vmem_limit_bytes=62 * 1024 * 1024, collective_id=2, has_side_effects=True
        ),
        name="induced",
    )(
        positions, field, inv_polar.reshape(blocks, TILE), x_spline.transpose(1, 0, 2),
        tile_list, tile_count, *[jnp.asarray(c) for c in constants], yz_spline,
    )


def solution(mesh):
    placed = (
        P(None, ("rep", "gx")),
        P(None, ("rep", "gx")),
        P(("rep", "gx")),
        P(None, None, ("rep", "gx")),
        P(None, ("rep", "gx"), None),
        P(("rep", "gx"), None),
        P(("rep", "gx")),
    )
    ranks = mesh.shape["gx"]

    def choose(*arrays):
        device = fast_device if fits_fast(ranks, arrays[0].shape[1] // TILE) else per_device
        return device(*arrays)

    return jax.shard_map(
        choose,
        mesh=mesh,
        in_specs=placed,
        out_specs=(P(None, ("rep", "gx")), P(None, ("rep", "gx"))),
        check_vma=False,
    )
```

```python
import jax
import jax.numpy as jnp
from jax import lax
from jax.experimental import pallas as pl
from jax.experimental.pallas import tpu as pltpu
from jax.sharding import PartitionSpec as P
import functools
import numpy as np

GRID = 128
ORDER = 5
TILE = 128
HALO_BLK = 3
ITERS = 3


PAIR_C = 0.025
RECIP_C = 8192.0
DAMP = 0.0008
EXACT = lax.Precision.HIGHEST


def mode_of(freq, size):
    half_size = size // 2
    mode_num = jnp.where(freq <= half_size, freq, freq - half_size)
    weight = jnp.where((freq == 0) | (freq == half_size), 1.0 / size, 2.0 / size)
    return (mode_num.astype(jnp.float32), weight.astype(jnp.float32))


def basis_rows(size, points):
    freq = jnp.arange(size, dtype=jnp.int32)
    half_size = size // 2
    mode_num = jnp.where(freq <= half_size, freq, freq - half_size)
    phase = mode_num[:, None] * points[None, :] % size
    angle = phase.astype(jnp.float32) * (2.0 * jnp.pi / size)
    return jnp.where((freq <= half_size)[:, None], jnp.cos(angle), jnp.sin(angle))


def kernel_block(x_modes, x_weights, y_modes, y_weights, z_modes, z_weights):
    mode_sq = (
        x_modes[:, None, None] * x_modes[:, None, None]
        + y_modes[None, :, None] * y_modes[None, :, None]
        + z_modes[None, None, :] * z_modes[None, None, :]
    )
    safe_sq = jnp.where(mode_sq > 0, mode_sq, 1.0)
    green = jnp.where(mode_sq > 0, RECIP_C * jnp.exp(-DAMP * safe_sq) / safe_sq, 0.0)
    return green * x_weights[:, None, None] * y_weights[None, :, None] * z_weights[None, None, :]


F32 = jnp.float32
BF16 = jnp.bfloat16
VMEM = pl.BlockSpec(memory_space=pltpu.VMEM)


def split(x):
    high = x.astype(BF16)
    return high, (x - high.astype(F32)).astype(BF16)


def dot(a, b):
    return jnp.dot(a, b, preferred_element_type=F32)


def params(**more):
    return pltpu.CompilerParams(vmem_limit_bytes=56 * 1024 * 1024, **more)


def prep_kernel(yz_ref, rows_ref, yft_ref, zf_ref, zft_ref):
    rows = jnp.concatenate(split(rows_ref[...]), axis=0)

    def transformed(t):
        high, low = split(jnp.concatenate([yz_ref[t], yz_ref[t + 1]], axis=0))
        contract = (((1,), (1,)), ((), ()))
        wide = lax.dot_general(rows, high, contract, preferred_element_type=F32)
        more = lax.dot_general(rows[:GRID], low, contract, preferred_element_type=F32)
        return wide[:GRID] + wide[GRID:] + more

    lines = transformed(0)
    yft_ref[0, 0] = lines[:, :TILE]
    yft_ref[0, 1] = lines[:, TILE:]
    lines = transformed(2)
    zft_ref[0] = jnp.concatenate(split(lines), axis=0)
    zf_ref[0] = jnp.concatenate(split(lines.T), axis=1)


def prepare(yz_spline, rows, blocks):
    return pl.pallas_call(
        prep_kernel,
        grid=(blocks,),
        in_specs=[
            pl.BlockSpec((4, TILE, GRID), lambda b: (0, b, 0)),
            pl.BlockSpec((GRID, GRID), lambda b: (0, 0)),
        ],
        out_specs=[
            pl.BlockSpec((1, 2, GRID, TILE), lambda b: (b, 0, 0, 0)),
            pl.BlockSpec((1, 2 * TILE, 2 * GRID), lambda b: (b, 0, 0)),
            pl.BlockSpec((1, 2 * GRID, 2 * TILE), lambda b: (b, 0, 0)),
        ],
        out_shape=[
            jax.ShapeDtypeStruct((blocks, 2, GRID, TILE), F32),
            jax.ShapeDtypeStruct((blocks, 2 * TILE, 2 * GRID), BF16),
            jax.ShapeDtypeStruct((blocks, 2 * GRID, 2 * TILE), BF16),
        ],
        compiler_params=params(),
        name="prep",
    )(yz_spline, rows)


def spread_kernel(planes, ky_count, pv_ref, xs_ref, yft_ref, zf_ref, out_ref):
    blocks = pv_ref.shape[0]
    ranks = out_ref.shape[0]
    out_ref[...] = jnp.zeros_like(out_ref)

    def one_block(b, carry):
        base = b * planes // blocks
        y, dy = yft_ref[b, 0], yft_ref[b, 1]
        v0, v1, v2 = (pv_ref[b, 3 + c : 4 + c, :] for c in range(3))
        highs, lows = [], []
        for k in range(ORDER):
            x, dx = xs_ref[b, k : k + 1, :], xs_ref[b, ORDER + k : ORDER + k + 1, :]
            lead = (v0 * dx) * y + (v1 * x) * dy
            high, low = split(jnp.concatenate([lead, (v2 * x) * y], axis=1))
            highs.append(high)
            lows.append(low)
        weights = zf_ref[b]
        wide = dot(jnp.concatenate(highs, axis=0), weights)
        total = (
            wide[:, :GRID] + wide[:, GRID:] + dot(jnp.concatenate(lows, axis=0), weights[:, :GRID])
        )
        for k in range(ORDER):
            part = total[k * GRID : (k + 1) * GRID].reshape(ranks, ky_count, GRID)
            out_ref[:, base + k, :ky_count, :] += part
        return carry

    lax.fori_loop(0, blocks, one_block, 0)


def gather_kernel(
    planes, ky_count, ret_ref, xs_ref, yft_ref, zft_ref, pair_ref, pv_ref, polar_ref,
    next_ref, pv_next_ref, wide_ref, low_ref,
):
    blocks = xs_ref.shape[0]
    extent = ret_ref.shape[1]
    for p in range(extent):
        high, low = split(ret_ref[:, p, :ky_count, :].reshape(GRID, GRID))
        wide_ref[p] = jnp.concatenate([high, high], axis=1)
        low_ref[p] = low

    def one_block(b, carry):
        base = b * planes // blocks
        weights = zft_ref[b]
        wide = wide_ref[pl.ds(base, ORDER)].reshape(ORDER * GRID, 2 * GRID)
        low = low_ref[pl.ds(base, ORDER)].reshape(ORDER * GRID, GRID)
        sums = dot(wide, weights) + dot(low, weights[:GRID])
        one = two = three = 0.0
        for k in range(ORDER):
            x, dx = xs_ref[b, k : k + 1, :], xs_ref[b, ORDER + k : ORDER + k + 1, :]
            plain = sums[k * GRID : (k + 1) * GRID, :TILE]
            one += dx * plain
            two += x * plain
            three += x * sums[k * GRID : (k + 1) * GRID, TILE:]
        y, dy = yft_ref[b, 0], yft_ref[b, 1]
        far = jnp.concatenate(
            [jnp.sum(t, axis=0, keepdims=True) for t in (y * one, dy * two, y * three)], axis=0
        )
        following = pair_ref[b] - far
        next_ref[b] = following
        pv_next_ref[b, 0:3] = pv_ref[b, 0:3]
        pv_next_ref[b, 3:6] = following / polar_ref[b]
        pv_next_ref[b, 6:8] = jnp.zeros((2, TILE), F32)
        return carry

    lax.fori_loop(0, blocks, one_block, 0)


def pair_sum(near_ref, pv_ref, before_ref, after_ref, out_ref, ext_ref, col_ref):
    blocks = pv_ref.shape[0]
    reach = 2 * HALO_BLK + 1
    first_row = lax.broadcasted_iota(jnp.int32, (HALO_BLK, 8, TILE), 1) == 0
    ext_ref[:HALO_BLK] = before_ref[...] + jnp.where(first_row, -1.0 * blocks, 0.0)
    ext_ref[HALO_BLK : HALO_BLK + blocks] = pv_ref[...]
    ext_ref[HALO_BLK + blocks :] = after_ref[...] + jnp.where(first_row, 1.0 * blocks, 0.0)
    lag = lax.broadcasted_iota(jnp.int32, (8, TILE), 1) - lax.broadcasted_iota(
        jnp.int32, (8, TILE), 0
    )

    def spread_columns(e, carry):
        for c in range(6):
            col_ref[e, c] = jnp.broadcast_to(ext_ref[e, c : c + 1, :], (TILE, TILE)).T
        return carry

    lax.fori_loop(0, blocks + 2 * HALO_BLK, spread_columns, 0)

    def one_home(b, carry):
        home = [jnp.broadcast_to(pv_ref[b, c : c + 1, :], (8, TILE)) for c in range(3)]

        def one_source(k, sums):
            shift = jnp.where(k == HALO_BLK, 0, 4 * TILE)
            direct = [jnp.zeros((8, TILE), F32) for c in range(3)]
            tilted = [jnp.zeros((8, TILE), F32) for c in range(3)]
            for j in range(TILE // 8):
                rows = slice(8 * j, 8 * j + 8)
                r = [home[c] - col_ref[b + k, c, rows, :] for c in range(3)]
                v = [col_ref[b + k, 3 + c, rows, :] for c in range(3)]
                inverse = lax.rsqrt(r[0] * r[0] + r[1] * r[1] + r[2] * r[2] + 1.0)
                inverse = jnp.where(lag != 8 * j + shift, inverse, 0.0)
                square = inverse * inverse
                third = square * inverse
                weight = third * square * (r[0] * v[0] + r[1] * v[1] + r[2] * v[2])
                for c in range(3):
                    direct[c] += third * v[c]
                    tilted[c] += weight * r[c]
            near = near_ref[b * reach + k]
            return tuple(
                sums[c] + near * (direct[c] - 3.0 * tilted[c]) for c in range(3)
            )

        sums = lax.fori_loop(0, reach, one_source, (jnp.zeros((8, TILE), F32),) * 3)
        out_ref[b] = PAIR_C * jnp.concatenate(
            [jnp.sum(t, axis=0, keepdims=True) for t in sums], axis=0
        )
        return carry

    lax.fori_loop(0, blocks, one_home, 0)


def greet(ranks, me):
    barrier = pltpu.get_barrier_semaphore()

    def signal(d, carry):
        pl.semaphore_signal(
            barrier,
            inc=1,
            device_id={"gx": lax.rem(me + d, ranks)},
            device_id_type=pl.DeviceIdType.MESH,
        )
        return carry

    lax.fori_loop(1, ranks, signal, 0)
    pl.semaphore_wait(barrier, ranks - 1)


def exchange(ranks, me, source, target, local_sem, send_sem, recv_sem):
    def copy(d, slot):
        peer = lax.rem(me + d, ranks)
        return pltpu.make_async_remote_copy(
            src_ref=source(peer),
            dst_ref=target(slot),
            send_sem=send_sem.at[d],
            recv_sem=recv_sem.at[d],
            device_id={"gx": peer},
            device_id_type=pl.DeviceIdType.MESH,
        )

    def start(d, carry):
        copy(d, me).start()
        return carry

    def finish(d, carry):
        copy(d, lax.rem(me - d + ranks, ranks)).wait()
        return carry

    lax.fori_loop(1, ranks, start, 0)
    own = pltpu.make_async_copy(source(me), target(me), local_sem)
    own.start()

    def wait():
        own.wait()
        lax.fori_loop(1, ranks, finish, 0)

    return wait


def middle_kernel(
    ranks, ky_count, near_ref, spec_ref, pv_ref, green_ref, across_ref, back_ref,
    ret_ref, pair_ref,
    before_ref, after_ref, ext_ref, col_ref, recv_ref, done_ref, local_sems, send1, recv1, send2, recv2, halo_send, halo_recv,
):
    me = lax.axis_index("gx")
    blocks = pv_ref.shape[0]
    extent = spec_ref.shape[1]
    rows = ranks * extent
    greet(ranks, me)
    halos = []
    for t, (piece, into, step) in enumerate(
        (
            (pv_ref.at[pl.ds(blocks - HALO_BLK, HALO_BLK)], before_ref, 1),
            (pv_ref.at[pl.ds(0, HALO_BLK)], after_ref, ranks - 1),
        )
    ):
        halos.append(
            pltpu.make_async_remote_copy(
                src_ref=piece,
                dst_ref=into,
                send_sem=halo_send.at[t],
                recv_sem=halo_recv.at[t],
                device_id={"gx": lax.rem(me + step, ranks)},
                device_id_type=pl.DeviceIdType.MESH,
            )
        )
        halos[-1].start()
    wait = exchange(
        ranks, me, lambda d: spec_ref.at[d], lambda d: recv_ref.at[d], local_sems.at[0], send1, recv1
    )
    across_high, across_low = split(across_ref[...])
    back_high, back_low = split(back_ref[...])
    wait()
    lines_in = recv_ref.reshape(rows * 8, GRID)
    lines_out = done_ref.reshape(rows * 8, GRID)
    for q in range(ky_count):
        high, low = split(lines_in[pl.ds(q, rows, stride=8), :])
        wide = dot(across_high, jnp.concatenate([high, low], axis=1))
        line = wide[:, :GRID] + wide[:, GRID:] + dot(across_low, high)
        high, low = split(line * green_ref[q])
        wide = dot(back_high, jnp.concatenate([high, low], axis=1))
        lines_out[pl.ds(q, rows, stride=8), :] = (
            wide[:, :GRID] + wide[:, GRID:] + dot(back_low, high)
        )
    wait = exchange(
        ranks, me, lambda d: done_ref.at[d], lambda d: ret_ref.at[d], local_sems.at[1], send2, recv2
    )
    for halo in halos:
        halo.wait()
    pair_sum(near_ref, pv_ref, before_ref, after_ref, pair_ref, ext_ref, col_ref)
    wait()


def middle(near, spec, pv, green, across, back, ranks, ky_count):
    dma = pltpu.SemaphoreType.DMA
    blocks = pv.shape[0]
    halo = pltpu.VMEM((HALO_BLK, 8, TILE), F32)
    return pl.pallas_call(
        functools.partial(middle_kernel, ranks, ky_count),
        in_specs=[pl.BlockSpec(memory_space=pltpu.SMEM)] + [VMEM] * 5,
        out_specs=[VMEM] * 2,
        out_shape=[
            jax.ShapeDtypeStruct(spec.shape, F32),
            jax.ShapeDtypeStruct((blocks, 3, TILE), F32),
        ],
        scratch_shapes=[
            halo,
            halo,
            pltpu.VMEM((blocks + 2 * HALO_BLK, 8, TILE), F32),
            pltpu.VMEM((blocks + 2 * HALO_BLK, 6, TILE, TILE), F32),
            pltpu.VMEM(spec.shape, F32),
            pltpu.VMEM(spec.shape, F32),
            dma((2,)), dma((ranks,)), dma((ranks,)), dma((ranks,)), dma((ranks,)),
            dma((2,)), dma((2,)),
        ],
        compiler_params=params(collective_id=0, has_side_effects=True),
        name="middle",
    )(near, spec, pv, green, across, back)


def combine(weights, parts):
    terms = [w * p for w, p in zip(weights, parts) if w is not None]
    return functools.reduce(jnp.add, terms)


def scaled(a, x, y):
    pairs = zip(x, y)
    return [p if q is None else (a * q if p is None else p + a * q) for p, q in pairs]


def solve_kernel(
    ranks, b0_ref, b1_ref, b2_ref, b3_ref, polar_ref,
    dipoles_ref, residual_ref, part_ref, slots, local_sem, send_sem, recv_sem,
):
    me = lax.axis_index("gx")
    bases = [ref[...] for ref in (b0_ref, b1_ref, b2_ref, b3_ref)]
    soft = [b / polar_ref[...] for b in bases]
    count = ITERS + 1
    place = {}
    part_ref[...] = jnp.zeros_like(part_ref)
    for i in range(count):
        for j in range(i, count):
            place[i, j] = place[j, i] = row = len(set(place.values()))
            part_ref[row : row + 1] = jnp.sum(
                jnp.sum(bases[i] * soft[j], axis=0), axis=0, keepdims=True
            )
    greet(ranks, me)
    wait = exchange(
        ranks, me, lambda d: part_ref, lambda d: slots.at[d], local_sem.at[0], send_sem, recv_sem
    )
    wait()
    sums = jnp.sum(jnp.sum(slots[...], axis=0), axis=1, keepdims=True)
    sums = jnp.broadcast_to(sums, (sums.shape[0], TILE))

    def inner(x, y):
        value = None
        for i in range(count):
            for j in range(count):
                if x[i] is not None and y[j] is not None:
                    row = place[i, j]
                    term = x[i] * y[j] * sums[row : row + 1]
                    value = term if value is None else value + term
        return value

    none = [None] * (count - 1)
    residual = [jnp.ones((1, TILE), F32)] + none
    direction = list(residual)
    dipoles = [None] * count
    rz_now = inner(residual, residual)
    for sweep in range(ITERS):
        image = scaled(-1.0, direction, [None] + direction[:-1])
        step = rz_now / inner(direction, image)
        dipoles = scaled(step, dipoles, direction)
        residual = scaled(-step, residual, image)
        if sweep + 1 < ITERS:
            rz_next = inner(residual, residual)
            direction = scaled(rz_next / rz_now, residual, direction)
            rz_now = rz_next
    dipoles_ref[...] = combine(dipoles, soft)
    residual_ref[...] = combine(residual, bases)


def solve(bases, polar, ranks):
    dma = pltpu.SemaphoreType.DMA
    shape = bases[0].shape
    return pl.pallas_call(
        functools.partial(solve_kernel, ranks),
        in_specs=[VMEM] * 5,
        out_specs=[VMEM] * 2,
        out_shape=[jax.ShapeDtypeStruct(shape, F32)] * 2,
        scratch_shapes=[
            pltpu.VMEM((16, TILE), F32), pltpu.VMEM((ranks, 16, TILE), F32),
            dma((1,)), dma((ranks,)), dma((ranks,)),
        ],
        compiler_params=params(collective_id=1, has_side_effects=True),
        name="solve",
    )(*bases, polar)


def fixed_rows(points):
    half_size = GRID // 2
    freq = np.arange(GRID)
    mode_num = np.where(freq <= half_size, freq, freq - half_size)
    angle = (mode_num[:, None] * points[None, :] % GRID) * (2.0 * np.pi / GRID)
    return np.where((freq <= half_size)[:, None], np.cos(angle), np.sin(angle)).astype(np.float32)


def per_device(positions, field, inv_polar, x_spline, yz_spline, tile_list, tile_count):
    ranks = lax.axis_size("gx")
    rank_index = lax.axis_index("gx")
    atoms_here = positions.shape[1]
    planes = GRID // ranks
    extent = planes + 4
    blocks = atoms_here // TILE
    reach = 2 * HALO_BLK + 1
    ky_count = GRID // ranks

    def blocked(x):
        return x.reshape(-1, blocks, TILE).transpose(1, 0, 2)

    all_freq = jnp.arange(GRID, dtype=jnp.int32)
    fourier_rows = jnp.asarray(fixed_rows(np.arange(GRID)))
    ky_freq = rank_index * ky_count + jnp.arange(ky_count, dtype=jnp.int32)
    full_modes, full_weights = mode_of(all_freq, GRID)
    ky_modes, ky_weights = mode_of(ky_freq, GRID)
    green = kernel_block(ky_modes, ky_weights, full_modes, full_weights, full_modes, full_weights)
    source_rows = np.arange(ranks * extent)
    points = (source_rows // extent * planes - 2 + source_rows % extent) % GRID
    across = fixed_rows(points)
    back = jnp.asarray(np.ascontiguousarray(across.T))
    across = jnp.asarray(across)
    slots = jnp.arange(tile_list.shape[1], dtype=jnp.int32)
    wanted = jnp.arange(blocks, dtype=jnp.int32)[:, None] + jnp.arange(reach, dtype=jnp.int32)
    live = (slots[None, :] < tile_count[:, None])[:, :, None]
    near = jnp.any((tile_list[:, :, None] == wanted[:, None, :]) & live, axis=1)
    near = near.astype(F32).reshape(-1)
    yft, zf, zft = prepare(yz_spline, fourier_rows, blocks)
    xs = blocked(x_spline.reshape(2 * ORDER, atoms_here))
    pos = blocked(positions)
    polar = inv_polar.reshape(blocks, 1, TILE)
    spec_shape = jax.ShapeDtypeStruct((ranks, extent, 8, GRID), F32)
    rows_shape = jax.ShapeDtypeStruct((blocks, 3, TILE), F32)

    def advance(pv):
        spec = pl.pallas_call(
            functools.partial(spread_kernel, planes, ky_count),
            in_specs=[VMEM] * 4,
            out_specs=VMEM,
            out_shape=spec_shape,
            compiler_params=params(),
            name="spread",
        )(pv, xs, yft, zf)
        ret, pair = middle(near, spec, pv, green, across, back, ranks, ky_count)
        return pl.pallas_call(
            functools.partial(gather_kernel, planes, ky_count),
            in_specs=[VMEM] * 7,
            out_specs=[VMEM] * 2,
            out_shape=[rows_shape, jax.ShapeDtypeStruct((blocks, 8, TILE), F32)],
            scratch_shapes=[
                pltpu.VMEM((extent, GRID, 2 * GRID), BF16),
                pltpu.VMEM((extent, GRID, GRID), BF16),
            ],
            compiler_params=params(),
            name="gather",
        )(ret, xs, yft, zft, pair, pv, polar)

    bases = [blocked(field)]
    pv = jnp.concatenate([pos, bases[0] / polar, jnp.zeros((blocks, 2, TILE), F32)], axis=1)
    for sweep in range(ITERS):
        following, pv = advance(pv)
        bases.append(following)
    dipoles, residual = solve(bases, polar, ranks)

    def flat(x):
        return x.transpose(1, 0, 2).reshape(3, atoms_here)

    return flat(dipoles), flat(residual)


FIELD0 = 5


def spline_rows(u):
    v = 1.0 - u

    def inner(p):
        return ((((-4.0 * p + 4.0) * p + 6.0) * p + 4.0) * p + 1.0) * (1.0 / 24.0)

    def slope(p):
        return (((-4.0 * p + 3.0) * p + 3.0) * p + 1.0) * (1.0 / 6.0)

    middle_value = ((((6.0 * u - 12.0) * u - 6.0) * u + 12.0) * u + 11.0) * (1.0 / 24.0)
    middle_slope = (((2.0 * u - 3.0) * u - 1.0) * u + 1.0) * 0.5
    values = [v * v * v * v * (1.0 / 24.0), inner(v), middle_value, inner(u), u * u * u * u * (1.0 / 24.0)]
    slopes = [v * v * v * (-1.0 / 6.0), -slope(v), middle_slope, slope(u), u * u * u * (1.0 / 6.0)]
    return values, slopes


def turn(steps):
    wrapped = steps - GRID * jnp.floor(steps * (1.0 / GRID) + 0.5)
    half = wrapped * (np.pi / GRID)
    square = half * half
    sine = -1.0 / 39916800.0
    for c in (1.0 / 362880.0, -1.0 / 5040.0, 1.0 / 120.0, -1.0 / 6.0, 1.0):
        sine = sine * square + c
    sine = sine * half
    cosine = 1.0 / 479001600.0
    for c in (-1.0 / 3628800.0, 1.0 / 40320.0, -1.0 / 720.0, 1.0 / 24.0, -0.5, 1.0):
        cosine = cosine * square + c
    return 1.0 - 2.0 * sine * sine, 2.0 * sine * cosine


def total_of(x):
    return jnp.sum(jnp.sum(x, axis=0, keepdims=True), axis=1, keepdims=True)


def pick(rows, index):
    return jnp.take_along_axis(rows, index, axis=0, mode="promise_in_bounds")


def iota(shape, dim):
    return lax.broadcasted_iota(jnp.int32, shape, dim)


CONTRACT_LANES = (((1,), (1,)), ((), ()))


def fast_kernel(
    ranks, pos_ref, field_ref, polar_ref, xs_ref, list_ref, count_ref,
    center_ref, eye_ref, zin_ref, zout_ref, xin_ref, xout_ref, yz_ref,
    dip_ref, res_ref,
    lines, info, table, flipped, yq, xw, wt, wz, vx, mix, hold, grid, spec, wide, low, green, tens, cols, place, sides, ext,
    bases, pair, out_part, pair_part, in_part, part, slots, energy,
    local_sem, all_send, all_recv, gram_send, gram_recv, side_send, side_recv,
    ag_send, ag_recv, on_send, on_recv, pair_send, pair_recv, rs_send, rs_recv,
):
    me = lax.axis_index("gx")
    blocks = polar_ref.shape[0]
    planes = GRID // ranks
    kys = GRID // ranks
    halves = blocks // 4
    reach = 2 * HALO_BLK + 1

    def lanes(b):
        return slice(b * TILE, (b + 1) * TILE)

    loads = [
        pltpu.make_async_copy(yz_ref.at[2 * t], lines.at[t], local_sem.at[t]) for t in range(2)
    ]
    for load in loads:
        load.start()

    barrier = pltpu.get_barrier_semaphore()

    def greet_one(d, carry):
        pl.semaphore_signal(
            barrier, inc=1, device_id={"gx": lax.rem(me + d, ranks)}, device_id_type=pl.DeviceIdType.MESH
        )
        return carry

    lax.fori_loop(1, ranks, greet_one, 0)

    for c in range(3):
        for b in range(blocks):
            place[c, b : b + 1, :] = pos_ref[c : c + 1, lanes(b)]
    for c in range(3):
        for b in range(blocks):
            bases[0, c, b : b + 1, :] = field_ref[c : c + 1, lanes(b)]
    for c in range(3):
        info[me, FIELD0 + c] = bases[0, c] / polar_ref[...]
    offset = -1.5
    for k in range(1, ORDER):
        offset = offset + (1.0 * k) * xs_ref[k, 0:1, :]
    for b in range(blocks):
        info[me, 4, b : b + 1, :] = offset[:, lanes(b)]
    with jax.named_scope("yz_wait"):
        for load in loads:
            load.wait()
    marks = iota((GRID, TILE), 0).astype(F32)
    with jax.named_scope("moments"):
        for t in range(2):
            for b in range(blocks):
                line = lines[t, lanes(b), :]
                high = line.astype(BF16)
                rest = line - high.astype(F32)
                mid, tail = split(rest)
                moment = lax.dot_general(
                    center_ref[...], jnp.concatenate([high, mid, tail], axis=1), CONTRACT_LANES,
                    preferred_element_type=F32,
                )
                moment, weight = moment[:GRID], moment[GRID:]
                best = jnp.max(
                    jnp.where((jnp.abs(moment) < 0.5001) & (weight > 0.25), marks, -1.0), axis=0, keepdims=True
                )
                shift = jnp.sum(jnp.where(marks == best, moment, 0.0), axis=0, keepdims=True)
                start = best - 2.0
                info[me, 2 * t, b : b + 1, :] = jnp.where(start < 0, start + GRID, start)
                info[me, 2 * t + 1, b : b + 1, :] = shift + 0.5

    with jax.named_scope("greet_wait"):
        pl.semaphore_wait(barrier, ranks - 1)
    neighbours = [
        pltpu.make_async_remote_copy(
            src_ref=place, dst_ref=sides.at[t], send_sem=side_send.at[t], recv_sem=side_recv.at[t],
            device_id={"gx": lax.rem(me + step, ranks)}, device_id_type=pl.DeviceIdType.MESH,
        )
        for t, step in enumerate((1, ranks - 1))
    ]
    for copy in neighbours:
        copy.start()

    mesh_id = pl.DeviceIdType.MESH
    chips = ranks // 2
    rows_of_chips = chips // 2
    core, chip = lax.rem(me, 2), me // 2
    partner = me + 1 - 2 * core

    def away(d, count):
        step = (d + 1) // 2
        return lax.rem(jnp.where(d % 2 == 1, step, count - step), count)

    def slab_at(d):
        return lax.rem(me + away(d, ranks), ranks)

    def tell_all(i, owner):
        return pltpu.make_async_remote_copy(
            src_ref=info.at[owner], dst_ref=info.at[owner], send_sem=all_send.at[i], recv_sem=all_recv.at[i],
            device_id={"gx": lax.rem(me + i, ranks)}, device_id_type=mesh_id,
        )

    def got_all(d):
        off = away(d, ranks)
        tell_all(lax.rem(ranks - off, ranks), lax.rem(me + off, ranks)).wait_recv()

    def chip_at(d):
        down, side = away(d // 2, rows_of_chips), d % 2
        return lax.rem(chip // 2 + down, rows_of_chips) * 2 + lax.rem(chip % 2 + side, 2)

    def mirrored(d):
        down, side = away(d // 2, rows_of_chips), d % 2
        return lax.rem(rows_of_chips - down, rows_of_chips) * 2 + side

    def forth(d):
        return away(d // 2, rows_of_chips) * 2 + d % 2

    def same(d):
        return 2 * chip_at(d) + core

    def other(d):
        return 2 * chip_at(d) + 1 - core

    def vector(owner):
        return info.at[owner, pl.ds(FIELD0, 3)]

    def direct(d):
        return pltpu.make_async_remote_copy(
            src_ref=vector(me), dst_ref=vector(me), send_sem=ag_send.at[forth(d)], recv_sem=ag_recv.at[forth(d)],
            device_id={"gx": same(d)}, device_id_type=mesh_id,
        )

    def got_direct(d):
        pltpu.make_async_remote_copy(
            src_ref=vector(same(d)), dst_ref=vector(same(d)), send_sem=ag_send.at[mirrored(d)],
            recv_sem=ag_recv.at[mirrored(d)], device_id={"gx": same(d)}, device_id_type=mesh_id,
        ).wait_recv()

    def forward(d, owner):
        return pltpu.make_async_remote_copy(
            src_ref=vector(owner), dst_ref=vector(owner), send_sem=on_send.at[d], recv_sem=on_recv.at[d],
            device_id={"gx": partner}, device_id_type=mesh_id,
        )

    def hand_over(d):
        return pltpu.make_async_remote_copy(
            src_ref=out_part.at[other(d)], dst_ref=pair_part.at[d], send_sem=pair_send.at[d],
            recv_sem=pair_recv.at[d], device_id={"gx": partner}, device_id_type=mesh_id,
        )

    def fold(d):
        return pltpu.make_async_remote_copy(
            src_ref=out_part.at[same(d)], dst_ref=in_part.at[forth(d)], send_sem=rs_send.at[forth(d)],
            recv_sem=rs_recv.at[forth(d)], device_id={"gx": same(d)}, device_id_type=mesh_id,
        )

    def each(low, high, act):
        def one(d, carry):
            act(d)
            return carry

        lax.fori_loop(low, high, one, 0)

    each(1, ranks, lambda d: tell_all(away(d, ranks), me).start())
    def modes(freq):
        number = jnp.where(freq <= GRID // 2, freq, freq - GRID // 2)
        return number.astype(F32), jnp.where((freq == 0) | (freq == GRID // 2), 1.0 / GRID, 2.0 / GRID)

    x_modes, x_weights = modes(iota((GRID, GRID), 0))
    z_modes, z_weights = modes(iota((GRID, GRID), 1))
    flat_sq = x_modes * x_modes + z_modes * z_modes
    flat_weights = x_weights * z_weights

    def filter_one(q, carry):
        y_modes, y_weights = modes(jnp.full((GRID, GRID), me * kys + q, jnp.int32))
        mode_sq = flat_sq + y_modes * y_modes
        safe_sq = jnp.where(mode_sq > 0, mode_sq, 1.0)
        value = jnp.where(mode_sq > 0, RECIP_C * jnp.exp(-DAMP * safe_sq) / safe_sq, 0.0)
        green[q] = value * (flat_weights * y_weights)
        return carry

    with jax.named_scope("filter"):
        lax.fori_loop(0, kys, filter_one, 0)

    def spread_columns(e, rows):
        for c in range(3):
            cols[e, c] = jnp.broadcast_to(rows[c], (TILE, TILE)).T

    def position_columns(e, carry):
        spread_columns(e, [ext[e, c : c + 1, :] for c in range(3)])
        return carry

    for e in range(blocks):
        for c in range(3):
            ext[e + HALO_BLK, c : c + 1, :] = place[c, e : e + 1, :]
    with jax.named_scope("poscols"):
        lax.fori_loop(HALO_BLK, HALO_BLK + blocks, position_columns, 0)
    with jax.named_scope("side_wait"):
        for copy in neighbours:
            copy.wait()
    for e in range(HALO_BLK):
        for c in range(3):
            move = 1.0 * blocks if c == 0 else 0.0
            row = blocks - HALO_BLK + e
            ext[e, c : c + 1, :] = sides[0, c, row : row + 1, :] - move
            ext[blocks + HALO_BLK + e, c : c + 1, :] = sides[1, c, e : e + 1, :] + move
    with jax.named_scope("poscols2"):
        lax.fori_loop(0, HALO_BLK, position_columns, 0)
        lax.fori_loop(HALO_BLK + blocks, 2 * HALO_BLK + blocks, position_columns, 0)
    lag = iota((8, TILE), 1) - iota((8, TILE), 0)

    def tensors(index, carry):
        b, k = index // reach, index % reach
        near = jnp.float32(0.0)
        for s in range(reach):
            near = jnp.where((list_ref[b, s] == b + k) & (s < count_ref[b]), 1.0, near)
        home = [jnp.broadcast_to(ext[b + HALO_BLK, c : c + 1, :], (8, TILE)) for c in range(3)]
        hide = jnp.where(k == HALO_BLK, 0, 4 * TILE)
        for j in range(TILE // 8):
            rows = slice(8 * j, 8 * j + 8)
            r = [home[c] - cols[b + k, c, rows, :] for c in range(3)]
            inverse = lax.rsqrt(r[0] * r[0] + r[1] * r[1] + r[2] * r[2] + 1.0)
            live = jnp.where(lag != 8 * j + hide, near, 0.0)
            square = live * inverse * inverse
            tens[index, 0, rows, :] = PAIR_C * (square * inverse)
            weight = (3.0 * PAIR_C) ** 0.5 * (square * inverse * lax.rsqrt(inverse))
            for c in range(3):
                tens[index, 1 + c, rows, :] = weight * r[c]
        return carry

    with jax.named_scope("tensors"):
        lax.fori_loop(0, blocks * reach, tensors, 0)

    freq = me * kys + iota((kys, TILE), 0)
    sine_mode = freq > GRID // 2
    number = jnp.where(sine_mode, freq - GRID // 2, freq).astype(F32)
    lead_in = jnp.where(sine_mode, GRID // 4, 0).astype(F32)
    shifts = [turn(number * (1.0 * k)) for k in range(ORDER)]

    wz[...] = jnp.zeros_like(wz)

    def beside(ref, at, parts):
        return jnp.concatenate([ref[at, t] for t in parts], axis=1)

    def flip(at):
        for j in range(4):
            both = slice(2 * j * TILE, (2 * j + 2) * TILE)
            turned = lax.dot_general(
                eye_ref[...], beside(table, at, range(2 * j, 2 * j + 2)), CONTRACT_LANES,
                preferred_element_type=F32,
            )
            flipped[at, both, :] = turned.astype(BF16)

    def block_tables(slab, b):
        at, j = slab * halves + b // 4, b % 4
        first = jnp.broadcast_to(info[slab, 0, b : b + 1, :], (kys, TILE))
        cosine, sine = turn(number * first - lead_in)
        for t in range(2):
            rows = [wt[ORDER * t + k, b : b + 1, :] for k in range(ORDER)]
            real = combine([s[0] for s in shifts], rows)
            imag = combine([s[1] for s in shifts], rows)
            yq[slab * blocks + b, t] = cosine * real - sine * imag
        begin = jnp.broadcast_to(info[slab, 2, b : b + 1, :], (8, TILE)).astype(jnp.int32)
        for i in range(GRID // 16):
            gaps = [
                jnp.minimum((iota((8, TILE), 0) + (16 * i + 8 * r - begin)) & (GRID - 1), 7)
                for r in range(2)
            ]
            for t in range(2):
                dense = jnp.concatenate([pick(wz[t, b], gap) for gap in gaps], axis=0)
                high, rest = split(dense)
                table[at, 2 * j + t, 16 * i : 16 * i + 16, :] = high
                table[at, 2 * j + t, GRID + 16 * i : GRID + 16 * i + 16, :] = rest

    def slab_tables(d, carry):
        with jax.named_scope("info_wait"):
            @pl.when(d > 0)
            def _():
                got_all(d)

        slab = slab_at(d)
        values, slopes = spline_rows(info[slab, 4])
        for k in range(ORDER):
            xw[slab, k] = values[k]
            xw[slab, ORDER + k] = slopes[k]
        for t in range(2):
            values, slopes = spline_rows(info[slab, 2 * t + 1])
            for k in range(ORDER):
                if t == 0:
                    wt[k] = values[k]
                    wt[ORDER + k] = slopes[k]
                else:
                    for b in range(blocks):
                        wz[0, b, k : k + 1, :] = values[k][b : b + 1, :]
                        wz[1, b, k : k + 1, :] = slopes[k][b : b + 1, :]

        before = slab_at(jnp.maximum(d - 1, 0)) * halves + halves - 1
        with jax.named_scope("tables"):
            for h in range(halves):
                flip(before if h == 0 else slab * halves + h - 1)
                for j in range(4):
                    block_tables(slab, 4 * h + j)
        return carry

    lax.fori_loop(0, ranks, slab_tables, 0)
    flip(slab_at(ranks - 1) * halves + halves - 1)
    each(1, ranks, lambda i: tell_all(i, me).wait_send())

    def weigh(slab, slot):
        v = [info[slab, FIELD0 + c] for c in range(3)]
        for k in range(ORDER):
            x, dx = xw[slab, k], xw[slab, ORDER + k]
            vx[slot, k] = v[0] * dx
            vx[slot, ORDER + k] = v[1] * x
            vx[slot, 2 * ORDER + k] = v[2] * x
        for h in range(halves):
            for j in range(4):
                b = 4 * h + j
                y, dy = yq[slab * blocks + b, 0], yq[slab * blocks + b, 1]
                none = jnp.zeros((kys, TILE), F32)
                lead, tail = [none] * 8, [none] * 8
                for k in range(ORDER):
                    lead[j + k] = vx[slot, k, b : b + 1, :] * y + vx[slot, ORDER + k, b : b + 1, :] * dy
                    tail[j + k] = vx[slot, 2 * ORDER + k, b : b + 1, :] * y
                for t, pieces in enumerate((lead, tail)):
                    high, rest = split(jnp.concatenate(pieces, axis=0))
                    mix[slot, h, : 8 * kys, lanes(2 * j + t)] = high
                    mix[slot, h, 8 * kys :, lanes(2 * j + t)] = rest

    def window(slab, h):
        return pl.ds(pl.multiple_of((slab * planes + 4 * h) * kys, 4 * kys), 8 * kys)

    def spread_slab(slab, slot):
        count = 8 * kys
        for h in range(halves):
            sums = dot(mix[slot, h], flipped[slab * halves + h])
            grid[window(slab, h), :] += sums[:count, :GRID] + sums[:count, GRID:] + sums[count:, :GRID]

    def read_slab(slab, slot):
        for h in range(halves):
            at = window(slab, h)
            high, rest = wide[at, :], low[at, :]
            left = jnp.concatenate(
                [jnp.concatenate([high, rest], axis=0), jnp.concatenate([high, jnp.zeros_like(rest)], axis=0)],
                axis=1,
            )
            hold[slot, h] = dot(left, beside(table, slab * halves + h, range(8)))

    def gather_slab(slab, slot):
        count = 8 * kys
        for h in range(halves):
            for j in range(4):
                b = 4 * h + j
                one = two = three = 0.0
                for k in range(ORDER):
                    rows = slice((j + k) * kys, (j + k + 1) * kys)
                    more = slice(count + (j + k) * kys, count + (j + k + 1) * kys)
                    plain = hold[slot, h, rows, lanes(2 * j)] + hold[slot, h, more, lanes(2 * j)]
                    tilted = hold[slot, h, rows, lanes(2 * j + 1)] + hold[slot, h, more, lanes(2 * j + 1)]
                    x, dx = xw[slab, k, b : b + 1, :], xw[slab, ORDER + k, b : b + 1, :]
                    one += dx * plain
                    two += x * plain
                    three += x * tilted
                y, dy = yq[slab * blocks + b, 0], yq[slab * blocks + b, 1]
                for c, term in enumerate((y * one, dy * two, y * three)):
                    out_part[slab, c, b : b + 1, :] = jnp.sum(term, axis=0, keepdims=True)

    count = ITERS + 1
    entries = {}
    for i in range(ITERS):
        for j in range(i, ITERS):
            entries[i, j] = entries[j, i] = len(set(entries.values()))
    last = len(set(entries.values()))
    for i in range(ITERS - 1):
        entries[i, ITERS] = entries[i + 1, ITERS - 1]
    entries[ITERS - 1, ITERS] = last

    def tell(i, row):
        return pltpu.make_async_remote_copy(
            src_ref=part, dst_ref=slots.at[lax.rem(me + row, ranks)], send_sem=gram_send.at[i],
            recv_sem=gram_recv.at[i], device_id={"gx": lax.rem(me + i, ranks)},
            device_id_type=pl.DeviceIdType.MESH,
        )

    def send_products():
        column = iota((1, TILE), 1)
        packed = jnp.zeros((1, TILE), F32)
        for i in range(ITERS):
            for j in range(i, ITERS):
                value = 0.0
                for c in range(3):
                    value += bases[i, c] * (bases[j, c] / polar_ref[...])
                packed = jnp.where(column == entries[i, j], total_of(value), packed)
        value = 0.0
        for c in range(3):
            value += pair[c] * info[me, FIELD0 + c]
        packed = jnp.where(column == last, total_of(value) - total_of(energy[...]), packed)
        part[...] = packed
        slots[me] = packed

        def one(i, carry):
            tell(i, 0).start()
            return carry

        lax.fori_loop(1, ranks, one, 0)

    def vector_columns(n):
        n = jnp.minimum(n, blocks + 2 * HALO_BLK - 1)
        e = jnp.where(n < blocks, n + HALO_BLK, jnp.where(n < blocks + HALO_BLK, n - blocks, n))
        step = jnp.where(e < HALO_BLK, ranks - 1, jnp.where(e < HALO_BLK + blocks, 0, 1))
        slab = lax.rem(me + step, ranks)
        row = lax.rem(e + blocks - HALO_BLK, blocks)
        spread_columns(e, [info[slab, FIELD0 + c, pl.ds(row, 1), :] for c in range(3)])

    def pair_rows(b, low, high, fresh):
        def one_source(k, sums):
            sums = list(sums)
            for j in range(TILE // 8):
                rows = slice(8 * j, 8 * j + 8)
                v = [cols[b + k, c, rows, :] for c in range(3)]
                w = [tens[b * reach + k, 1 + c, rows, :] for c in range(3)]
                third = tens[b * reach + k, 0, rows, :]
                along = w[0] * v[0] + w[1] * v[1] + w[2] * v[2]
                for c in range(3):
                    sums[c] = sums[c] + third * v[c]
                    sums[3 + c] = sums[3 + c] + along * w[c]
            return tuple(sums)

        sums = lax.fori_loop(low, high, one_source, (jnp.zeros((8, TILE), F32),) * 6)
        for c in range(3):
            value = jnp.sum(sums[c] - sums[3 + c], axis=0, keepdims=True)
            if fresh:
                pair[c, pl.ds(b, 1), :] = value
            else:
                pair[c, pl.ds(b, 1), :] += value

    def pair_own():
        each(0, blocks, lambda b: pair_rows(
            b, jnp.maximum(HALO_BLK - b, 0), jnp.minimum(blocks + HALO_BLK - b, reach), True
        ))

    def pair_edges():
        each(0, HALO_BLK, lambda b: pair_rows(b, 0, HALO_BLK - b, False))
        each(blocks - HALO_BLK, blocks, lambda b: pair_rows(b, blocks + HALO_BLK - b, reach, False))

    def sweep(it, carry):
        @pl.when(it > 0)
        def _():
            forward(0, me).start()
            each(1, chips, lambda d: direct(d).start())

        grid[...] = jnp.zeros_like(grid)

        def pass_on(d):
            got_direct(d)
            forward(d, same(d)).start()

        def spread_two(m, inner):
            following = jnp.minimum(m + 1, chips - 1)
            with jax.named_scope("far_wait"):

                @pl.when((it > 0) & (m + 2 < chips))
                def _():
                    pass_on(m + 2)

                @pl.when(it > 0)
                def _():
                    forward(m, other(m)).wait_recv()

            with jax.named_scope("spread"):
                weigh(other(m), 1)
                spread_slab(same(m), 0)
                first = jnp.where(m < blocks // 2, 2 * m, jnp.maximum(2 * m - 2, blocks - 2))
                for n in (first, first + 1):
                    vector_columns(n)
                weigh(same(following), 0)
                spread_slab(other(m), 1)
            return inner

        weigh(me, 0)

        @pl.when(it == ITERS - 1)
        def _():
            with jax.named_scope("pair"):
                each(0, blocks, vector_columns)
                pair_own()

        with jax.named_scope("near_wait"):

            @pl.when(it > 0)
            def _():
                pass_on(1)

        lax.fori_loop(0, chips, spread_two, 0)

        @pl.when(it > 0)
        def _():
            forward(0, me).wait_send()
            each(1, chips, lambda d: forward(d, same(d)).wait_send())

        @pl.when(it == ITERS - 1)
        def _():
            with jax.named_scope("pair"):
                pair_edges()

        with jax.named_scope("fold"):
            size = GRID * kys
            edge = 2 * kys
            grid[size : size + edge, :] += grid[0:edge, :]
            grid[edge : 2 * edge, :] += grid[size + edge : size + 2 * edge, :]

        step = 2 * GRID
        with jax.named_scope("zin"):
            for i in range(size // step):
                high, rest = split(grid[edge + i * step : edge + (i + 1) * step, :])
                sums = dot(jnp.concatenate([high, rest], axis=1), zin_ref[...])
                spec[i * step : (i + 1) * step, :] = sums[:, :GRID] + sums[:, GRID:]
        with jax.named_scope("xinout"):
            power = jnp.zeros((8, GRID), F32)
            for q in range(0, kys, 2):
                pairs = [pl.ds(q, GRID, stride=kys), pl.ds(q + 1, GRID, stride=kys)]
                high, rest = split(jnp.concatenate([spec[s, :] for s in pairs], axis=1))
                line = dot(xin_ref[...], jnp.concatenate([high, rest, high], axis=0))
                passed = line * jnp.concatenate([green[q], green[q + 1]], axis=1)
                worth = line * passed
                power += jnp.sum((worth[:, :GRID] + worth[:, GRID:]).reshape(GRID // 8, 8, GRID), axis=0)
                line = passed
                high, rest = split(line)
                line = dot(xout_ref[...], jnp.concatenate([high, rest, high], axis=0))
                spec[pairs[0], :] = line[:, :GRID]
                spec[pairs[1], :] = line[:, GRID:]
            energy[...] = power

        @pl.when(it == ITERS - 1)
        def _():
            with jax.named_scope("gram"):
                send_products()
        with jax.named_scope("zout"):
            for i in range(size // step):
                high, rest = split(spec[i * step : (i + 1) * step, :])
                sums = dot(jnp.concatenate([high, rest], axis=1), zout_ref[...])
                high, rest = split(sums[:, :GRID] + sums[:, GRID:])
                rows = slice(edge + i * step, edge + (i + 1) * step)
                wide[rows, :] = high
                low[rows, :] = rest
            for ref in (wide, low):
                ref[0:edge, :] = ref[size : size + edge, :]
                ref[size + edge : size + 2 * edge, :] = ref[edge : 2 * edge, :]

        def turn_of(t):
            d = chips - 1 - lax.rem(t, chips)
            return 2 * chip_at(d) + jnp.where(t < chips, 1 - core, core)

        def gather_two(m, inner):
            with jax.named_scope("gather"):
                read_slab(turn_of(2 * m + 1), 1)
                gather_slab(turn_of(2 * m), 0)
                read_slab(turn_of(jnp.minimum(2 * m + 2, ranks - 1)), 0)
                gather_slab(turn_of(2 * m + 1), 1)
            for t in (2 * m, 2 * m + 1):
                d = chips - 1 - lax.rem(t, chips)

                @pl.when(t < chips)
                def _(d=d):
                    hand_over(d).start()

                @pl.when(t >= chips)
                def _(d=d):
                    hand_over(d).wait_recv()
                    for c in range(3):
                        out_part[same(d), c] += pair_part[d, c]

                @pl.when((t >= chips) & (d > 0))
                def _(d=d):
                    fold(d).start()

            return inner

        read_slab(turn_of(0), 0)
        lax.fori_loop(0, chips, gather_two, 0)

        @pl.when(it < ITERS - 1)
        def _():
            with jax.named_scope("pair"):
                pair_own()
                pair_edges()

        @pl.when(it > 0)
        def _():
            each(1, chips, lambda d: direct(d).wait_send())

        each(0, chips, lambda d: hand_over(d).wait_send())
        with jax.named_scope("rs_wait"):
            each(1, chips, lambda d: fold(d).wait())
        with jax.named_scope("update"):
            for c in range(3):
                total = out_part[me, c]
                for i in range(1, chips):
                    total = total + in_part[i, c]
                following = pair[c] - total
                bases[it + 1, c] = following
                info[me, FIELD0 + c] = following / polar_ref[...]
        return carry

    lax.fori_loop(0, ITERS, sweep, 0)

    def tell_wait(i, carry):
        tell(i, ranks - i).wait()
        return carry

    with jax.named_scope("gram_wait"):
        lax.fori_loop(1, ranks, tell_wait, 0)
    sums = jnp.sum(slots[...], axis=0)
    sums = {r: jnp.broadcast_to(sums[:, r : r + 1], (1, TILE)) for r in range(last + 1)}
    dipoles, residual = krylov(sums, entries, count)
    for c in range(3):
        basis = [bases[i, c] for i in range(count)]
        first = combine(dipoles, [b / polar_ref[...] for b in basis])
        second = combine(residual, basis)
        for b in range(blocks):
            dip_ref[c : c + 1, lanes(b)] = first[b : b + 1, :]
            res_ref[c : c + 1, lanes(b)] = second[b : b + 1, :]


def krylov(sums, place, count):
    def inner(x, y):
        value = None
        for i in range(count):
            for j in range(count):
                if x[i] is not None and y[j] is not None:
                    row = place[i, j]
                    term = x[i] * y[j] * sums[row]
                    value = term if value is None else value + term
        return value

    none = [None] * (count - 1)
    residual = [jnp.ones((1, TILE), F32)] + none
    direction = list(residual)
    dipoles = [None] * count
    rz_now = inner(residual, residual)
    for sweep in range(ITERS):
        image = scaled(-1.0, direction, [None] + direction[:-1])
        step = rz_now / inner(direction, image)
        dipoles = scaled(step, dipoles, direction)
        residual = scaled(-step, residual, image)
        if sweep + 1 < ITERS:
            rz_next = inner(residual, residual)
            direction = scaled(rz_next / rz_now, residual, direction)
            rz_now = rz_next
    return dipoles, residual


def fast_shapes(ranks, blocks):
    kys = GRID // ranks
    ext_blocks = blocks + 2 * HALO_BLK
    rows = (GRID + 4) * kys
    dma = pltpu.SemaphoreType.DMA
    tile = (blocks, TILE)
    buffers = [
        ((2, blocks * TILE, GRID), F32),
        ((ranks, 8) + tile, F32),
        ((ranks * blocks // 4, 8, 2 * GRID, TILE), BF16),
        ((ranks * blocks // 4, 8 * TILE, 2 * GRID), BF16),
        ((ranks * blocks, 2, kys, TILE), F32),
        ((ranks, 2 * ORDER) + tile, F32),
        ((2 * ORDER,) + tile, F32),
        ((2, blocks, 8, TILE), F32),
        ((2, 3 * ORDER) + tile, F32),
        ((2, blocks // 4, 16 * kys, 8 * TILE), BF16),
        ((2, blocks // 4, 16 * kys, 8 * TILE), F32),
        ((rows, GRID), F32),
        ((GRID * kys, GRID), F32),
        ((rows, GRID), BF16),
        ((rows, GRID), BF16),
        ((kys, GRID, GRID), F32),
        ((blocks * (2 * HALO_BLK + 1), 4, TILE, TILE), F32),
        ((ext_blocks, 3, TILE, TILE), F32),
        ((3,) + tile, F32),
        ((2, 3) + tile, F32),
        ((ext_blocks, 8, TILE), F32),
        ((ITERS + 1, 3) + tile, F32),
        ((3,) + tile, F32),
        ((ranks, 3) + tile, F32),
        ((ranks // 2, 3) + tile, F32),
        ((ranks // 2, 3) + tile, F32),
        ((1, TILE), F32),
        ((ranks, 1, TILE), F32),
        ((8, GRID), F32),
    ]
    sems = [dma((2,))] + [dma((ranks,))] * 4 + [dma((2,))] * 2 + [dma((ranks // 2,))] * 8
    return buffers, sems


def fits_fast(ranks, blocks):
    if blocks != 8 or GRID % ranks or GRID // ranks != blocks:
        return False
    buffers, _ = fast_shapes(ranks, blocks)
    return sum(int(np.prod(s)) * np.dtype(t).itemsize for s, t in buffers) < 60 * 1024 * 1024


def halves_of(x):
    high = x.astype(BF16)
    return high, (x - high.astype(np.float32)).astype(BF16)


def fast_device(positions, field, inv_polar, x_spline, yz_spline, tile_list, tile_count):
    ranks = lax.axis_size("gx")
    atoms_here = positions.shape[1]
    blocks = atoms_here // TILE
    line = np.arange(GRID)
    center = (line[None, :] - line[:, None] + GRID // 2) % GRID - GRID // 2
    center = np.concatenate([center, np.eye(GRID)], axis=0)
    center = np.concatenate([center.astype(np.float32).astype(BF16)] * 3, axis=1)
    rows = fixed_rows(line)

    def along_z(m):
        high, rest = halves_of(np.ascontiguousarray(m))
        return np.concatenate(
            [np.concatenate([high, rest], axis=1), np.concatenate([high, np.zeros_like(rest)], axis=1)], axis=0
        )

    def along_x(m):
        high, rest = halves_of(np.ascontiguousarray(m))
        return np.concatenate([high, high, rest], axis=1)

    eye = np.eye(2 * TILE, dtype=np.float32).astype(BF16)
    constants = [center, eye, along_z(rows.T), along_z(rows), along_x(rows), along_x(rows.T)]
    buffers, sems = fast_shapes(ranks, blocks)
    smem = pl.BlockSpec(memory_space=pltpu.SMEM)
    outs = pl.pallas_call(
        functools.partial(fast_kernel, ranks),
        in_specs=[VMEM] * 4 + [smem] * 2 + [VMEM] * len(constants) + [pl.BlockSpec(memory_space=pl.ANY)],
        out_specs=[VMEM] * 2,
        out_shape=[jax.ShapeDtypeStruct(positions.shape, F32)] * 2,
        scratch_shapes=[pltpu.VMEM(s, t) for s, t in buffers] + sems,
        compiler_params=pltpu.CompilerParams(
            vmem_limit_bytes=62 * 1024 * 1024, collective_id=2, has_side_effects=True
        ),
        name="induced",
    )(
        positions, field, inv_polar.reshape(blocks, TILE), x_spline.transpose(1, 0, 2),
        tile_list, tile_count, *[jnp.asarray(c) for c in constants], yz_spline,
    )
    return pl.pallas_call(
        finish_kernel,
        in_specs=[VMEM] * 2,
        out_specs=[VMEM] * 2,
        out_shape=[jax.ShapeDtypeStruct(positions.shape, F32)] * 2,
        name="finish",
    )(*outs)


def finish_kernel(dipoles_in, residual_in, dipoles_out, residual_out):
    dipoles_out[...] = dipoles_in[...]
    residual_out[...] = residual_in[...]


def solution(mesh):
    placed = (
        P(None, ("rep", "gx")),
        P(None, ("rep", "gx")),
        P(("rep", "gx")),
        P(None, None, ("rep", "gx")),
        P(None, ("rep", "gx"), None),
        P(("rep", "gx"), None),
        P(("rep", "gx")),
    )
    ranks = mesh.shape["gx"]

    def choose(*arrays):
        device = fast_device if fits_fast(ranks, arrays[0].shape[1] // TILE) else per_device
        return device(*arrays)

    return jax.shard_map(
        choose,
        mesh=mesh,
        in_specs=placed,
        out_specs=(P(None, ("rep", "gx")), P(None, ("rep", "gx"))),
        check_vma=False,
    )
```

```python
import jax
import jax.numpy as jnp
from jax import lax
from jax.experimental import pallas as pl
from jax.experimental.pallas import tpu as pltpu
from jax.sharding import PartitionSpec as P
import functools
import numpy as np

GRID = 128
ORDER = 5
TILE = 128
HALO_BLK = 3
ITERS = 3


PAIR_C = 0.025
RECIP_C = 8192.0
DAMP = 0.0008
EXACT = lax.Precision.HIGHEST


def mode_of(freq, size):
    half_size = size // 2
    mode_num = jnp.where(freq <= half_size, freq, freq - half_size)
    weight = jnp.where((freq == 0) | (freq == half_size), 1.0 / size, 2.0 / size)
    return (mode_num.astype(jnp.float32), weight.astype(jnp.float32))


def basis_rows(size, points):
    freq = jnp.arange(size, dtype=jnp.int32)
    half_size = size // 2
    mode_num = jnp.where(freq <= half_size, freq, freq - half_size)
    phase = mode_num[:, None] * points[None, :] % size
    angle = phase.astype(jnp.float32) * (2.0 * jnp.pi / size)
    return jnp.where((freq <= half_size)[:, None], jnp.cos(angle), jnp.sin(angle))


def kernel_block(x_modes, x_weights, y_modes, y_weights, z_modes, z_weights):
    mode_sq = (
        x_modes[:, None, None] * x_modes[:, None, None]
        + y_modes[None, :, None] * y_modes[None, :, None]
        + z_modes[None, None, :] * z_modes[None, None, :]
    )
    safe_sq = jnp.where(mode_sq > 0, mode_sq, 1.0)
    green = jnp.where(mode_sq > 0, RECIP_C * jnp.exp(-DAMP * safe_sq) / safe_sq, 0.0)
    return green * x_weights[:, None, None] * y_weights[None, :, None] * z_weights[None, None, :]


F32 = jnp.float32
BF16 = jnp.bfloat16
VMEM = pl.BlockSpec(memory_space=pltpu.VMEM)


def split(x):
    high = x.astype(BF16)
    return high, (x - high.astype(F32)).astype(BF16)


def dot(a, b):
    return jnp.dot(a, b, preferred_element_type=F32)


def params(**more):
    return pltpu.CompilerParams(vmem_limit_bytes=56 * 1024 * 1024, **more)


def prep_kernel(yz_ref, rows_ref, yft_ref, zf_ref, zft_ref):
    rows = jnp.concatenate(split(rows_ref[...]), axis=0)

    def transformed(t):
        high, low = split(jnp.concatenate([yz_ref[t], yz_ref[t + 1]], axis=0))
        contract = (((1,), (1,)), ((), ()))
        wide = lax.dot_general(rows, high, contract, preferred_element_type=F32)
        more = lax.dot_general(rows[:GRID], low, contract, preferred_element_type=F32)
        return wide[:GRID] + wide[GRID:] + more

    lines = transformed(0)
    yft_ref[0, 0] = lines[:, :TILE]
    yft_ref[0, 1] = lines[:, TILE:]
    lines = transformed(2)
    zft_ref[0] = jnp.concatenate(split(lines), axis=0)
    zf_ref[0] = jnp.concatenate(split(lines.T), axis=1)


def prepare(yz_spline, rows, blocks):
    return pl.pallas_call(
        prep_kernel,
        grid=(blocks,),
        in_specs=[
            pl.BlockSpec((4, TILE, GRID), lambda b: (0, b, 0)),
            pl.BlockSpec((GRID, GRID), lambda b: (0, 0)),
        ],
        out_specs=[
            pl.BlockSpec((1, 2, GRID, TILE), lambda b: (b, 0, 0, 0)),
            pl.BlockSpec((1, 2 * TILE, 2 * GRID), lambda b: (b, 0, 0)),
            pl.BlockSpec((1, 2 * GRID, 2 * TILE), lambda b: (b, 0, 0)),
        ],
        out_shape=[
            jax.ShapeDtypeStruct((blocks, 2, GRID, TILE), F32),
            jax.ShapeDtypeStruct((blocks, 2 * TILE, 2 * GRID), BF16),
            jax.ShapeDtypeStruct((blocks, 2 * GRID, 2 * TILE), BF16),
        ],
        compiler_params=params(),
        name="prep",
    )(yz_spline, rows)


def spread_kernel(planes, ky_count, pv_ref, xs_ref, yft_ref, zf_ref, out_ref):
    blocks = pv_ref.shape[0]
    ranks = out_ref.shape[0]
    out_ref[...] = jnp.zeros_like(out_ref)

    def one_block(b, carry):
        base = b * planes // blocks
        y, dy = yft_ref[b, 0], yft_ref[b, 1]
        v0, v1, v2 = (pv_ref[b, 3 + c : 4 + c, :] for c in range(3))
        highs, lows = [], []
        for k in range(ORDER):
            x, dx = xs_ref[b, k : k + 1, :], xs_ref[b, ORDER + k : ORDER + k + 1, :]
            lead = (v0 * dx) * y + (v1 * x) * dy
            high, low = split(jnp.concatenate([lead, (v2 * x) * y], axis=1))
            highs.append(high)
            lows.append(low)
        weights = zf_ref[b]
        wide = dot(jnp.concatenate(highs, axis=0), weights)
        total = (
            wide[:, :GRID] + wide[:, GRID:] + dot(jnp.concatenate(lows, axis=0), weights[:, :GRID])
        )
        for k in range(ORDER):
            part = total[k * GRID : (k + 1) * GRID].reshape(ranks, ky_count, GRID)
            out_ref[:, base + k, :ky_count, :] += part
        return carry

    lax.fori_loop(0, blocks, one_block, 0)


def gather_kernel(
    planes, ky_count, ret_ref, xs_ref, yft_ref, zft_ref, pair_ref, pv_ref, polar_ref,
    next_ref, pv_next_ref, wide_ref, low_ref,
):
    blocks = xs_ref.shape[0]
    extent = ret_ref.shape[1]
    for p in range(extent):
        high, low = split(ret_ref[:, p, :ky_count, :].reshape(GRID, GRID))
        wide_ref[p] = jnp.concatenate([high, high], axis=1)
        low_ref[p] = low

    def one_block(b, carry):
        base = b * planes // blocks
        weights = zft_ref[b]
        wide = wide_ref[pl.ds(base, ORDER)].reshape(ORDER * GRID, 2 * GRID)
        low = low_ref[pl.ds(base, ORDER)].reshape(ORDER * GRID, GRID)
        sums = dot(wide, weights) + dot(low, weights[:GRID])
        one = two = three = 0.0
        for k in range(ORDER):
            x, dx = xs_ref[b, k : k + 1, :], xs_ref[b, ORDER + k : ORDER + k + 1, :]
            plain = sums[k * GRID : (k + 1) * GRID, :TILE]
            one += dx * plain
            two += x * plain
            three += x * sums[k * GRID : (k + 1) * GRID, TILE:]
        y, dy = yft_ref[b, 0], yft_ref[b, 1]
        far = jnp.concatenate(
            [jnp.sum(t, axis=0, keepdims=True) for t in (y * one, dy * two, y * three)], axis=0
        )
        following = pair_ref[b] - far
        next_ref[b] = following
        pv_next_ref[b, 0:3] = pv_ref[b, 0:3]
        pv_next_ref[b, 3:6] = following / polar_ref[b]
        pv_next_ref[b, 6:8] = jnp.zeros((2, TILE), F32)
        return carry

    lax.fori_loop(0, blocks, one_block, 0)


def pair_sum(near_ref, pv_ref, before_ref, after_ref, out_ref, ext_ref, col_ref):
    blocks = pv_ref.shape[0]
    reach = 2 * HALO_BLK + 1
    first_row = lax.broadcasted_iota(jnp.int32, (HALO_BLK, 8, TILE), 1) == 0
    ext_ref[:HALO_BLK] = before_ref[...] + jnp.where(first_row, -1.0 * blocks, 0.0)
    ext_ref[HALO_BLK : HALO_BLK + blocks] = pv_ref[...]
    ext_ref[HALO_BLK + blocks :] = after_ref[...] + jnp.where(first_row, 1.0 * blocks, 0.0)
    lag = lax.broadcasted_iota(jnp.int32, (8, TILE), 1) - lax.broadcasted_iota(
        jnp.int32, (8, TILE), 0
    )

    def spread_columns(e, carry):
        for c in range(6):
            col_ref[e, c] = jnp.broadcast_to(ext_ref[e, c : c + 1, :], (TILE, TILE)).T
        return carry

    lax.fori_loop(0, blocks + 2 * HALO_BLK, spread_columns, 0)

    def one_home(b, carry):
        home = [jnp.broadcast_to(pv_ref[b, c : c + 1, :], (8, TILE)) for c in range(3)]

        def one_source(k, sums):
            shift = jnp.where(k == HALO_BLK, 0, 4 * TILE)
            direct = [jnp.zeros((8, TILE), F32) for c in range(3)]
            tilted = [jnp.zeros((8, TILE), F32) for c in range(3)]
            for j in range(TILE // 8):
                rows = slice(8 * j, 8 * j + 8)
                r = [home[c] - col_ref[b + k, c, rows, :] for c in range(3)]
                v = [col_ref[b + k, 3 + c, rows, :] for c in range(3)]
                inverse = lax.rsqrt(r[0] * r[0] + r[1] * r[1] + r[2] * r[2] + 1.0)
                inverse = jnp.where(lag != 8 * j + shift, inverse, 0.0)
                square = inverse * inverse
                third = square * inverse
                weight = third * square * (r[0] * v[0] + r[1] * v[1] + r[2] * v[2])
                for c in range(3):
                    direct[c] += third * v[c]
                    tilted[c] += weight * r[c]
            near = near_ref[b * reach + k]
            return tuple(
                sums[c] + near * (direct[c] - 3.0 * tilted[c]) for c in range(3)
            )

        sums = lax.fori_loop(0, reach, one_source, (jnp.zeros((8, TILE), F32),) * 3)
        out_ref[b] = PAIR_C * jnp.concatenate(
            [jnp.sum(t, axis=0, keepdims=True) for t in sums], axis=0
        )
        return carry

    lax.fori_loop(0, blocks, one_home, 0)


def greet(ranks, me):
    barrier = pltpu.get_barrier_semaphore()

    def signal(d, carry):
        pl.semaphore_signal(
            barrier,
            inc=1,
            device_id={"gx": lax.rem(me + d, ranks)},
            device_id_type=pl.DeviceIdType.MESH,
        )
        return carry

    lax.fori_loop(1, ranks, signal, 0)
    pl.semaphore_wait(barrier, ranks - 1)


def exchange(ranks, me, source, target, local_sem, send_sem, recv_sem):
    def copy(d, slot):
        peer = lax.rem(me + d, ranks)
        return pltpu.make_async_remote_copy(
            src_ref=source(peer),
            dst_ref=target(slot),
            send_sem=send_sem.at[d],
            recv_sem=recv_sem.at[d],
            device_id={"gx": peer},
            device_id_type=pl.DeviceIdType.MESH,
        )

    def start(d, carry):
        copy(d, me).start()
        return carry

    def finish(d, carry):
        copy(d, lax.rem(me - d + ranks, ranks)).wait()
        return carry

    lax.fori_loop(1, ranks, start, 0)
    own = pltpu.make_async_copy(source(me), target(me), local_sem)
    own.start()

    def wait():
        own.wait()
        lax.fori_loop(1, ranks, finish, 0)

    return wait


def middle_kernel(
    ranks, ky_count, near_ref, spec_ref, pv_ref, green_ref, across_ref, back_ref,
    ret_ref, pair_ref,
    before_ref, after_ref, ext_ref, col_ref, recv_ref, done_ref, local_sems, send1, recv1, send2, recv2, halo_send, halo_recv,
):
    me = lax.axis_index("gx")
    blocks = pv_ref.shape[0]
    extent = spec_ref.shape[1]
    rows = ranks * extent
    greet(ranks, me)
    halos = []
    for t, (piece, into, step) in enumerate(
        (
            (pv_ref.at[pl.ds(blocks - HALO_BLK, HALO_BLK)], before_ref, 1),
            (pv_ref.at[pl.ds(0, HALO_BLK)], after_ref, ranks - 1),
        )
    ):
        halos.append(
            pltpu.make_async_remote_copy(
                src_ref=piece,
                dst_ref=into,
                send_sem=halo_send.at[t],
                recv_sem=halo_recv.at[t],
                device_id={"gx": lax.rem(me + step, ranks)},
                device_id_type=pl.DeviceIdType.MESH,
            )
        )
        halos[-1].start()
    wait = exchange(
        ranks, me, lambda d: spec_ref.at[d], lambda d: recv_ref.at[d], local_sems.at[0], send1, recv1
    )
    across_high, across_low = split(across_ref[...])
    back_high, back_low = split(back_ref[...])
    wait()
    lines_in = recv_ref.reshape(rows * 8, GRID)
    lines_out = done_ref.reshape(rows * 8, GRID)
    for q in range(ky_count):
        high, low = split(lines_in[pl.ds(q, rows, stride=8), :])
        wide = dot(across_high, jnp.concatenate([high, low], axis=1))
        line = wide[:, :GRID] + wide[:, GRID:] + dot(across_low, high)
        high, low = split(line * green_ref[q])
        wide = dot(back_high, jnp.concatenate([high, low], axis=1))
        lines_out[pl.ds(q, rows, stride=8), :] = (
            wide[:, :GRID] + wide[:, GRID:] + dot(back_low, high)
        )
    wait = exchange(
        ranks, me, lambda d: done_ref.at[d], lambda d: ret_ref.at[d], local_sems.at[1], send2, recv2
    )
    for halo in halos:
        halo.wait()
    pair_sum(near_ref, pv_ref, before_ref, after_ref, pair_ref, ext_ref, col_ref)
    wait()


def middle(near, spec, pv, green, across, back, ranks, ky_count):
    dma = pltpu.SemaphoreType.DMA
    blocks = pv.shape[0]
    halo = pltpu.VMEM((HALO_BLK, 8, TILE), F32)
    return pl.pallas_call(
        functools.partial(middle_kernel, ranks, ky_count),
        in_specs=[pl.BlockSpec(memory_space=pltpu.SMEM)] + [VMEM] * 5,
        out_specs=[VMEM] * 2,
        out_shape=[
            jax.ShapeDtypeStruct(spec.shape, F32),
            jax.ShapeDtypeStruct((blocks, 3, TILE), F32),
        ],
        scratch_shapes=[
            halo,
            halo,
            pltpu.VMEM((blocks + 2 * HALO_BLK, 8, TILE), F32),
            pltpu.VMEM((blocks + 2 * HALO_BLK, 6, TILE, TILE), F32),
            pltpu.VMEM(spec.shape, F32),
            pltpu.VMEM(spec.shape, F32),
            dma((2,)), dma((ranks,)), dma((ranks,)), dma((ranks,)), dma((ranks,)),
            dma((2,)), dma((2,)),
        ],
        compiler_params=params(collective_id=0, has_side_effects=True),
        name="middle",
    )(near, spec, pv, green, across, back)


def combine(weights, parts):
    terms = [w * p for w, p in zip(weights, parts) if w is not None]
    return functools.reduce(jnp.add, terms)


def scaled(a, x, y):
    pairs = zip(x, y)
    return [p if q is None else (a * q if p is None else p + a * q) for p, q in pairs]


def solve_kernel(
    ranks, b0_ref, b1_ref, b2_ref, b3_ref, polar_ref,
    dipoles_ref, residual_ref, part_ref, slots, local_sem, send_sem, recv_sem,
):
    me = lax.axis_index("gx")
    bases = [ref[...] for ref in (b0_ref, b1_ref, b2_ref, b3_ref)]
    soft = [b / polar_ref[...] for b in bases]
    count = ITERS + 1
    place = {}
    part_ref[...] = jnp.zeros_like(part_ref)
    for i in range(count):
        for j in range(i, count):
            place[i, j] = place[j, i] = row = len(set(place.values()))
            part_ref[row : row + 1] = jnp.sum(
                jnp.sum(bases[i] * soft[j], axis=0), axis=0, keepdims=True
            )
    greet(ranks, me)
    wait = exchange(
        ranks, me, lambda d: part_ref, lambda d: slots.at[d], local_sem.at[0], send_sem, recv_sem
    )
    wait()
    sums = jnp.sum(jnp.sum(slots[...], axis=0), axis=1, keepdims=True)
    sums = jnp.broadcast_to(sums, (sums.shape[0], TILE))

    def inner(x, y):
        value = None
        for i in range(count):
            for j in range(count):
                if x[i] is not None and y[j] is not None:
                    row = place[i, j]
                    term = x[i] * y[j] * sums[row : row + 1]
                    value = term if value is None else value + term
        return value

    none = [None] * (count - 1)
    residual = [jnp.ones((1, TILE), F32)] + none
    direction = list(residual)
    dipoles = [None] * count
    rz_now = inner(residual, residual)
    for sweep in range(ITERS):
        image = scaled(-1.0, direction, [None] + direction[:-1])
        step = rz_now / inner(direction, image)
        dipoles = scaled(step, dipoles, direction)
        residual = scaled(-step, residual, image)
        if sweep + 1 < ITERS:
            rz_next = inner(residual, residual)
            direction = scaled(rz_next / rz_now, residual, direction)
            rz_now = rz_next
    dipoles_ref[...] = combine(dipoles, soft)
    residual_ref[...] = combine(residual, bases)


def solve(bases, polar, ranks):
    dma = pltpu.SemaphoreType.DMA
    shape = bases[0].shape
    return pl.pallas_call(
        functools.partial(solve_kernel, ranks),
        in_specs=[VMEM] * 5,
        out_specs=[VMEM] * 2,
        out_shape=[jax.ShapeDtypeStruct(shape, F32)] * 2,
        scratch_shapes=[
            pltpu.VMEM((16, TILE), F32), pltpu.VMEM((ranks, 16, TILE), F32),
            dma((1,)), dma((ranks,)), dma((ranks,)),
        ],
        compiler_params=params(collective_id=1, has_side_effects=True),
        name="solve",
    )(*bases, polar)


def fixed_rows(points):
    half_size = GRID // 2
    freq = np.arange(GRID)
    mode_num = np.where(freq <= half_size, freq, freq - half_size)
    angle = (mode_num[:, None] * points[None, :] % GRID) * (2.0 * np.pi / GRID)
    return np.where((freq <= half_size)[:, None], np.cos(angle), np.sin(angle)).astype(np.float32)


def per_device(positions, field, inv_polar, x_spline, yz_spline, tile_list, tile_count):
    ranks = lax.axis_size("gx")
    rank_index = lax.axis_index("gx")
    atoms_here = positions.shape[1]
    planes = GRID // ranks
    extent = planes + 4
    blocks = atoms_here // TILE
    reach = 2 * HALO_BLK + 1
    ky_count = GRID // ranks

    def blocked(x):
        return x.reshape(-1, blocks, TILE).transpose(1, 0, 2)

    all_freq = jnp.arange(GRID, dtype=jnp.int32)
    fourier_rows = jnp.asarray(fixed_rows(np.arange(GRID)))
    ky_freq = rank_index * ky_count + jnp.arange(ky_count, dtype=jnp.int32)
    full_modes, full_weights = mode_of(all_freq, GRID)
    ky_modes, ky_weights = mode_of(ky_freq, GRID)
    green = kernel_block(ky_modes, ky_weights, full_modes, full_weights, full_modes, full_weights)
    source_rows = np.arange(ranks * extent)
    points = (source_rows // extent * planes - 2 + source_rows % extent) % GRID
    across = fixed_rows(points)
    back = jnp.asarray(np.ascontiguousarray(across.T))
    across = jnp.asarray(across)
    slots = jnp.arange(tile_list.shape[1], dtype=jnp.int32)
    wanted = jnp.arange(blocks, dtype=jnp.int32)[:, None] + jnp.arange(reach, dtype=jnp.int32)
    live = (slots[None, :] < tile_count[:, None])[:, :, None]
    near = jnp.any((tile_list[:, :, None] == wanted[:, None, :]) & live, axis=1)
    near = near.astype(F32).reshape(-1)
    yft, zf, zft = prepare(yz_spline, fourier_rows, blocks)
    xs = blocked(x_spline.reshape(2 * ORDER, atoms_here))
    pos = blocked(positions)
    polar = inv_polar.reshape(blocks, 1, TILE)
    spec_shape = jax.ShapeDtypeStruct((ranks, extent, 8, GRID), F32)
    rows_shape = jax.ShapeDtypeStruct((blocks, 3, TILE), F32)

    def advance(pv):
        spec = pl.pallas_call(
            functools.partial(spread_kernel, planes, ky_count),
            in_specs=[VMEM] * 4,
            out_specs=VMEM,
            out_shape=spec_shape,
            compiler_params=params(),
            name="spread",
        )(pv, xs, yft, zf)
        ret, pair = middle(near, spec, pv, green, across, back, ranks, ky_count)
        return pl.pallas_call(
            functools.partial(gather_kernel, planes, ky_count),
            in_specs=[VMEM] * 7,
            out_specs=[VMEM] * 2,
            out_shape=[rows_shape, jax.ShapeDtypeStruct((blocks, 8, TILE), F32)],
            scratch_shapes=[
                pltpu.VMEM((extent, GRID, 2 * GRID), BF16),
                pltpu.VMEM((extent, GRID, GRID), BF16),
            ],
            compiler_params=params(),
            name="gather",
        )(ret, xs, yft, zft, pair, pv, polar)

    bases = [blocked(field)]
    pv = jnp.concatenate([pos, bases[0] / polar, jnp.zeros((blocks, 2, TILE), F32)], axis=1)
    for sweep in range(ITERS):
        following, pv = advance(pv)
        bases.append(following)
    dipoles, residual = solve(bases, polar, ranks)

    def flat(x):
        return x.transpose(1, 0, 2).reshape(3, atoms_here)

    return flat(dipoles), flat(residual)


FIELD0 = 5


def spline_rows(u):
    v = 1.0 - u

    def inner(p):
        return ((((-4.0 * p + 4.0) * p + 6.0) * p + 4.0) * p + 1.0) * (1.0 / 24.0)

    def slope(p):
        return (((-4.0 * p + 3.0) * p + 3.0) * p + 1.0) * (1.0 / 6.0)

    middle_value = ((((6.0 * u - 12.0) * u - 6.0) * u + 12.0) * u + 11.0) * (1.0 / 24.0)
    middle_slope = (((2.0 * u - 3.0) * u - 1.0) * u + 1.0) * 0.5
    values = [v * v * v * v * (1.0 / 24.0), inner(v), middle_value, inner(u), u * u * u * u * (1.0 / 24.0)]
    slopes = [v * v * v * (-1.0 / 6.0), -slope(v), middle_slope, slope(u), u * u * u * (1.0 / 6.0)]
    return values, slopes


def turn(steps):
    wrapped = steps - GRID * jnp.floor(steps * (1.0 / GRID) + 0.5)
    half = wrapped * (np.pi / GRID)
    square = half * half
    sine = -1.0 / 39916800.0
    for c in (1.0 / 362880.0, -1.0 / 5040.0, 1.0 / 120.0, -1.0 / 6.0, 1.0):
        sine = sine * square + c
    sine = sine * half
    cosine = 1.0 / 479001600.0
    for c in (-1.0 / 3628800.0, 1.0 / 40320.0, -1.0 / 720.0, 1.0 / 24.0, -0.5, 1.0):
        cosine = cosine * square + c
    return 1.0 - 2.0 * sine * sine, 2.0 * sine * cosine


def total_of(x):
    return jnp.sum(jnp.sum(x, axis=0, keepdims=True), axis=1, keepdims=True)


def pick(rows, index):
    return jnp.take_along_axis(rows, index, axis=0, mode="promise_in_bounds")


def iota(shape, dim):
    return lax.broadcasted_iota(jnp.int32, shape, dim)


CONTRACT_LANES = (((1,), (1,)), ((), ()))


def fast_kernel(
    ranks, pos_ref, field_ref, polar_ref, xs_ref, list_ref, count_ref,
    center_ref, eye_in, zin_in, zout_in, xin_in, xout_in, yz_ref,
    dip_ref, res_ref,
    eye_ref, zin_ref, zout_ref, xin_ref, xout_ref,
    lines, info, table, flipped, yq, xw, wt, wz, vx, mix, hold, grid, spec, wide, low, green, tens, cols, place, sides, ext,
    bases, pair, out_part, pair_part, in_part, part, slots, energy,
    local_sem, all_send, all_recv, side_send, side_recv,
    ag_send, ag_recv, on_send, on_recv, pair_send, pair_recv, rs_send, rs_recv,
):
    me = lax.axis_index("gx")
    blocks = polar_ref.shape[0]
    planes = GRID // ranks
    kys = GRID // ranks
    halves = blocks // 4
    reach = 2 * HALO_BLK + 1

    def lanes(b):
        return slice(b * TILE, (b + 1) * TILE)

    loads = [
        pltpu.make_async_copy(yz_ref.at[2 * t], lines.at[t], local_sem.at[t]) for t in range(2)
    ]
    for load in loads:
        load.start()
    constants = [
        pltpu.make_async_copy(source, target, local_sem.at[2 + t])
        for t, (source, target) in enumerate(
            ((eye_in, eye_ref), (zin_in, zin_ref), (zout_in, zout_ref), (xin_in, xin_ref), (xout_in, xout_ref))
        )
    ]
    for load in constants:
        load.start()

    barrier = pltpu.get_barrier_semaphore()

    def greet_one(d, carry):
        pl.semaphore_signal(
            barrier, inc=1, device_id={"gx": lax.rem(me + d, ranks)}, device_id_type=pl.DeviceIdType.MESH
        )
        return carry

    lax.fori_loop(1, ranks, greet_one, 0)

    for c in range(3):
        for b in range(blocks):
            place[c, b : b + 1, :] = pos_ref[c : c + 1, lanes(b)]
    for c in range(3):
        for b in range(blocks):
            bases[0, c, b : b + 1, :] = field_ref[c : c + 1, lanes(b)]
    for c in range(3):
        info[me, FIELD0 + c] = bases[0, c] / polar_ref[...]
    offset = -1.5
    for k in range(1, ORDER):
        offset = offset + (1.0 * k) * xs_ref[k, 0:1, :]
    for b in range(blocks):
        info[me, 4, b : b + 1, :] = offset[:, lanes(b)]
    with jax.named_scope("yz_wait"):
        for load in loads:
            load.wait()
    marks = iota((GRID, TILE), 0).astype(F32)
    with jax.named_scope("moments"):
        for t in range(2):
            for b in range(blocks):
                line = lines[t, lanes(b), :]
                high = line.astype(BF16)
                rest = line - high.astype(F32)
                mid, tail = split(rest)
                moment = lax.dot_general(
                    center_ref[...], jnp.concatenate([high, mid, tail], axis=1), CONTRACT_LANES,
                    preferred_element_type=F32,
                )
                moment, weight = moment[:GRID], moment[GRID:]
                best = jnp.max(
                    jnp.where((jnp.abs(moment) < 0.5001) & (weight > 0.25), marks, -1.0), axis=0, keepdims=True
                )
                shift = jnp.sum(jnp.where(marks == best, moment, 0.0), axis=0, keepdims=True)
                start = best - 2.0
                info[me, 2 * t, b : b + 1, :] = jnp.where(start < 0, start + GRID, start)
                info[me, 2 * t + 1, b : b + 1, :] = shift + 0.5

    with jax.named_scope("greet_wait"):
        pl.semaphore_wait(barrier, ranks - 1)
    neighbours = [
        pltpu.make_async_remote_copy(
            src_ref=place, dst_ref=sides.at[t], send_sem=side_send.at[t], recv_sem=side_recv.at[t],
            device_id={"gx": lax.rem(me + step, ranks)}, device_id_type=pl.DeviceIdType.MESH,
        )
        for t, step in enumerate((1, ranks - 1))
    ]
    for copy in neighbours:
        copy.start()

    mesh_id = pl.DeviceIdType.MESH
    chips = ranks // 2
    rows_of_chips = chips // 2
    core, chip = lax.rem(me, 2), me // 2
    partner = me + 1 - 2 * core

    def away(d, count):
        step = (d + 1) // 2
        return lax.rem(jnp.where(d % 2 == 1, step, count - step), count)

    def slab_at(d):
        return lax.rem(me + away(d, ranks), ranks)

    def tell_all(i, owner):
        return pltpu.make_async_remote_copy(
            src_ref=info.at[owner], dst_ref=info.at[owner], send_sem=all_send.at[i], recv_sem=all_recv.at[i],
            device_id={"gx": lax.rem(me + i, ranks)}, device_id_type=mesh_id,
        )

    def got_all(d):
        off = away(d, ranks)
        tell_all(lax.rem(ranks - off, ranks), lax.rem(me + off, ranks)).wait_recv()

    def chip_at(d):
        down, side = away(d // 2, rows_of_chips), d % 2
        return lax.rem(chip // 2 + down, rows_of_chips) * 2 + lax.rem(chip % 2 + side, 2)

    def mirrored(d):
        down, side = away(d // 2, rows_of_chips), d % 2
        return lax.rem(rows_of_chips - down, rows_of_chips) * 2 + side

    def forth(d):
        return away(d // 2, rows_of_chips) * 2 + d % 2

    def same(d):
        return 2 * chip_at(d) + core

    def other(d):
        return 2 * chip_at(d) + 1 - core

    def vector(owner):
        return info.at[owner, pl.ds(FIELD0, 3)]

    def direct(d):
        return pltpu.make_async_remote_copy(
            src_ref=vector(me), dst_ref=vector(me), send_sem=ag_send.at[forth(d)], recv_sem=ag_recv.at[forth(d)],
            device_id={"gx": same(d)}, device_id_type=mesh_id,
        )

    def got_direct(d):
        pltpu.make_async_remote_copy(
            src_ref=vector(same(d)), dst_ref=vector(same(d)), send_sem=ag_send.at[mirrored(d)],
            recv_sem=ag_recv.at[mirrored(d)], device_id={"gx": same(d)}, device_id_type=mesh_id,
        ).wait_recv()

    def forward(d, owner):
        return pltpu.make_async_remote_copy(
            src_ref=vector(owner), dst_ref=vector(owner), send_sem=on_send.at[d], recv_sem=on_recv.at[d],
            device_id={"gx": partner}, device_id_type=mesh_id,
        )

    def hand_over(d):
        return pltpu.make_async_remote_copy(
            src_ref=out_part.at[other(d)], dst_ref=pair_part.at[d], send_sem=pair_send.at[d],
            recv_sem=pair_recv.at[d], device_id={"gx": partner}, device_id_type=mesh_id,
        )

    def fold(d):
        return pltpu.make_async_remote_copy(
            src_ref=out_part.at[same(d)], dst_ref=in_part.at[forth(d)], send_sem=rs_send.at[forth(d)],
            recv_sem=rs_recv.at[forth(d)], device_id={"gx": same(d)}, device_id_type=mesh_id,
        )

    def each(low, high, act):
        def one(d, carry):
            act(d)
            return carry

        lax.fori_loop(low, high, one, 0)

    each(1, ranks, lambda d: tell_all(away(d, ranks), me).start())
    for load in constants:
        load.wait()

    def modes(freq):
        number = jnp.where(freq <= GRID // 2, freq, freq - GRID // 2)
        return number.astype(F32), jnp.where((freq == 0) | (freq == GRID // 2), 1.0 / GRID, 2.0 / GRID)

    x_modes, x_weights = modes(iota((GRID, GRID), 0))
    z_modes, z_weights = modes(iota((GRID, GRID), 1))
    flat_sq = x_modes * x_modes + z_modes * z_modes
    flat_weights = x_weights * z_weights

    def filter_one(q, carry):
        y_modes, y_weights = modes(jnp.full((GRID, GRID), me * kys + q, jnp.int32))
        mode_sq = flat_sq + y_modes * y_modes
        safe_sq = jnp.where(mode_sq > 0, mode_sq, 1.0)
        value = jnp.where(mode_sq > 0, RECIP_C * jnp.exp(-DAMP * safe_sq) / safe_sq, 0.0)
        green[q] = value * (flat_weights * y_weights)
        return carry

    with jax.named_scope("filter"):
        lax.fori_loop(0, kys, filter_one, 0)

    def spread_columns(e, rows):
        for c in range(3):
            cols[e, c] = jnp.broadcast_to(rows[c], (TILE, TILE)).T

    def position_columns(e, carry):
        spread_columns(e, [ext[e, c : c + 1, :] for c in range(3)])
        return carry

    for e in range(blocks):
        for c in range(3):
            ext[e + HALO_BLK, c : c + 1, :] = place[c, e : e + 1, :]
    with jax.named_scope("poscols"):
        lax.fori_loop(HALO_BLK, HALO_BLK + blocks, position_columns, 0)
    lag = iota((8, TILE), 1) - iota((8, TILE), 0)

    def tensor(b, k):
        index = b * reach + k
        near = jnp.float32(0.0)
        for s in range(reach):
            near = jnp.where((list_ref[b, s] == b + k) & (s < count_ref[b]), PAIR_C, near)
        home = [jnp.broadcast_to(ext[b + HALO_BLK, c : c + 1, :], (8, TILE)) for c in range(3)]
        hide = jnp.where(k == HALO_BLK, 0, 4 * TILE)
        for j in range(TILE // 8):
            rows = slice(8 * j, 8 * j + 8)
            r = [home[c] - cols[b + k, c, rows, :] for c in range(3)]
            inverse = lax.rsqrt(r[0] * r[0] + r[1] * r[1] + r[2] * r[2] + 1.0)
            third = jnp.where(lag != 8 * j + hide, near, 0.0) * inverse * inverse * inverse
            tens[index, 0, rows, :] = third
            weight = third * (lax.rsqrt(inverse) * (3.0 / PAIR_C) ** 0.5)
            for c in range(3):
                tens[index, 1 + c, rows, :] = weight * r[c]

    def tensors_of(b, low, high):
        each(low, high, lambda k: tensor(b, k))

    with jax.named_scope("tensors"):
        each(0, blocks, lambda b: tensors_of(
            b, jnp.maximum(HALO_BLK - b, 0), jnp.minimum(blocks + HALO_BLK - b, reach)
        ))
    with jax.named_scope("side_wait"):
        for copy in neighbours:
            copy.wait()
    for e in range(HALO_BLK):
        for c in range(3):
            move = 1.0 * blocks if c == 0 else 0.0
            row = blocks - HALO_BLK + e
            ext[e, c : c + 1, :] = sides[0, c, row : row + 1, :] - move
            ext[blocks + HALO_BLK + e, c : c + 1, :] = sides[1, c, e : e + 1, :] + move
    with jax.named_scope("poscols2"):
        lax.fori_loop(0, HALO_BLK, position_columns, 0)
        lax.fori_loop(HALO_BLK + blocks, 2 * HALO_BLK + blocks, position_columns, 0)
    with jax.named_scope("tensors2"):
        each(0, HALO_BLK, lambda b: tensors_of(b, 0, HALO_BLK - b))
        each(blocks - HALO_BLK, blocks, lambda b: tensors_of(b, blocks + HALO_BLK - b, reach))

    freq = me * kys + iota((kys, TILE), 0)
    sine_mode = freq > GRID // 2
    number = jnp.where(sine_mode, freq - GRID // 2, freq).astype(F32)
    lead_in = jnp.where(sine_mode, GRID // 4, 0).astype(F32)
    shifts = [turn(number * (1.0 * k)) for k in range(ORDER)]

    wz[...] = jnp.zeros_like(wz)

    def beside(ref, at, parts):
        return jnp.concatenate([ref[at, t] for t in parts], axis=1)

    def flip(at):
        for j in range(4):
            both = slice(2 * j * TILE, (2 * j + 2) * TILE)
            turned = lax.dot_general(
                eye_ref[...], beside(table, at, range(2 * j, 2 * j + 2)), CONTRACT_LANES,
                preferred_element_type=F32,
            )
            flipped[at, both, :] = turned.astype(BF16)

    def block_tables(slab, b):
        at, j = slab * halves + b // 4, b % 4
        first = jnp.broadcast_to(info[slab, 0, b : b + 1, :], (kys, TILE))
        cosine, sine = turn(number * first - lead_in)
        for t in range(2):
            rows = [wt[ORDER * t + k, b : b + 1, :] for k in range(ORDER)]
            real = combine([s[0] for s in shifts], rows)
            imag = combine([s[1] for s in shifts], rows)
            yq[slab * blocks + b, t] = cosine * real - sine * imag
        begin = jnp.broadcast_to(info[slab, 2, b : b + 1, :], (8, TILE)).astype(jnp.int32)
        for i in range(GRID // 16):
            gaps = [
                jnp.minimum((iota((8, TILE), 0) + (16 * i + 8 * r - begin)) & (GRID - 1), 7)
                for r in range(2)
            ]
            for t in range(2):
                dense = jnp.concatenate([pick(wz[t, b], gap) for gap in gaps], axis=0)
                high, rest = split(dense)
                table[at, 2 * j + t, 16 * i : 16 * i + 16, :] = high
                table[at, 2 * j + t, GRID + 16 * i : GRID + 16 * i + 16, :] = rest

    def slab_tables(d, carry):
        with jax.named_scope("info_wait"):
            @pl.when(d > 0)
            def _():
                got_all(d)

        slab = slab_at(d)
        values, slopes = spline_rows(info[slab, 4])
        for k in range(ORDER):
            xw[slab, k] = values[k]
            xw[slab, ORDER + k] = slopes[k]
        for t in range(2):
            values, slopes = spline_rows(info[slab, 2 * t + 1])
            for k in range(ORDER):
                if t == 0:
                    wt[k] = values[k]
                    wt[ORDER + k] = slopes[k]
                else:
                    for b in range(blocks):
                        wz[0, b, k : k + 1, :] = values[k][b : b + 1, :]
                        wz[1, b, k : k + 1, :] = slopes[k][b : b + 1, :]

        before = slab_at(jnp.maximum(d - 1, 0)) * halves + halves - 1
        with jax.named_scope("tables"):
            for h in range(halves):
                flip(before if h == 0 else slab * halves + h - 1)
                for j in range(4):
                    block_tables(slab, 4 * h + j)
        return carry

    lax.fori_loop(0, ranks, slab_tables, 0)
    flip(slab_at(ranks - 1) * halves + halves - 1)
    each(1, ranks, lambda i: tell_all(i, me).wait_send())

    def weigh(slab, slot):
        v = [info[slab, FIELD0 + c] for c in range(3)]
        for k in range(ORDER):
            x, dx = xw[slab, k], xw[slab, ORDER + k]
            vx[slot, k] = v[0] * dx
            vx[slot, ORDER + k] = v[1] * x
            vx[slot, 2 * ORDER + k] = v[2] * x
        for h in range(halves):
            for j in range(4):
                b = 4 * h + j
                y, dy = yq[slab * blocks + b, 0], yq[slab * blocks + b, 1]
                none = jnp.zeros((kys, TILE), F32)
                lead, tail = [none] * 8, [none] * 8
                for k in range(ORDER):
                    lead[j + k] = vx[slot, k, b : b + 1, :] * y + vx[slot, ORDER + k, b : b + 1, :] * dy
                    tail[j + k] = vx[slot, 2 * ORDER + k, b : b + 1, :] * y
                for t, pieces in enumerate((lead, tail)):
                    high, rest = split(jnp.concatenate(pieces, axis=0))
                    mix[slot, h, : 8 * kys, lanes(2 * j + t)] = high
                    mix[slot, h, 8 * kys :, lanes(2 * j + t)] = rest

    def window(slab, h):
        return pl.ds(pl.multiple_of((slab * planes + 4 * h) * kys, 4 * kys), 8 * kys)

    def spread_slab(slab, slot):
        count = 8 * kys
        for h in range(halves):
            sums = dot(mix[slot, h], flipped[slab * halves + h])
            grid[window(slab, h), :] += sums[:count, :GRID] + sums[:count, GRID:] + sums[count:, :GRID]

    def read_slab(slab, slot):
        for h in range(halves):
            at = window(slab, h)
            high, rest = wide[at, :], low[at, :]
            left = jnp.concatenate(
                [jnp.concatenate([high, rest], axis=0), jnp.concatenate([high, jnp.zeros_like(rest)], axis=0)],
                axis=1,
            )
            hold[slot, h] = dot(left, beside(table, slab * halves + h, range(8)))

    def gather_slab(slab, slot):
        count = 8 * kys
        for h in range(halves):
            for j in range(4):
                b = 4 * h + j
                one = two = three = 0.0
                for k in range(ORDER):
                    rows = slice((j + k) * kys, (j + k + 1) * kys)
                    more = slice(count + (j + k) * kys, count + (j + k + 1) * kys)
                    plain = hold[slot, h, rows, lanes(2 * j)] + hold[slot, h, more, lanes(2 * j)]
                    tilted = hold[slot, h, rows, lanes(2 * j + 1)] + hold[slot, h, more, lanes(2 * j + 1)]
                    x, dx = xw[slab, k, b : b + 1, :], xw[slab, ORDER + k, b : b + 1, :]
                    one += dx * plain
                    two += x * plain
                    three += x * tilted
                y, dy = yq[slab * blocks + b, 0], yq[slab * blocks + b, 1]
                for c, term in enumerate((y * one, dy * two, y * three)):
                    out_part[slab, c, b : b + 1, :] = jnp.sum(term, axis=0, keepdims=True)

    count = ITERS + 1
    entries = {}
    for i in range(ITERS):
        for j in range(i, ITERS):
            entries[i, j] = entries[j, i] = len(set(entries.values()))
    last = len(set(entries.values()))
    for i in range(ITERS - 1):
        entries[i, ITERS] = entries[i + 1, ITERS - 1]
    entries[ITERS - 1, ITERS] = last

    def tell(i, row):
        return pltpu.make_async_remote_copy(
            src_ref=part, dst_ref=slots.at[lax.rem(me + row, ranks)], send_sem=all_send.at[i],
            recv_sem=all_recv.at[i], device_id={"gx": lax.rem(me + i, ranks)},
            device_id_type=pl.DeviceIdType.MESH,
        )

    def send_products():
        column = iota((1, TILE), 1)
        packed = jnp.zeros((1, TILE), F32)
        for i in range(ITERS):
            for j in range(i, ITERS):
                value = 0.0
                for c in range(3):
                    value += bases[i, c] * (bases[j, c] / polar_ref[...])
                packed = jnp.where(column == entries[i, j], total_of(value), packed)
        value = 0.0
        for c in range(3):
            value += pair[c] * info[me, FIELD0 + c]
        packed = jnp.where(column == last, total_of(value) - total_of(energy[...]), packed)
        part[...] = packed
        slots[me] = packed

        def one(i, carry):
            tell(i, 0).start()
            return carry

        lax.fori_loop(1, ranks, one, 0)

    def vector_columns(n):
        n = jnp.minimum(n, blocks + 2 * HALO_BLK - 1)
        e = jnp.where(n < blocks, n + HALO_BLK, jnp.where(n < blocks + HALO_BLK, n - blocks, n))
        step = jnp.where(e < HALO_BLK, ranks - 1, jnp.where(e < HALO_BLK + blocks, 0, 1))
        slab = lax.rem(me + step, ranks)
        row = lax.rem(e + blocks - HALO_BLK, blocks)
        spread_columns(e, [info[slab, FIELD0 + c, pl.ds(row, 1), :] for c in range(3)])

    def pair_rows(b, low, high, fresh):
        def one_source(k, sums):
            sums = list(sums)
            for j in range(TILE // 8):
                rows = slice(8 * j, 8 * j + 8)
                v = [cols[b + k, c, rows, :] for c in range(3)]
                w = [tens[b * reach + k, 1 + c, rows, :] for c in range(3)]
                third = tens[b * reach + k, 0, rows, :]
                along = w[0] * v[0] + w[1] * v[1] + w[2] * v[2]
                for c in range(3):
                    sums[c] = sums[c] + third * v[c]
                    sums[3 + c] = sums[3 + c] + along * w[c]
            return tuple(sums)

        sums = lax.fori_loop(low, high, one_source, (jnp.zeros((8, TILE), F32),) * 6)
        for c in range(3):
            value = jnp.sum(sums[c] - sums[3 + c], axis=0, keepdims=True)
            if fresh:
                pair[c, pl.ds(b, 1), :] = value
            else:
                pair[c, pl.ds(b, 1), :] += value

    def pair_own():
        each(0, blocks, lambda b: pair_rows(
            b, jnp.maximum(HALO_BLK - b, 0), jnp.minimum(blocks + HALO_BLK - b, reach), True
        ))

    def pair_edges():
        each(0, HALO_BLK, lambda b: pair_rows(b, 0, HALO_BLK - b, False))
        each(blocks - HALO_BLK, blocks, lambda b: pair_rows(b, blocks + HALO_BLK - b, reach, False))

    def land(it):
        with jax.named_scope("rs_wait"):
            each(1, chips, lambda d: fold(d).wait())
        for c in range(3):
            total = out_part[me, c]
            for i in range(1, chips):
                total = total + in_part[i, c]
            following = pair[c] - total
            bases[it + 1, c] = following
            info[me, FIELD0 + c] = following / polar_ref[...]

    def sweep(it, carry):
        @pl.when(it > 0)
        def _():
            forward(0, me).start()
            each(1, chips, lambda d: direct(d).start())

        grid[...] = jnp.zeros_like(grid)

        def pass_on(d):
            got_direct(d)
            forward(d, same(d)).start()

        def spread_two(m, inner):
            following = jnp.minimum(m + 1, chips - 1)
            with jax.named_scope("far_wait"):

                @pl.when((it > 0) & (m + 2 < chips))
                def _():
                    pass_on(m + 2)

                @pl.when(it > 0)
                def _():
                    forward(m, other(m)).wait_recv()

            with jax.named_scope("spread"):
                weigh(other(m), 1)
                spread_slab(same(m), 0)
                first = jnp.where(m < blocks // 2, 2 * m, jnp.maximum(2 * m - 2, blocks - 2))
                for n in (first, first + 1):
                    vector_columns(n)
                weigh(same(following), 0)
                spread_slab(other(m), 1)
            return inner

        weigh(me, 0)

        @pl.when(it == ITERS - 1)
        def _():
            with jax.named_scope("pair"):
                each(0, blocks, vector_columns)
                pair_own()

        with jax.named_scope("near_wait"):

            @pl.when(it > 0)
            def _():
                pass_on(1)

        lax.fori_loop(0, chips, spread_two, 0)

        @pl.when(it > 0)
        def _():
            forward(0, me).wait_send()
            each(1, chips, lambda d: forward(d, same(d)).wait_send())

        @pl.when(it == ITERS - 1)
        def _():
            with jax.named_scope("pair"):
                pair_edges()

        with jax.named_scope("fold"):
            size = GRID * kys
            edge = 2 * kys
            grid[size : size + edge, :] += grid[0:edge, :]
            grid[edge : 2 * edge, :] += grid[size + edge : size + 2 * edge, :]

        step = 2 * GRID
        with jax.named_scope("zin"):
            for i in range(size // step):
                high, rest = split(grid[edge + i * step : edge + (i + 1) * step, :])
                sums = dot(jnp.concatenate([high, rest], axis=1), zin_ref[...])
                spec[i * step : (i + 1) * step, :] = sums[:, :GRID] + sums[:, GRID:]
        with jax.named_scope("xinout"):
            power = jnp.zeros((8, GRID), F32)
            for q in range(0, kys, 2):
                pairs = [pl.ds(q, GRID, stride=kys), pl.ds(q + 1, GRID, stride=kys)]
                high, rest = split(jnp.concatenate([spec[s, :] for s in pairs], axis=1))
                line = dot(xin_ref[...], jnp.concatenate([high, rest, high], axis=0))
                passed = line * jnp.concatenate([green[q], green[q + 1]], axis=1)
                worth = line * passed
                power += jnp.sum((worth[:, :GRID] + worth[:, GRID:]).reshape(GRID // 8, 8, GRID), axis=0)
                line = passed
                high, rest = split(line)
                line = dot(xout_ref[...], jnp.concatenate([high, rest, high], axis=0))
                spec[pairs[0], :] = line[:, :GRID]
                spec[pairs[1], :] = line[:, GRID:]
            energy[...] = power

        @pl.when(it == ITERS - 1)
        def _():
            with jax.named_scope("gram"):
                send_products()
        with jax.named_scope("zout"):
            for i in range(size // step):
                high, rest = split(spec[i * step : (i + 1) * step, :])
                sums = dot(jnp.concatenate([high, rest], axis=1), zout_ref[...])
                high, rest = split(sums[:, :GRID] + sums[:, GRID:])
                rows = slice(edge + i * step, edge + (i + 1) * step)
                wide[rows, :] = high
                low[rows, :] = rest
            for ref in (wide, low):
                ref[0:edge, :] = ref[size : size + edge, :]
                ref[size + edge : size + 2 * edge, :] = ref[edge : 2 * edge, :]

        def turn_of(t):
            d = chips - 1 - lax.rem(t, chips)
            return 2 * chip_at(d) + jnp.where(t < chips, 1 - core, core)

        def gather_two(m, inner):
            with jax.named_scope("gather"):
                read_slab(turn_of(2 * m + 1), 1)
                gather_slab(turn_of(2 * m), 0)
                read_slab(turn_of(jnp.minimum(2 * m + 2, ranks - 1)), 0)
                gather_slab(turn_of(2 * m + 1), 1)
            for t in (2 * m, 2 * m + 1):
                d = chips - 1 - lax.rem(t, chips)

                @pl.when(t < chips)
                def _(d=d):
                    hand_over(d).start()

                @pl.when(t >= chips)
                def _(d=d):
                    hand_over(d).wait_recv()
                    for c in range(3):
                        out_part[same(d), c] += pair_part[d, c]

                @pl.when((t >= chips) & (d > 0))
                def _(d=d):
                    fold(d).start()

            return inner

        read_slab(turn_of(0), 0)
        lax.fori_loop(0, chips, gather_two, 0)

        @pl.when(it < ITERS - 1)
        def _():
            with jax.named_scope("pair"):
                pair_own()
                pair_edges()

        @pl.when(it > 0)
        def _():
            each(1, chips, lambda d: direct(d).wait_send())

        each(0, chips, lambda d: hand_over(d).wait_send())

        @pl.when(it < ITERS - 1)
        def _():
            land(it)

        return carry

    lax.fori_loop(0, ITERS, sweep, 0)

    def tell_wait(i, carry):
        tell(i, ranks - i).wait()
        return carry

    with jax.named_scope("gram_wait"):
        lax.fori_loop(1, ranks, tell_wait, 0)
    sums = jnp.sum(slots[...], axis=0)
    sums = {r: jnp.broadcast_to(sums[:, r : r + 1], (1, TILE)) for r in range(last + 1)}
    dipoles, residual = krylov(sums, entries, count)
    for c in range(3):
        first = combine(dipoles, [bases[i, c] / polar_ref[...] for i in range(ITERS)])
        for b in range(blocks):
            dip_ref[c : c + 1, lanes(b)] = first[b : b + 1, :]
    land(ITERS - 1)
    for c in range(3):
        second = combine(residual, [bases[i, c] for i in range(count)])
        for b in range(blocks):
            res_ref[c : c + 1, lanes(b)] = second[b : b + 1, :]


def krylov(sums, place, count):
    def inner(x, y):
        value = None
        for i in range(count):
            for j in range(count):
                if x[i] is not None and y[j] is not None:
                    row = place[i, j]
                    term = x[i] * y[j] * sums[row]
                    value = term if value is None else value + term
        return value

    none = [None] * (count - 1)
    residual = [jnp.ones((1, TILE), F32)] + none
    direction = list(residual)
    dipoles = [None] * count
    rz_now = inner(residual, residual)
    for sweep in range(ITERS):
        image = scaled(-1.0, direction, [None] + direction[:-1])
        step = rz_now / inner(direction, image)
        dipoles = scaled(step, dipoles, direction)
        residual = scaled(-step, residual, image)
        if sweep + 1 < ITERS:
            rz_next = inner(residual, residual)
            direction = scaled(rz_next / rz_now, residual, direction)
            rz_now = rz_next
    return dipoles, residual


def fast_shapes(ranks, blocks):
    kys = GRID // ranks
    ext_blocks = blocks + 2 * HALO_BLK
    rows = (GRID + 4) * kys
    dma = pltpu.SemaphoreType.DMA
    tile = (blocks, TILE)
    buffers = [
        ((2, blocks * TILE, GRID), F32),
        ((ranks, 8) + tile, F32),
        ((ranks * blocks // 4, 8, 2 * GRID, TILE), BF16),
        ((ranks * blocks // 4, 8 * TILE, 2 * GRID), BF16),
        ((ranks * blocks, 2, kys, TILE), F32),
        ((ranks, 2 * ORDER) + tile, F32),
        ((2 * ORDER,) + tile, F32),
        ((2, blocks, 8, TILE), F32),
        ((2, 3 * ORDER) + tile, F32),
        ((2, blocks // 4, 16 * kys, 8 * TILE), BF16),
        ((2, blocks // 4, 16 * kys, 8 * TILE), F32),
        ((rows, GRID), F32),
        ((GRID * kys, GRID), F32),
        ((rows, GRID), BF16),
        ((rows, GRID), BF16),
        ((kys, GRID, GRID), F32),
        ((blocks * (2 * HALO_BLK + 1), 4, TILE, TILE), F32),
        ((ext_blocks, 3, TILE, TILE), F32),
        ((3,) + tile, F32),
        ((2, 3) + tile, F32),
        ((ext_blocks, 8, TILE), F32),
        ((ITERS + 1, 3) + tile, F32),
        ((3,) + tile, F32),
        ((ranks, 3) + tile, F32),
        ((ranks // 2, 3) + tile, F32),
        ((ranks // 2, 3) + tile, F32),
        ((1, TILE), F32),
        ((ranks, 1, TILE), F32),
        ((8, GRID), F32),
    ]
    sems = [dma((7,))] + [dma((ranks,))] * 2 + [dma((2,))] * 2 + [dma((ranks // 2,))] * 8
    return buffers, sems


def fits_fast(ranks, blocks):
    if blocks != 8 or GRID % ranks or GRID // ranks != blocks:
        return False
    buffers, _ = fast_shapes(ranks, blocks)
    return sum(int(np.prod(s)) * np.dtype(t).itemsize for s, t in buffers) < 60 * 1024 * 1024


def halves_of(x):
    high = x.astype(BF16)
    return high, (x - high.astype(np.float32)).astype(BF16)


def fast_device(positions, field, inv_polar, x_spline, yz_spline, tile_list, tile_count):
    ranks = lax.axis_size("gx")
    atoms_here = positions.shape[1]
    blocks = atoms_here // TILE
    line = np.arange(GRID)
    center = (line[None, :] - line[:, None] + GRID // 2) % GRID - GRID // 2
    center = np.concatenate([center, np.eye(GRID)], axis=0)
    center = np.concatenate([center.astype(np.float32).astype(BF16)] * 3, axis=1)
    rows = fixed_rows(line)

    def along_z(m):
        high, rest = halves_of(np.ascontiguousarray(m))
        return np.concatenate(
            [np.concatenate([high, rest], axis=1), np.concatenate([high, np.zeros_like(rest)], axis=1)], axis=0
        )

    def along_x(m):
        high, rest = halves_of(np.ascontiguousarray(m))
        return np.concatenate([high, high, rest], axis=1)

    eye = np.eye(2 * TILE, dtype=np.float32).astype(BF16)
    constants = [center, eye, along_z(rows.T), along_z(rows), along_x(rows), along_x(rows.T)]
    buffers, sems = fast_shapes(ranks, blocks)
    smem = pl.BlockSpec(memory_space=pltpu.SMEM)
    outs = pl.pallas_call(
        functools.partial(fast_kernel, ranks),
        in_specs=[VMEM] * 4 + [smem] * 2 + [VMEM] + [pl.BlockSpec(memory_space=pl.ANY)] * len(constants),
        out_specs=[VMEM] * 2,
        out_shape=[jax.ShapeDtypeStruct(positions.shape, F32)] * 2,
        scratch_shapes=[pltpu.VMEM(c.shape, BF16) for c in constants[1:]]
        + [pltpu.VMEM(s, t) for s, t in buffers] + sems,
        compiler_params=pltpu.CompilerParams(
            vmem_limit_bytes=62 * 1024 * 1024, collective_id=2, has_side_effects=True
        ),
        name="induced",
    )(
        positions, field, inv_polar.reshape(blocks, TILE), x_spline.transpose(1, 0, 2),
        tile_list, tile_count, *[jnp.asarray(c) for c in constants], yz_spline,
    )
    return pl.pallas_call(
        finish_kernel,
        in_specs=[VMEM] * 2,
        out_specs=[VMEM] * 2,
        out_shape=[jax.ShapeDtypeStruct(positions.shape, F32)] * 2,
        name="finish",
    )(*outs)


def finish_kernel(dipoles_in, residual_in, dipoles_out, residual_out):
    dipoles_out[...] = dipoles_in[...]
    residual_out[...] = residual_in[...]


def solution(mesh):
    placed = (
        P(None, ("rep", "gx")),
        P(None, ("rep", "gx")),
        P(("rep", "gx")),
        P(None, None, ("rep", "gx")),
        P(None, ("rep", "gx"), None),
        P(("rep", "gx"), None),
        P(("rep", "gx")),
    )
    ranks = mesh.shape["gx"]

    def choose(*arrays):
        device = fast_device if fits_fast(ranks, arrays[0].shape[1] // TILE) else per_device
        return device(*arrays)

    return jax.shard_map(
        choose,
        mesh=mesh,
        in_specs=placed,
        out_specs=(P(None, ("rep", "gx")), P(None, ("rep", "gx"))),
        check_vma=False,
    )
```
